8 devices in a mesh: spin: 1 (over z), depth: 2 (over y), row: 2 (over x), col: 2 (over core).
Axes of the slice: x: 2, y: 2, z: 1, core: 2. Of those that a mesh axis runs over, the one named last changes fastest.
Arguments:
- hamiltonian: float32 [16, 1536, 1536], P('spin', 'row', 'col')
- spec_bounds: float32 [16, 2], P('spin')
- occ_count: int32 [16], P('spin')
Outputs:
- output 1: float32 [16, 1536, 1536], P('spin', 'row', 'col')
- output 2: float32 [16], P('spin')
All inputs are finite; a program needn't handle non-finite values.
Results may differ from the reference program's by a relative error of at most 0.001.
Values sent between devices are 32-bit elements.
A program may use at most 1 GiB of HBM per device.

```python
import jax
import jax.numpy as jnp
from jax import lax

ORDER = 1536
KPTS = 16
STEPS = 3


def setup_inputs(seed: int = 0, part: int = 0) -> dict:
    key_base = jax.random.fold_in(jax.random.key(seed), part)
    key_off, key_site, key_shift, key_margin, key_occ = jax.random.split(key_base, 5)
    raw_off = jax.random.normal(key_off, (KPTS, ORDER, ORDER), jnp.float32)
    coup_scale = (0.5 / ORDER) ** 0.5
    coupling = (raw_off + jnp.swapaxes(raw_off, 1, 2)) * coup_scale
    site_draw = jax.random.uniform(key_site, (KPTS, ORDER), jnp.float32)
    site_shift = jax.random.uniform(key_shift, (KPTS, 1), jnp.float32, -1.5, -0.5)
    onsite = site_shift + 0.8 * site_draw * site_draw
    identity = jnp.eye(ORDER, dtype=jnp.float32)
    hamiltonian = coupling + onsite[:, :, None] * identity
    margin = jax.random.uniform(key_margin, (KPTS, 2), jnp.float32, 0.1, 1.5)
    lower_bd = jnp.min(onsite, axis=1) - 2.0 - margin[:, 0]
    upper_bd = jnp.max(onsite, axis=1) + 2.0 + margin[:, 1]
    spec_bounds = jnp.stack([lower_bd, upper_bd], axis=1)
    occ_count = jax.random.randint(key_occ, (KPTS,), ORDER * 3 // 20, ORDER * 3 // 8 + 1, dtype=jnp.int32)
    return {'hamiltonian': hamiltonian, 'spec_bounds': spec_bounds, 'occ_count': occ_count}


def purify_one(operands):
    hamilton, bounds_one, occ_one = operands
    highest = lax.Precision.HIGHEST
    occupied = occ_one.astype(jnp.float32)
    chem_pot = jnp.trace(hamilton) / ORDER
    scale_fac = jnp.minimum(occupied / (bounds_one[1] - chem_pot), (ORDER - occupied) / (chem_pot - bounds_one[0]))
    identity = jnp.eye(ORDER, dtype=jnp.float32)
    start_dens = (scale_fac / ORDER) * (chem_pot * identity - hamilton) + (occupied / ORDER) * identity

    def purify_step(density, unused):
        dens_sq = jnp.dot(density, density, precision=highest, preferred_element_type=jnp.float32)
        dens_cube = jnp.dot(dens_sq, density, precision=highest, preferred_element_type=jnp.float32)
        tr_one = jnp.trace(density)
        tr_two = jnp.sum(density * density)
        tr_three = jnp.sum(dens_sq * density)
        purify_coef = (tr_two - tr_three) / (tr_one - tr_two)
        new_dens = ((1.0 - 2.0 * purify_coef) * density + (1.0 + purify_coef) * dens_sq - dens_cube) / (1.0 - purify_coef)
        return new_dens, None

    final_dens, unused_out = lax.scan(purify_step, start_dens, None, length=STEPS)
    energy = 2.0 * jnp.sum(final_dens * hamilton)
    return final_dens, energy


def reference(hamiltonian, spec_bounds, occ_count):
    density, energy = lax.map(purify_one, (hamiltonian, spec_bounds, occ_count))
    return density, energy
```

```python
import functools

import jax
import jax.numpy as jnp
from jax import lax
from jax.experimental import pallas as pl
from jax.experimental.pallas import tpu as pltpu
from jax.sharding import PartitionSpec as P

STEPS = 3
G = 3
NB = 2 * G
UPPER = NB * (NB + 1) // 2
F32 = jnp.float32
BF16 = jnp.bfloat16
PASSES = ((0, 2), (2, 0), (1, 1), (0, 1), (1, 0), (0, 0))
MESH = pl.DeviceIdType.MESH


def slot_of(row, col):
    return row * (2 * NB - 1 - row) // 2 + col


def slot3_of(row, col):
    return row * (2 * G - 1 - row) // 2 + col


def upper_tile(row, step):
    wrap = (row + step) // NB
    other = row + step - NB * wrap
    return row * (1 - wrap) + other * wrap, other * (1 - wrap) + row * wrap


def limbs(val):
    high = val.astype(BF16)
    rest = val - high.astype(F32)
    mid = rest.astype(BF16)
    low = (rest - mid.astype(F32)).astype(BF16)
    return high, mid, low


def put(ref, row, col, val, diag):
    for piece, part in enumerate(limbs(val)):
        ref[piece, row, col] = part
    if not diag:
        for piece, part in enumerate(limbs(val.T)):
            ref[piece, col, row] = part


def get(ref, row, col):
    low = ref[1, row, col].astype(F32) + ref[2, row, col].astype(F32)
    return ref[0, row, col].astype(F32) + low


def chain(left, right, row, col, passes):
    acc = None
    for k in range(NB):
        for p, q in passes:
            part = jnp.dot(left[p, row, k], right[q, k, col], preferred_element_type=F32)
            acc = part if acc is None else acc + part
    return acc


def fold(val):
    size = val.shape[0]
    return jnp.sum(val.reshape(size // 8, 8, val.shape[1]), axis=0)


def total(val):
    return jnp.sum(jnp.sum(val, axis=0, keepdims=True), axis=1, keepdims=True)


def flip(bit, by):
    return bit + by - 2 * bit * by


def main_kernel(
    bounds, occ, ham, land, ener,
    buf_a, buf_b, buf_c, stage, sums, e_vec,
    so_sem, r_sem, in_send, land_sem, out_send, e_sem, e_send,
):
    tile = stage.shape[2]
    order = NB * tile
    y, x, c = lax.axis_index('depth'), lax.axis_index('row'), lax.axis_index('col')
    own = y * 4 + x * 2 + c
    differ = flip(x, c)

    def device(dy, dx, cd):
        return {'depth': dy, 'row': dx, 'col': cd}

    barrier = pltpu.get_barrier_semaphore()
    for k in range(1, 8):
        pl.semaphore_signal(
            barrier, inc=1,
            device_id=device(flip(y, k // 4), flip(x, (k // 2) % 2), flip(c, k % 2)),
            device_id_type=MESH,
        )
    pl.semaphore_wait(barrier, 7)

    def h_tile(mat, i, j):
        return ham.at[mat, pl.ds(i * tile, tile), pl.ds(j * tile, tile)]

    diag_tiles = [(i, j) for i in range(G) for j in range(i, G)]
    full_tiles = [(i, j) for i in range(G) for j in range(G)]

    def send_in(rnd, carry):
        other = own + 1 - 2 * c

        @pl.when(differ == 0)
        def _():
            for i, j in diag_tiles:
                for cd in range(2):
                    mat = rnd * 8 + y * 4 + (1 - x) * 2 + cd
                    pltpu.make_async_remote_copy(
                        h_tile(mat, i, j), stage.at[rnd, slot_of(G + i, G + j)],
                        in_send, r_sem.at[rnd],
                        device_id=device(y, 1 - x, cd), device_id_type=MESH,
                    ).start()
            for i, j in diag_tiles:
                pltpu.make_async_copy(
                    h_tile(rnd * 8 + own, i, j), stage.at[rnd, slot_of(i, j)], so_sem.at[rnd]
                ).start()
                pltpu.make_async_remote_copy(
                    h_tile(rnd * 8 + other, i, j), stage.at[rnd, slot_of(i, j)],
                    in_send, so_sem.at[rnd],
                    device_id=device(y, x, 1 - c), device_id_type=MESH,
                ).start()

        @pl.when(differ == 1)
        def _():
            for i, j in full_tiles:
                pltpu.make_async_copy(
                    h_tile(rnd * 8 + own, i, j), stage.at[rnd, slot_of(i, G + j)], so_sem.at[rnd]
                ).start()
                pltpu.make_async_remote_copy(
                    h_tile(rnd * 8 + other, i, j), stage.at[rnd, slot_of(i, G + j)],
                    in_send, so_sem.at[rnd],
                    device_id=device(y, x, 1 - c), device_id_type=MESH,
                ).start()

        return carry

    lax.fori_loop(0, 2, send_in, 0)

    def wait_for(ref, sem):
        pltpu.make_async_copy(ref, ref, sem).wait()

    rows = lax.broadcasted_iota(jnp.int32, (tile, tile), 0)
    cols = lax.broadcasted_iota(jnp.int32, (tile, tile), 1)
    eye = jnp.where(rows == cols, 1.0, 0.0).astype(F32)

    def send_out(rnd, row, col):
        mat = rnd * 8 + own
        src = stage.at[rnd, slot_of(row, col)]
        k_row, k_col = row // G, col // G

        def start(dy, xd, cd, dst, may_be_self):
            def remote():
                pltpu.make_async_remote_copy(
                    src, dst, out_send, land_sem,
                    device_id=device(flip(y, dy), xd, cd), device_id_type=MESH,
                ).start()

            if may_be_self:
                pl.when(cd == c)(lambda: pltpu.make_async_copy(src, dst, land_sem).start())
                pl.when(cd != c)(remote)
            else:
                remote()

        @pl.when(k_col == 1)
        def _():
            place = k_row * slot3_of(row - G, col - G) + (1 - k_row) * (row * G + col - G)
            dst = land.at[mat * (9 - 3 * k_row) + place]
            cd = (1 - x) * k_row + x * (1 - k_row)
            start(0, 1 - x, cd, dst, False)
            start(1, 1 - x, cd, dst, False)

        @pl.when(k_row == 0)
        def _():
            place = (1 - k_col) * slot3_of(row, col) + k_col * (row * G + col - G)
            dst = land.at[mat * (6 + 3 * k_col) + place]
            cd = x * (1 - k_col) + (1 - x) * k_col
            start(1, x, cd, dst, False)
            start(0, x, cd, dst, True)

    def tiles_of(turn):
        out = []
        for half in range(2):
            row = turn * 2 + half
            for step in range(3):
                out.append((*upper_tile(row, step), step == 0))
        out.append((turn, turn + 3, False))
        return out

    def square(src):
        def turn(v, carry):
            for row, col, diag in tiles_of(v):
                if diag:
                    cross = chain(src, src, row, col, ((0, 2), (0, 1)))
                    val = chain(src, src, row, col, ((1, 1), (0, 0)))
                    val = val + (cross + cross.T)
                else:
                    val = chain(src, src, row, col, PASSES)
                put(buf_b, row, col, val, diag)
                sums[2] += fold(val * get(src, row, col)) * (1.0 if diag else 2.0)
            return carry

        sums[2] = jnp.zeros_like(sums[2])
        lax.fori_loop(0, 3, turn, 0)

    def coefs():
        t1, t2, t3 = total(sums[0]), total(sums[1]), total(sums[2])
        coef = (t2 - t3) / (t1 - t2)
        inv = 1.0 / (1.0 - coef)
        return (1.0 - 2.0 * coef) * inv, (1.0 + coef) * inv, inv

    def count(val, diag):
        if diag:
            sums[0] += fold(val * eye)
        sums[1] += fold(val * val) * (1.0 if diag else 2.0)

    def combine(src, row, col, co):
        acc = chain(buf_b, src, row, col, PASSES)
        return co[0] * get(src, row, col) + co[1] * get(buf_b, row, col) - co[2] * acc

    def cube(src, dst):
        co = coefs()
        sums[0:2] = jnp.zeros_like(sums[0:2])

        def turn(v, carry):
            for row, col, diag in tiles_of(v):
                val = combine(src, row, col, co)
                put(dst, row, col, val, diag)
                count(val, diag)
            return carry

        lax.fori_loop(0, 3, turn, 0)

    def cube_last(src, rnd):
        co = coefs()
        sums[0] = jnp.zeros_like(sums[0])

        def unit(v, step):
            last = v // NB
            row, col = upper_tile(v * (1 - last), step)
            return row * (1 - last) + step * last, col * (1 - last) + (step + 3) * last

        def turn(v, carry):
            @pl.when(v > 0)
            def _():
                for step in range(3):
                    send_out(rnd, *unit(v - 1, step))

            for step in range(3):
                row, col = unit(v, step)
                val = combine(src, row, col, co)
                slot = slot_of(row, col)
                weight = 2.0 if step else 1.0 + (v // NB).astype(F32)
                sums[0] += fold(val * stage[rnd, slot]) * weight
                stage[rnd, slot] = val
            return carry

        lax.fori_loop(0, 7, turn, 0)
        for step in range(3):
            send_out(rnd, *unit(6, step))

    def one_matrix(rnd, carry):
        mat = rnd * 8 + own
        wait_for(stage.at[rnd, pl.ds(0, 15)], so_sem.at[rnd])
        wait_for(stage.at[rnd, pl.ds(15, 6)], r_sem.at[rnd])
        diag_sum = fold(stage[rnd, slot_of(0, 0)] * eye)
        for i in range(1, NB):
            diag_sum += fold(stage[rnd, slot_of(i, i)] * eye)
        mean = total(diag_sum) / order
        filled = occ[mat].astype(F32)
        scale = jnp.minimum(
            filled / (bounds[mat, 1] - mean), (order - filled) / (mean - bounds[mat, 0])
        )
        on_diag = (scale * mean + filled) / order
        slope = scale / order
        sums[0:2] = jnp.zeros_like(sums[0:2])

        def first(v, c_):
            for row, col, diag in tiles_of(v):
                val = stage[rnd, slot_of(row, col)] * -slope
                if diag:
                    val = val + on_diag * eye
                put(buf_a, row, col, val, diag)
                count(val, diag)
            return c_

        lax.fori_loop(0, 3, first, 0)

        def step(s, c_):
            pl.when(s != 1)(lambda: square(buf_a))
            pl.when(s == 1)(lambda: square(buf_c))
            pl.when(s == 0)(lambda: cube(buf_a, buf_c))
            pl.when(s == 1)(lambda: cube(buf_c, buf_a))
            pl.when(s == 2)(lambda: cube_last(buf_a, rnd))
            return c_

        lax.fori_loop(0, STEPS, step, 0)
        e_vec[rnd] = jnp.broadcast_to(2.0 * total(sums[0]), e_vec.shape[1:])
        for k in range(1, 8):
            pltpu.make_async_remote_copy(
                e_vec.at[rnd], ener.at[mat], e_send, e_sem,
                device_id=device(flip(y, k // 4), flip(x, (k // 2) % 2), flip(c, k % 2)),
                device_id_type=MESH,
            ).start()
        pltpu.make_async_copy(e_vec.at[rnd], ener.at[mat], e_sem).start()
        return carry

    lax.fori_loop(0, 2, one_matrix, 0)

    wait_for(ener.at[pl.ds(0, 14)], e_send)
    wait_for(ener, e_sem)

    @pl.when(differ == 0)
    def _():
        wait_for(land.at[pl.ds(0, 36)], in_send)
        wait_for(land.at[pl.ds(0, 108)], out_send)
        wait_for(land.at[pl.ds(0, 96)], land_sem)

    @pl.when(differ == 1)
    def _():
        wait_for(land.at[pl.ds(0, 18)], in_send)
        wait_for(land.at[pl.ds(0, 102)], out_send)
        wait_for(land, land_sem)


def unpack_kernel(where, in0, in1, in2, out):
    tile = in0.shape[2]
    mat = pl.program_id(0)
    x, differ = where[0], where[1]
    turned = flip((mat // 2) % 2, x)

    def at(i, j):
        return (0, pl.ds(i * tile, tile), pl.ds(j * tile, tile))

    @pl.when(differ == 0)
    def _():
        packed = [in0[0, 0], in0[0, 1], in0[0, 2], in1[0, 0], in1[0, 1], in1[0, 2]]
        for i in range(G):
            for j in range(i, G):
                val = packed[slot3_of(i, j)]
                out[at(i, j)] = val
                if i != j:
                    out[at(j, i)] = val.T

    @pl.when(differ * (1 - turned) == 1)
    def _():
        for i, ref in enumerate((in0, in1, in2)):
            for j in range(G):
                out[at(i, j)] = ref[0, j]

    @pl.when(differ * turned == 1)
    def _():
        for i, ref in enumerate((in0, in1, in2)):
            for j in range(G):
                out[at(j, i)] = ref[0, j].T


def solution(mesh):
    def local_purify(ham, bounds, occ):
        mats, blk, _ = ham.shape
        tile = blk // G
        x, c = lax.axis_index('row'), lax.axis_index('col')
        any_spec = pl.BlockSpec(memory_space=pltpu.HBM)
        smem = pl.BlockSpec(memory_space=pltpu.SMEM)
        limb = pltpu.VMEM((3, NB, NB, tile, tile), BF16)
        flops = 2 * 6 * 21 * 36 * 2 * tile**3
        land, ener = pl.pallas_call(
            main_kernel,
            out_shape=(
                jax.ShapeDtypeStruct((mats * G * G, tile, tile), F32),
                jax.ShapeDtypeStruct((mats, 8, 128), F32),
            ),
            in_specs=[smem, smem, any_spec],
            out_specs=(any_spec, any_spec),
            scratch_shapes=[
                limb, limb, limb,
                pltpu.VMEM((2, UPPER, tile, tile), F32),
                pltpu.VMEM((3, 8, tile), F32),
                pltpu.VMEM((2, 8, 128), F32),
                pltpu.SemaphoreType.DMA((2,)),
                pltpu.SemaphoreType.DMA((2,)),
                pltpu.SemaphoreType.DMA,
                pltpu.SemaphoreType.DMA,
                pltpu.SemaphoreType.DMA,
                pltpu.SemaphoreType.DMA,
                pltpu.SemaphoreType.DMA,
            ],
            compiler_params=pltpu.CompilerParams(
                collective_id=0, has_side_effects=True, vmem_limit_bytes=67043328
            ),
            cost_estimate=pl.CostEstimate(flops=flops, bytes_accessed=120 * 2**20, transcendentals=0),
            name='purify',
        )(bounds, occ, ham)

        where = jnp.stack([x, x + c - 2 * x * c]).astype(jnp.int32)
        quads = land.reshape(mats * G, G, tile, tile)

        def part(k):
            def index(m, ref):
                off = ref[1]
                last = 0 if k == 2 else 2 * m + k
                return off * (3 * m + k) + (1 - off) * last, 0, 0, 0

            return pl.BlockSpec((1, G, tile, tile), index)

        density = pl.pallas_call(
            unpack_kernel,
            out_shape=jax.ShapeDtypeStruct(ham.shape, F32),
            grid_spec=pltpu.PrefetchScalarGridSpec(
                num_scalar_prefetch=1,
                grid=(mats,),
                in_specs=[part(0), part(1), part(2)],
                out_specs=pl.BlockSpec((1, blk, blk), lambda m, ref: (m, 0, 0)),
            ),
            compiler_params=pltpu.CompilerParams(vmem_limit_bytes=40 * 2**20),
            cost_estimate=pl.CostEstimate(flops=10**6, bytes_accessed=75 * 2**20, transcendentals=0),
            name='unpack',
        )(where, quads, quads, quads)
        return density, ener[:, 0, 0]

    mat_spec = P('spin', 'row', 'col')
    return jax.shard_map(
        local_purify, mesh=mesh,
        in_specs=(mat_spec, P('spin', None), P('spin')),
        out_specs=(mat_spec, P('spin')), check_vma=False,
    )
```

```python
import functools

import jax
import jax.numpy as jnp
from jax import lax
from jax.experimental import pallas as pl
from jax.experimental.pallas import tpu as pltpu
from jax.sharding import PartitionSpec as P

STEPS = 3
G = 3
NB = 2 * G
UPPER = NB * (NB + 1) // 2
UPPER3 = G * (G + 1) // 2
F32 = jnp.float32
BF16 = jnp.bfloat16
PASSES = ((0, 2), (2, 0), (1, 1), (0, 1), (1, 0), (0, 0))
MESH = pl.DeviceIdType.MESH


def slot_of(row, col):
    return row * (2 * NB - 1 - row) // 2 + col


def slot3_of(row, col):
    return row * (2 * G - 1 - row) // 2 + col


def upper_tile(row, step):
    wrap = (row + step) // NB
    other = row + step - NB * wrap
    return row * (1 - wrap) + other * wrap, other * (1 - wrap) + row * wrap


def limbs(val):
    high = val.astype(BF16)
    rest = val - high.astype(F32)
    mid = rest.astype(BF16)
    low = (rest - mid.astype(F32)).astype(BF16)
    return high, mid, low


def put(ref, row, col, val, diag):
    for piece, part in enumerate(limbs(val)):
        ref[piece, row, col] = part
    if not diag:
        for piece, part in enumerate(limbs(val.T)):
            ref[piece, col, row] = part


def get(ref, row, col):
    low = ref[1, row, col].astype(F32) + ref[2, row, col].astype(F32)
    return ref[0, row, col].astype(F32) + low


def chain(left, right, row, col, passes):
    acc = None
    for k in range(NB):
        for p, q in passes:
            part = jnp.dot(left[p, row, k], right[q, k, col], preferred_element_type=F32)
            acc = part if acc is None else acc + part
    return acc


def fold(val):
    size = val.shape[0]
    return jnp.sum(val.reshape(size // 8, 8, val.shape[1]), axis=0)


def total(val):
    return jnp.sum(jnp.sum(val, axis=0, keepdims=True), axis=1, keepdims=True)


def flip(bit, by):
    return bit + by - 2 * bit * by


def main_kernel(
    bounds, occ, ham, land, ener,
    buf_a, buf_b, buf_c, stage, sums, e_vec,
    so_sem, r_sem, in_send, land_sem, relay_sem, out_send, e_sem, e_send,
):
    tile = stage.shape[2]
    order = NB * tile
    y, x, c = lax.axis_index('depth'), lax.axis_index('row'), lax.axis_index('col')
    own = y * 4 + x * 2 + c
    differ = flip(x, c)

    def device(dy, dx, cd):
        return {'depth': dy, 'row': dx, 'col': cd}

    barrier = pltpu.get_barrier_semaphore()
    for k in range(1, 8):
        pl.semaphore_signal(
            barrier, inc=1,
            device_id=device(flip(y, k // 4), flip(x, (k // 2) % 2), flip(c, k % 2)),
            device_id_type=MESH,
        )
    pl.semaphore_wait(barrier, 7)

    def h_tile(mat, i, j):
        return ham.at[mat, pl.ds(i * tile, tile), pl.ds(j * tile, tile)]

    diag_tiles = [(i, j) for i in range(G) for j in range(i, G)]
    full_tiles = [(i, j) for i in range(G) for j in range(G)]

    def send_in(rnd, carry):
        other = own + 1 - 2 * c

        @pl.when(differ == 0)
        def _():
            for cd in range(2):
                for i, j in diag_tiles:
                    mat = rnd * 8 + y * 4 + (1 - x) * 2 + cd
                    pltpu.make_async_remote_copy(
                        h_tile(mat, i, j), stage.at[rnd, slot_of(G + i, G + j)],
                        in_send, r_sem.at[rnd],
                        device_id=device(y, 1 - x, cd), device_id_type=MESH,
                    ).start()
            for i, j in diag_tiles:
                pltpu.make_async_copy(
                    h_tile(rnd * 8 + own, i, j), stage.at[rnd, slot_of(i, j)], so_sem.at[rnd]
                ).start()
                pltpu.make_async_remote_copy(
                    h_tile(rnd * 8 + other, i, j), stage.at[rnd, slot_of(i, j)],
                    in_send, so_sem.at[rnd],
                    device_id=device(y, x, 1 - c), device_id_type=MESH,
                ).start()

        @pl.when(differ == 1)
        def _():
            for i, j in full_tiles:
                pltpu.make_async_copy(
                    h_tile(rnd * 8 + own, i, j), stage.at[rnd, slot_of(i, G + j)], so_sem.at[rnd]
                ).start()
                pltpu.make_async_remote_copy(
                    h_tile(rnd * 8 + other, i, j), stage.at[rnd, slot_of(i, G + j)],
                    in_send, so_sem.at[rnd],
                    device_id=device(y, x, 1 - c), device_id_type=MESH,
                ).start()

        return carry

    lax.fori_loop(0, 2, send_in, 0)

    def wait_for(ref, sem):
        pltpu.make_async_copy(ref, ref, sem).wait()

    rows = lax.broadcasted_iota(jnp.int32, (tile, tile), 0)
    cols = lax.broadcasted_iota(jnp.int32, (tile, tile), 1)
    eye = jnp.where(rows == cols, 1.0, 0.0).astype(F32)

    def send_out(rnd, row, col):
        mat = rnd * 8 + own
        src = stage.at[rnd, slot_of(row, col)]
        k_row, k_col = row // G, col // G

        def start(dy, xd, cd, dst, sem):
            pltpu.make_async_remote_copy(
                src, dst, out_send, sem,
                device_id=device(flip(y, dy), xd, cd), device_id_type=MESH,
            ).start()

        @pl.when(k_row + k_col == 1)
        def _():
            place = row * G + col - G
            dst = land.at[mat * 9 + place]
            start(1, x, 1 - x, dst, relay_sem.at[rnd, c, place])
            start(0, 1 - x, x, dst, land_sem)
            pl.when(differ == 1)(lambda: pltpu.make_async_copy(src, dst, land_sem).start())
            pl.when(differ == 0)(lambda: start(0, x, 1 - x, dst, land_sem))

        @pl.when(k_row == 1)
        def _():
            place = slot3_of(row - G, col - G)
            start(0, 1 - x, 1 - x, land.at[mat * 6 + place], relay_sem.at[rnd, c, place])

        @pl.when(k_col == 0)
        def _():
            dst = land.at[mat * 6 + slot3_of(row, col)]
            start(1, x, x, dst, land_sem)
            pl.when(differ == 0)(lambda: pltpu.make_async_copy(src, dst, land_sem).start())
            pl.when(differ == 1)(lambda: start(0, x, x, dst, land_sem))

    def relay(rnd, place):
        def pass_on(first_owner, per, dev):
            for cd in range(2):
                tile_ref = land.at[(rnd * 8 + first_owner + cd) * per + place]
                wait_for(tile_ref, relay_sem.at[rnd, cd, place])
                pltpu.make_async_remote_copy(
                    tile_ref, tile_ref, out_send, land_sem, device_id=dev, device_id_type=MESH
                ).start()

        @pl.when(differ == 1)
        def _():
            pass_on((1 - y) * 4 + x * 2, 9, device(y, 1 - x, x))

        @pl.when((differ == 0) & (place < UPPER3))
        def _():
            pass_on(y * 4 + (1 - x) * 2, 6, device(1 - y, x, x))

    def relay_early(rnd, turn):
        pl.when((rnd == 1) & (turn >= 3) & (turn < 3 + G * G))(lambda: relay(0, turn - 3))

    def tiles_of(turn):
        out = []
        for half in range(2):
            row = turn * 2 + half
            for step in range(3):
                out.append((*upper_tile(row, step), step == 0))
        out.append((turn, turn + 3, False))
        return out

    def square(src, rnd, before):
        def turn(v, carry):
            relay_early(rnd, before + v)
            for row, col, diag in tiles_of(v):
                if diag:
                    cross = chain(src, src, row, col, ((0, 2), (0, 1)))
                    val = chain(src, src, row, col, ((1, 1), (0, 0)))
                    val = val + (cross + cross.T)
                else:
                    val = chain(src, src, row, col, PASSES)
                put(buf_b, row, col, val, diag)
                sums[2] += fold(val * get(src, row, col)) * (1.0 if diag else 2.0)
            return carry

        sums[2] = jnp.zeros_like(sums[2])
        lax.fori_loop(0, 3, turn, 0)

    def coefs():
        t1, t2, t3 = total(sums[0]), total(sums[1]), total(sums[2])
        coef = (t2 - t3) / (t1 - t2)
        inv = 1.0 / (1.0 - coef)
        return (1.0 - 2.0 * coef) * inv, (1.0 + coef) * inv, inv

    def count(val, diag):
        if diag:
            sums[0] += fold(val * eye)
        sums[1] += fold(val * val) * (1.0 if diag else 2.0)

    def combine(src, row, col, co):
        acc = chain(buf_b, src, row, col, PASSES)
        return co[0] * get(src, row, col) + co[1] * get(buf_b, row, col) - co[2] * acc

    def cube(src, dst, rnd, before):
        co = coefs()
        sums[0:2] = jnp.zeros_like(sums[0:2])

        def turn(v, carry):
            relay_early(rnd, before + v)
            for row, col, diag in tiles_of(v):
                val = combine(src, row, col, co)
                put(dst, row, col, val, diag)
                count(val, diag)
            return carry

        lax.fori_loop(0, 3, turn, 0)

    def cube_last(src, rnd):
        co = coefs()
        sums[0] = jnp.zeros_like(sums[0])

        def unit(v, step):
            late = (v + 3) // 6
            half = (v - 3) % 2
            base = G * (1 - (v - 3) // 2)
            row = base + half * (1 + step // 2)
            col = base + (1 - half) * step + half * (1 + (step + 1) // 2)
            return row * late + v * (1 - late), col * late + (G + step) * (1 - late)

        def turn(v, carry):
            @pl.when(v > 0)
            def _():
                for step in range(3):
                    send_out(rnd, *unit(v - 1, step))

            for step in range(3):
                row, col = unit(v, step)
                val = combine(src, row, col, co)
                slot = slot_of(row, col)
                weight = jnp.where(row == col, 1.0, 2.0)
                sums[0] += fold(val * stage[rnd, slot]) * weight
                stage[rnd, slot] = val
            return carry

        lax.fori_loop(0, 7, turn, 0)
        for step in range(3):
            send_out(rnd, *unit(6, step))

    def one_matrix(rnd, carry):
        mat = rnd * 8 + own
        wait_for(stage.at[rnd, pl.ds(0, 15)], so_sem.at[rnd])
        wait_for(stage.at[rnd, pl.ds(15, 6)], r_sem.at[rnd])
        diag_sum = fold(stage[rnd, slot_of(0, 0)] * eye)
        for i in range(1, NB):
            diag_sum += fold(stage[rnd, slot_of(i, i)] * eye)
        mean = total(diag_sum) / order
        filled = occ[mat].astype(F32)
        scale = jnp.minimum(
            filled / (bounds[1, mat] - mean), (order - filled) / (mean - bounds[0, mat])
        )
        on_diag = (scale * mean + filled) / order
        slope = scale / order
        sums[0:2] = jnp.zeros_like(sums[0:2])

        def first(v, c_):
            for row, col, diag in tiles_of(v):
                val = stage[rnd, slot_of(row, col)] * -slope
                if diag:
                    val = val + on_diag * eye
                put(buf_a, row, col, val, diag)
                count(val, diag)
            return c_

        lax.fori_loop(0, 3, first, 0)

        def step(s, c_):
            pl.when(s != 1)(lambda: square(buf_a, rnd, 6 * s))
            pl.when(s == 1)(lambda: square(buf_c, rnd, 6))
            pl.when(s == 0)(lambda: cube(buf_a, buf_c, rnd, 3))
            pl.when(s == 1)(lambda: cube(buf_c, buf_a, rnd, 9))
            pl.when(s == 2)(lambda: cube_last(buf_a, rnd))
            return c_

        lax.fori_loop(0, STEPS, step, 0)
        e_vec[rnd] = jnp.broadcast_to(2.0 * total(sums[0]), e_vec.shape[1:])
        for k in range(1, 8):
            pltpu.make_async_remote_copy(
                e_vec.at[rnd], ener.at[mat], e_send, e_sem,
                device_id=device(flip(y, k // 4), flip(x, (k // 2) % 2), flip(c, k % 2)),
                device_id_type=MESH,
            ).start()
        pltpu.make_async_copy(e_vec.at[rnd], ener.at[mat], e_sem).start()
        return carry

    lax.fori_loop(0, 2, one_matrix, 0)

    for place in range(G * G):
        relay(1, place)
    wait_for(ener.at[pl.ds(0, 14)], e_send)
    wait_for(ener, e_sem)

    @pl.when(differ == 0)
    def _():
        wait_for(land.at[pl.ds(0, 36)], in_send)
        wait_for(land.at[pl.ds(0, 102)], out_send)
        wait_for(land.at[pl.ds(0, 72)], land_sem)

    @pl.when(differ == 1)
    def _():
        wait_for(land.at[pl.ds(0, 18)], in_send)
        wait_for(land.at[pl.ds(0, 108)], out_send)
        wait_for(land.at[pl.ds(0, 108)], land_sem)


PER = 2


def unpack_kernel(where, in0, in1, in2, out):
    tile = in0.shape[2]
    x, differ = where[0], where[1]
    tiles = [ref.at[0, k] for ref in (in0, in1, in2) for k in range(3 * PER)]

    for sub in range(PER):
        mat = pl.program_id(0) * PER + sub
        turned = flip((mat // 2) % 2, x)

        def at(i, j):
            return (sub, pl.ds(i * tile, tile), pl.ds(j * tile, tile))

        @pl.when(differ == 0)
        def _():
            for i in range(G):
                for j in range(i, G):
                    val = tiles[UPPER3 * sub + slot3_of(i, j)][...]
                    out[at(i, j)] = val
                    if i != j:
                        out[at(j, i)] = val.T

        @pl.when(differ * (1 - turned) == 1)
        def _():
            for i in range(G):
                for j in range(G):
                    out[at(i, j)] = tiles[G * G * sub + i * G + j][...]

        @pl.when(differ * turned == 1)
        def _():
            for i in range(G):
                for j in range(G):
                    out[at(j, i)] = tiles[G * G * sub + i * G + j][...].T


def solution(mesh):
    def local_purify(ham, bounds, occ):
        mats, blk, _ = ham.shape
        tile = blk // G
        x, c = lax.axis_index('row'), lax.axis_index('col')
        any_spec = pl.BlockSpec(memory_space=pltpu.HBM)
        smem = pl.BlockSpec(memory_space=pltpu.SMEM)
        limb = pltpu.VMEM((3, NB, NB, tile, tile), BF16)
        flops = 2 * 6 * 21 * 36 * 2 * tile**3
        land, ener = pl.pallas_call(
            main_kernel,
            out_shape=(
                jax.ShapeDtypeStruct((mats * G * G, tile, tile), F32),
                jax.ShapeDtypeStruct((mats, 8, 128), F32),
            ),
            in_specs=[smem, smem, any_spec],
            out_specs=(any_spec, any_spec),
            scratch_shapes=[
                limb, limb, limb,
                pltpu.VMEM((2, UPPER, tile, tile), F32),
                pltpu.VMEM((3, 8, tile), F32),
                pltpu.VMEM((2, 8, 128), F32),
                pltpu.SemaphoreType.DMA((2,)),
                pltpu.SemaphoreType.DMA((2,)),
                pltpu.SemaphoreType.DMA,
                pltpu.SemaphoreType.DMA,
                pltpu.SemaphoreType.DMA((2, 2, G * G)),
                pltpu.SemaphoreType.DMA,
                pltpu.SemaphoreType.DMA,
                pltpu.SemaphoreType.DMA,
            ],
            compiler_params=pltpu.CompilerParams(
                collective_id=0, has_side_effects=True, vmem_limit_bytes=67043328
            ),
            cost_estimate=pl.CostEstimate(flops=flops, bytes_accessed=120 * 2**20, transcendentals=0),
            name='purify',
        )(bounds.T, occ, ham)

        where = jnp.stack([x, x + c - 2 * x * c]).astype(jnp.int32)
        quads = land.reshape(mats * G // PER, G * PER, tile, tile)

        def part(k):
            def index(m, ref):
                off = ref[1]
                last = 0 if k == 2 else 2 * m + k
                return off * (3 * m + k) + (1 - off) * last, 0, 0, 0

            return pl.BlockSpec((1, G * PER, tile, tile), index)

        density = pl.pallas_call(
            unpack_kernel,
            out_shape=jax.ShapeDtypeStruct(ham.shape, F32),
            grid_spec=pltpu.PrefetchScalarGridSpec(
                num_scalar_prefetch=1,
                grid=(mats // PER,),
                in_specs=[part(0), part(1), part(2)],
                out_specs=pl.BlockSpec((PER, blk, blk), lambda m, ref: (m, 0, 0)),
            ),
            compiler_params=pltpu.CompilerParams(vmem_limit_bytes=40 * 2**20),
            cost_estimate=pl.CostEstimate(flops=10**6, bytes_accessed=75 * 2**20, transcendentals=0),
            name='unpack',
        )(where, quads, quads, quads)
        return density, ener[:, 0, 0]

    mat_spec = P('spin', 'row', 'col')
    return jax.shard_map(
        local_purify, mesh=mesh,
        in_specs=(mat_spec, P('spin', None), P('spin')),
        out_specs=(mat_spec, P('spin')), check_vma=False,
    )
```

```python
import functools

import jax
import jax.numpy as jnp
from jax import lax
from jax.experimental import pallas as pl
from jax.experimental.pallas import tpu as pltpu
from jax.sharding import PartitionSpec as P

STEPS = 3
G = 3
NB = 2 * G
UPPER = NB * (NB + 1) // 2
UPPER3 = G * (G + 1) // 2
OVER_X = 7
F32 = jnp.float32
BF16 = jnp.bfloat16
PASSES = ((0, 2), (2, 0), (1, 1), (0, 1), (1, 0), (0, 0))
MESH = pl.DeviceIdType.MESH


def slot_of(row, col):
    return row * (2 * NB - 1 - row) // 2 + col


def slot3_of(row, col):
    return row * (2 * G - 1 - row) // 2 + col


def upper_tile(row, step):
    wrap = (row + step) // NB
    other = row + step - NB * wrap
    return row * (1 - wrap) + other * wrap, other * (1 - wrap) + row * wrap


def limbs(val):
    high = val.astype(BF16)
    rest = val - high.astype(F32)
    mid = rest.astype(BF16)
    low = (rest - mid.astype(F32)).astype(BF16)
    return high, mid, low


def put(ref, row, col, val, diag):
    for piece, part in enumerate(limbs(val)):
        ref[piece, row, col] = part
    if not diag:
        for piece, part in enumerate(limbs(val.T)):
            ref[piece, col, row] = part


def get(ref, row, col):
    low = ref[1, row, col].astype(F32) + ref[2, row, col].astype(F32)
    return ref[0, row, col].astype(F32) + low


def chain(left, right, row, col, passes):
    acc = None
    for k in range(NB):
        for p, q in passes:
            part = jnp.dot(left[p, row, k], right[q, k, col], preferred_element_type=F32)
            acc = part if acc is None else acc + part
    return acc


def fold(val):
    size = val.shape[0]
    return jnp.sum(val.reshape(size // 8, 8, val.shape[1]), axis=0)


def total(val):
    return jnp.sum(jnp.sum(val, axis=0, keepdims=True), axis=1, keepdims=True)


def flip(bit, by):
    return bit + by - 2 * bit * by


def main_kernel(
    bounds, occ, ham, land, ener,
    buf_a, buf_b, buf_c, stage, sums, e_vec,
    so_sem, r_sem, in_send, land_sem, relay_sem, out_send, e_sem, e_send,
):
    tile = stage.shape[2]
    order = NB * tile
    y, x, c = lax.axis_index('depth'), lax.axis_index('row'), lax.axis_index('col')
    own = y * 4 + x * 2 + c
    differ = flip(x, c)

    def device(dy, dx, cd):
        return {'depth': dy, 'row': dx, 'col': cd}

    barrier = pltpu.get_barrier_semaphore()
    for k in range(1, 8):
        pl.semaphore_signal(
            barrier, inc=1,
            device_id=device(flip(y, k // 4), flip(x, (k // 2) % 2), flip(c, k % 2)),
            device_id_type=MESH,
        )
    pl.semaphore_wait(barrier, 7)

    def h_tile(mat, i, j):
        return ham.at[mat, pl.ds(i * tile, tile), pl.ds(j * tile, tile)]

    def parts(diag):
        half = tile // 2
        if not diag:
            return [(slice(None), slice(None))]
        return [(pl.ds(0, half), slice(None)), (pl.ds(half, half), pl.ds(half, half))]

    diag_tiles = [(i, j) for i in range(G) for j in range(i, G)]
    full_tiles = [(i, j) for i in range(G) for j in range(G)]

    def send_in(rnd, carry):
        other = own + 1 - 2 * c

        @pl.when(differ == 0)
        def _():
            for cd in range(2):
                for i, j in diag_tiles:
                    mat = rnd * 8 + y * 4 + (1 - x) * 2 + cd
                    for part in parts(i == j):
                        pltpu.make_async_remote_copy(
                            h_tile(mat, i, j).at[part],
                            stage.at[rnd, slot_of(G + i, G + j)].at[part],
                            in_send, r_sem.at[rnd],
                            device_id=device(y, 1 - x, cd), device_id_type=MESH,
                        ).start()
            for i, j in diag_tiles:
                pltpu.make_async_copy(
                    h_tile(rnd * 8 + own, i, j), stage.at[rnd, slot_of(i, j)], so_sem.at[rnd]
                ).start()
                pltpu.make_async_remote_copy(
                    h_tile(rnd * 8 + other, i, j), stage.at[rnd, slot_of(i, j)],
                    in_send, so_sem.at[rnd],
                    device_id=device(y, x, 1 - c), device_id_type=MESH,
                ).start()

        @pl.when(differ == 1)
        def _():
            for i, j in full_tiles:
                pltpu.make_async_copy(
                    h_tile(rnd * 8 + own, i, j), stage.at[rnd, slot_of(i, G + j)], so_sem.at[rnd]
                ).start()
                pltpu.make_async_remote_copy(
                    h_tile(rnd * 8 + other, i, j), stage.at[rnd, slot_of(i, G + j)],
                    in_send, so_sem.at[rnd],
                    device_id=device(y, x, 1 - c), device_id_type=MESH,
                ).start()

        return carry

    lax.fori_loop(0, 2, send_in, 0)

    def wait_for(ref, sem):
        pltpu.make_async_copy(ref, ref, sem).wait()

    rows = lax.broadcasted_iota(jnp.int32, (tile, tile), 0)
    cols = lax.broadcasted_iota(jnp.int32, (tile, tile), 1)
    eye = jnp.where(rows == cols, 1.0, 0.0).astype(F32)

    def send_out(rnd, row, col):
        mat = rnd * 8 + own
        src = stage.at[rnd, slot_of(row, col)]
        k_row, k_col = row // G, col // G

        def start(dy, xd, cd, dst, sem, diag=False):
            for part in parts(diag):
                pltpu.make_async_remote_copy(
                    src.at[part], dst.at[part], out_send, sem,
                    device_id=device(flip(y, dy), xd, cd), device_id_type=MESH,
                ).start()

        def keep(dst, diag=False):
            for part in parts(diag):
                pltpu.make_async_copy(src.at[part], dst.at[part], land_sem).start()

        @pl.when(k_row + k_col == 1)
        def _():
            place = row * G + col - G
            dst = land.at[mat * 9 + place]
            sem = relay_sem.at[rnd, c, place]

            @pl.when(place < OVER_X)
            def _():
                start(1, x, 1 - x, dst, sem)
                start(0, 1 - x, x, dst, land_sem)

            @pl.when(place >= OVER_X)
            def _():
                start(0, 1 - x, x, dst, sem)
                start(1, x, 1 - x, dst, land_sem)

            pl.when(differ == 1)(lambda: keep(dst))
            pl.when(differ == 0)(lambda: start(0, x, 1 - x, dst, land_sem))

        for diag in (False, True):
            same = (row == col) if diag else (row != col)

            @pl.when((k_row == 1) & same)
            def _():
                place = slot3_of(row - G, col - G)
                start(0, 1 - x, 1 - x, land.at[mat * 6 + place], relay_sem.at[rnd, c, place], diag)

            @pl.when((k_col == 0) & same)
            def _():
                dst = land.at[mat * 6 + slot3_of(row, col)]
                start(1, x, x, dst, land_sem, diag)
                pl.when(differ == 0)(lambda: keep(dst, diag))
                pl.when(differ == 1)(lambda: start(0, x, x, dst, land_sem, diag))

    def relay(rnd, place):
        def pass_on(first_owner, per, dev, diag=False):
            for cd in range(2):
                tile_ref = land.at[(rnd * 8 + first_owner + cd) * per + place]
                whole = tile_ref.at[pl.ds(0, tile * 3 // 4)] if diag else tile_ref
                wait_for(whole, relay_sem.at[rnd, cd, place])
                for part in parts(diag):
                    pltpu.make_async_remote_copy(
                        tile_ref.at[part], tile_ref.at[part], out_send, land_sem,
                        device_id=dev, device_id_type=MESH,
                    ).start()

        @pl.when((differ == 1) & (place < OVER_X))
        def _():
            pass_on((1 - y) * 4 + x * 2, 9, device(y, 1 - x, x))

        @pl.when((differ == 1) & (place >= OVER_X))
        def _():
            pass_on(y * 4 + (1 - x) * 2, 9, device(1 - y, x, c))

        on_diag = (place == 0) | (place == 3) | (place == 5)

        @pl.when((differ == 0) & (place < UPPER3) & on_diag)
        def _():
            pass_on(y * 4 + (1 - x) * 2, 6, device(1 - y, x, x), True)

        @pl.when((differ == 0) & (place < UPPER3) & ~on_diag)
        def _():
            pass_on(y * 4 + (1 - x) * 2, 6, device(1 - y, x, x))

    def relay_early(rnd, turn):
        pl.when((rnd == 1) & (turn >= 3) & (turn < 3 + G * G))(lambda: relay(0, turn - 3))

    def tiles_of(turn):
        out = []
        for half in range(2):
            row = turn * 2 + half
            for step in range(3):
                out.append((*upper_tile(row, step), step == 0))
        out.append((turn, turn + 3, False))
        return out

    def square(src, rnd, before):
        def turn(v, carry):
            relay_early(rnd, before + v)
            for row, col, diag in tiles_of(v):
                if diag:
                    cross = chain(src, src, row, col, ((0, 2), (0, 1)))
                    val = chain(src, src, row, col, ((1, 1), (0, 0)))
                    val = val + (cross + cross.T)
                else:
                    val = chain(src, src, row, col, PASSES)
                put(buf_b, row, col, val, diag)
                sums[2] += fold(val * get(src, row, col)) * (1.0 if diag else 2.0)
            return carry

        sums[2] = jnp.zeros_like(sums[2])
        lax.fori_loop(0, 3, turn, 0)

    def coefs():
        t1, t2, t3 = total(sums[0]), total(sums[1]), total(sums[2])
        coef = (t2 - t3) / (t1 - t2)
        inv = 1.0 / (1.0 - coef)
        return (1.0 - 2.0 * coef) * inv, (1.0 + coef) * inv, inv

    def count(val, diag):
        if diag:
            sums[0] += fold(val * eye)
        sums[1] += fold(val * val) * (1.0 if diag else 2.0)

    def combine(src, row, col, co):
        acc = chain(buf_b, src, row, col, PASSES)
        return co[0] * get(src, row, col) + co[1] * get(buf_b, row, col) - co[2] * acc

    def cube(src, dst, rnd, before):
        co = coefs()
        sums[0:2] = jnp.zeros_like(sums[0:2])

        def turn(v, carry):
            relay_early(rnd, before + v)
            for row, col, diag in tiles_of(v):
                val = combine(src, row, col, co)
                put(dst, row, col, val, diag)
                count(val, diag)
            return carry

        lax.fori_loop(0, 3, turn, 0)

    def cube_last(src, rnd):
        co = coefs()
        sums[0] = jnp.zeros_like(sums[0])

        def unit(v, step):
            late = (v + 3) // 6
            half = (v - 3) % 2
            base = G * (1 - (v - 3) // 2)
            row = base + half * (1 + step // 2)
            col = base + (1 - half) * step + half * (1 + (step + 1) // 2)
            return row * late + v * (1 - late), col * late + (G + step) * (1 - late)

        def turn(v, carry):
            @pl.when(v > 0)
            def _():
                for step in range(3):
                    send_out(rnd, *unit(v - 1, step))

            for step in range(3):
                row, col = unit(v, step)
                val = combine(src, row, col, co)
                slot = slot_of(row, col)
                weight = jnp.where(row == col, 1.0, 2.0)
                sums[0] += fold(val * stage[rnd, slot]) * weight
                stage[rnd, slot] = val
            return carry

        lax.fori_loop(0, 7, turn, 0)
        for step in range(3):
            send_out(rnd, *unit(6, step))

    def one_matrix(rnd, carry):
        mat = rnd * 8 + own
        wait_for(stage.at[rnd, pl.ds(0, 15)], so_sem.at[rnd])
        wait_for(stage.at[rnd, pl.ds(15, 6), pl.ds(0, tile * 7 // 8)], r_sem.at[rnd])
        half = tile // 2
        for i in range(G, NB):
            slot = slot_of(i, i)
            stage[rnd, slot, half:, :half] = stage[rnd, slot, :half, half:].T
        diag_sum = fold(stage[rnd, slot_of(0, 0)] * eye)
        for i in range(1, NB):
            diag_sum += fold(stage[rnd, slot_of(i, i)] * eye)
        mean = total(diag_sum) / order
        filled = occ[mat].astype(F32)
        scale = jnp.minimum(
            filled / (bounds[1, mat] - mean), (order - filled) / (mean - bounds[0, mat])
        )
        on_diag = (scale * mean + filled) / order
        slope = scale / order
        sums[0:2] = jnp.zeros_like(sums[0:2])

        def first(v, c_):
            for row, col, diag in tiles_of(v):
                val = stage[rnd, slot_of(row, col)] * -slope
                if diag:
                    val = val + on_diag * eye
                put(buf_a, row, col, val, diag)
                count(val, diag)
            return c_

        lax.fori_loop(0, 3, first, 0)

        def step(s, c_):
            pl.when(s != 1)(lambda: square(buf_a, rnd, 6 * s))
            pl.when(s == 1)(lambda: square(buf_c, rnd, 6))
            pl.when(s == 0)(lambda: cube(buf_a, buf_c, rnd, 3))
            pl.when(s == 1)(lambda: cube(buf_c, buf_a, rnd, 9))
            pl.when(s == 2)(lambda: cube_last(buf_a, rnd))
            return c_

        lax.fori_loop(0, STEPS, step, 0)
        e_vec[rnd] = jnp.broadcast_to(2.0 * total(sums[0]), e_vec.shape[1:])
        for k in range(1, 8):
            pltpu.make_async_remote_copy(
                e_vec.at[rnd], ener.at[mat], e_send, e_sem,
                device_id=device(flip(y, k // 4), flip(x, (k // 2) % 2), flip(c, k % 2)),
                device_id_type=MESH,
            ).start()
        pltpu.make_async_copy(e_vec.at[rnd], ener.at[mat], e_sem).start()
        return carry

    lax.fori_loop(0, 2, one_matrix, 0)

    def relay_late(place, carry):
        relay(1, place)
        return carry

    lax.fori_loop(0, G * G, relay_late, 0)
    wait_for(ener.at[pl.ds(0, 14)], e_send)
    wait_for(ener, e_sem)

    def wait_tiles(quarters, sem):
        wait_for(ham.at[pl.ds(0, 16), pl.ds(0, quarters * tile // 192), :], sem)

    @pl.when(differ == 0)
    def _():
        wait_tiles(48 + 84, in_send)
        wait_tiles(4 * 96, out_send)
        wait_tiles(4 * 63, land_sem)

    @pl.when(differ == 1)
    def _():
        wait_tiles(4 * 18, in_send)
        wait_tiles(414, out_send)
        wait_tiles(4 * 108, land_sem)


PER = 2


def unpack_kernel(in0, in1, in2, out):
    tile = in0.shape[2]
    half = tile // 2
    x, c = lax.axis_index('row'), lax.axis_index('col')
    differ = flip(x, c)
    tiles = [ref.at[0, k] for ref in (in0, in1, in2) for k in range(3 * PER)]

    for sub in range(PER):
        mat = pl.program_id(0) * PER + sub
        turned = flip((mat // 2) % 2, x)

        def write(i, j, val):
            rows, cols = val.shape
            out[sub, pl.ds(i * half, rows), pl.ds(j * half, cols)] = val

        @pl.when(differ == 0)
        def _():
            for i in range(G):
                for j in range(i, G):
                    ref = tiles[UPPER3 * sub + slot3_of(i, j)]
                    if i == j:
                        top = ref[:half, :]
                        write(2 * i, 2 * i, top)
                        write(2 * i + 1, 2 * i, top[:, half:].T)
                        write(2 * i + 1, 2 * i + 1, ref[half:, half:])
                    else:
                        val = ref[...]
                        write(2 * i, 2 * j, val)
                        write(2 * j, 2 * i, val.T)

        @pl.when(differ * (1 - turned) == 1)
        def _():
            for i in range(G):
                for j in range(G):
                    write(2 * i, 2 * j, tiles[G * G * sub + i * G + j][...])

        @pl.when(differ * turned == 1)
        def _():
            for i in range(G):
                for j in range(G):
                    write(2 * j, 2 * i, tiles[G * G * sub + i * G + j][...].T)


def solution(mesh):
    def local_purify(ham, bounds, occ):
        mats, blk, _ = ham.shape
        tile = blk // G
        any_spec = pl.BlockSpec(memory_space=pltpu.HBM)
        smem = pl.BlockSpec(memory_space=pltpu.SMEM)
        limb = pltpu.VMEM((3, NB, NB, tile, tile), BF16)
        flops = 2 * 6 * 21 * 36 * 2 * tile**3
        land, ener = pl.pallas_call(
            main_kernel,
            out_shape=(
                jax.ShapeDtypeStruct((mats * G * G, tile, tile), F32),
                jax.ShapeDtypeStruct((mats, 8, 128), F32),
            ),
            in_specs=[smem, smem, any_spec],
            out_specs=(any_spec, any_spec),
            scratch_shapes=[
                limb, limb, limb,
                pltpu.VMEM((2, UPPER, tile, tile), F32),
                pltpu.VMEM((3, 8, tile), F32),
                pltpu.VMEM((2, 8, 128), F32),
                pltpu.SemaphoreType.DMA((2,)),
                pltpu.SemaphoreType.DMA((2,)),
                pltpu.SemaphoreType.DMA,
                pltpu.SemaphoreType.DMA,
                pltpu.SemaphoreType.DMA((2, 2, G * G)),
                pltpu.SemaphoreType.DMA,
                pltpu.SemaphoreType.DMA,
                pltpu.SemaphoreType.DMA,
            ],
            compiler_params=pltpu.CompilerParams(
                collective_id=0, has_side_effects=True, vmem_limit_bytes=67043328
            ),
            cost_estimate=pl.CostEstimate(flops=flops, bytes_accessed=120 * 2**20, transcendentals=0),
            name='purify',
        )(bounds.T, occ, ham)

        quads = land.reshape(mats * G // PER, G * PER, tile, tile)

        def part(k):
            def index(m):
                off = flip(lax.axis_index('row'), lax.axis_index('col'))
                last = 0 if k == 2 else 2 * m + k
                return off * (3 * m + k) + (1 - off) * last, 0, 0, 0

            return pl.BlockSpec((1, G * PER, tile, tile), index)

        density = pl.pallas_call(
            unpack_kernel,
            out_shape=jax.ShapeDtypeStruct(ham.shape, F32),
            grid=(mats // PER,),
            in_specs=[part(0), part(1), part(2)],
            out_specs=pl.BlockSpec((PER, blk, blk), lambda m: (m, 0, 0)),
            compiler_params=pltpu.CompilerParams(vmem_limit_bytes=40 * 2**20),
            cost_estimate=pl.CostEstimate(flops=10**6, bytes_accessed=75 * 2**20, transcendentals=0),
            name='unpack',
        )(quads, quads, quads)
        return density, ener[:, 0, 0]

    mat_spec = P('spin', 'row', 'col')
    return jax.shard_map(
        local_purify, mesh=mesh,
        in_specs=(mat_spec, P('spin', None), P('spin')),
        out_specs=(mat_spec, P('spin')), check_vma=False,
    )
```

```python
import functools

import jax
import jax.numpy as jnp
from jax import lax
from jax.experimental import pallas as pl
from jax.experimental.pallas import tpu as pltpu
from jax.sharding import PartitionSpec as P

STEPS = 3
G = 3
NB = 2 * G
UPPER = NB * (NB + 1) // 2
UPPER3 = G * (G + 1) // 2
OVER_X = 7
F32 = jnp.float32
BF16 = jnp.bfloat16
PASSES = ((0, 2), (2, 0), (1, 1), (0, 1), (1, 0), (0, 0))
MESH = pl.DeviceIdType.MESH


def slot_of(row, col):
    return row * (2 * NB - 1 - row) // 2 + col


def slot3_of(row, col):
    return row * (2 * G - 1 - row) // 2 + col


def upper_tile(row, step):
    wrap = (row + step) // NB
    other = row + step - NB * wrap
    return row * (1 - wrap) + other * wrap, other * (1 - wrap) + row * wrap


def limbs(val):
    high = val.astype(BF16)
    rest = val - high.astype(F32)
    mid = rest.astype(BF16)
    low = (rest - mid.astype(F32)).astype(BF16)
    return high, mid, low


def put(ref, row, col, val, diag):
    for piece, part in enumerate(limbs(val)):
        ref[piece, row, col] = part
    if not diag:
        for piece, part in enumerate(limbs(val.T)):
            ref[piece, col, row] = part


def get(ref, row, col):
    low = ref[1, row, col].astype(F32) + ref[2, row, col].astype(F32)
    return ref[0, row, col].astype(F32) + low


def chain(left, right, row, col, passes):
    acc = None
    for k in range(NB):
        for p, q in passes:
            part = jnp.dot(left[p, row, k], right[q, k, col], preferred_element_type=F32)
            acc = part if acc is None else acc + part
    return acc


def fold(val):
    size = val.shape[0]
    return jnp.sum(val.reshape(size // 8, 8, val.shape[1]), axis=0)


def total(val):
    return jnp.sum(jnp.sum(val, axis=0, keepdims=True), axis=1, keepdims=True)


def flip(bit, by):
    return bit + by - 2 * bit * by


def main_kernel(
    bounds, occ, ham, land, ener,
    buf_a, buf_b, buf_c, stage, sums, e_vec,
    so_sem, r_sem, in_send, aid_sem, aid_send, land_sem, relay_sem, out_send, e_sem, e_send,
):
    tile = stage.shape[2]
    order = NB * tile
    y, x, c = lax.axis_index('depth'), lax.axis_index('row'), lax.axis_index('col')
    own = y * 4 + x * 2 + c
    differ = flip(x, c)

    def device(dy, dx, cd):
        return {'depth': dy, 'row': dx, 'col': cd}

    barrier = pltpu.get_barrier_semaphore()
    for k in range(1, 8):
        pl.semaphore_signal(
            barrier, inc=1,
            device_id=device(flip(y, k // 4), flip(x, (k // 2) % 2), flip(c, k % 2)),
            device_id_type=MESH,
        )
    pl.semaphore_wait(barrier, 7)

    def h_tile(mat, i, j):
        return ham.at[mat, pl.ds(i * tile, tile), pl.ds(j * tile, tile)]

    def parts(diag):
        half = tile // 2
        if not diag:
            return [(slice(None), slice(None))]
        return [(pl.ds(0, half), slice(None)), (pl.ds(half, half), pl.ds(half, half))]

    diag_tiles = [(i, j) for i in range(G) for j in range(i, G)]

    def send_in(e, carry):
        late = e // 3
        aid = (e % 3) % 2 * (1 - late)
        cd = (1 - late) * ((e + 1) // 2) + late * (e - 3)
        mat = 8 * (aid + late) + cd * (1 - aid) + y * 4
        put_in = 2 * aid + late

        @pl.when(differ == 0)
        def _():
            for i, j in diag_tiles:
                for part in parts(i == j):
                    pltpu.make_async_remote_copy(
                        h_tile(mat + (1 - x) * 2, i, j).at[part],
                        stage.at[put_in, slot_of(G + i, G + j)].at[part],
                        in_send, r_sem.at[put_in],
                        device_id=device(y, 1 - x, cd), device_id_type=MESH,
                    ).start()

        def near(tiles, shift):
            for i, j in tiles:
                near_tile(i, j, shift)

        def near_row(i, carry_):
            for j in range(G):
                near_tile(i, j, G)
            return carry_

        def near_tile(i, j, shift):
            src = h_tile(mat + x * 2, i, j)
            dst = stage.at[put_in, slot_of(i, shift + j)]

            @pl.when(cd == c)
            def _():
                pltpu.make_async_copy(src, dst, so_sem.at[put_in]).start()

            @pl.when(cd != c)
            def _():
                pltpu.make_async_remote_copy(
                    src, dst, in_send, so_sem.at[put_in],
                    device_id=device(y, x, cd), device_id_type=MESH,
                ).start()

        pl.when(differ == 0)(lambda: near(diag_tiles, 0))

        @pl.when(differ == 1)
        def _():
            lax.fori_loop(0, G, near_row, 0)

        return carry

    lax.fori_loop(0, 5, send_in, 0)

    def wait_for(ref, sem):
        pltpu.make_async_copy(ref, ref, sem).wait()

    rows = lax.broadcasted_iota(jnp.int32, (tile, tile), 0)
    cols = lax.broadcasted_iota(jnp.int32, (tile, tile), 1)
    eye = jnp.where(rows == cols, 1.0, 0.0).astype(F32)

    def send_out(rnd, row, col):
        mat = rnd * 8 + own
        src = stage.at[rnd, slot_of(row, col)]
        k_row, k_col = row // G, col // G

        def start(dy, xd, cd, dst, sem, diag=False):
            for part in parts(diag):
                pltpu.make_async_remote_copy(
                    src.at[part], dst.at[part], out_send, sem,
                    device_id=device(flip(y, dy), xd, cd), device_id_type=MESH,
                ).start()

        def keep(dst, diag=False):
            for part in parts(diag):
                pltpu.make_async_copy(src.at[part], dst.at[part], land_sem).start()

        @pl.when(k_row + k_col == 1)
        def _():
            place = row * G + col - G
            dst = land.at[mat * 9 + place]
            sem = relay_sem.at[rnd, c, place]

            @pl.when(place < OVER_X)
            def _():
                start(1, x, 1 - x, dst, sem)
                start(0, 1 - x, x, dst, land_sem)

            @pl.when(place >= OVER_X)
            def _():
                start(0, 1 - x, x, dst, sem)
                start(1, x, 1 - x, dst, land_sem)

            pl.when(differ == 1)(lambda: keep(dst))
            pl.when(differ == 0)(lambda: start(0, x, 1 - x, dst, land_sem))

        for diag in (False, True):
            same = (row == col) if diag else (row != col)

            @pl.when((k_row == 1) & same)
            def _():
                place = slot3_of(row - G, col - G)
                start(0, 1 - x, 1 - x, land.at[mat * 6 + place], relay_sem.at[rnd, c, place], diag)

            @pl.when((k_col == 0) & same)
            def _():
                dst = land.at[mat * 6 + slot3_of(row, col)]
                start(1, x, x, dst, land_sem, diag)
                pl.when(differ == 0)(lambda: keep(dst, diag))
                pl.when(differ == 1)(lambda: start(0, x, x, dst, land_sem, diag))

    def relay(rnd, place):
        def pass_on(first_owner, per, dev, diag=False):
            for cd in range(2):
                tile_ref = land.at[(rnd * 8 + first_owner + cd) * per + place]
                whole = tile_ref.at[pl.ds(0, tile * 3 // 4)] if diag else tile_ref
                wait_for(whole, relay_sem.at[rnd, cd, place])
                for part in parts(diag):
                    pltpu.make_async_remote_copy(
                        tile_ref.at[part], tile_ref.at[part], out_send, land_sem,
                        device_id=dev, device_id_type=MESH,
                    ).start()

        @pl.when((differ == 1) & (place < OVER_X))
        def _():
            pass_on((1 - y) * 4 + x * 2, 9, device(y, 1 - x, x))

        @pl.when((differ == 1) & (place >= OVER_X))
        def _():
            pass_on(y * 4 + (1 - x) * 2, 9, device(1 - y, x, c))

        on_diag = (place == 0) | (place == 3) | (place == 5)

        @pl.when((differ == 0) & (place < UPPER3) & on_diag)
        def _():
            pass_on(y * 4 + (1 - x) * 2, 6, device(1 - y, x, x), True)

        @pl.when((differ == 0) & (place < UPPER3) & ~on_diag)
        def _():
            pass_on(y * 4 + (1 - x) * 2, 6, device(1 - y, x, x))

    def relay_early(job, turn):
        one = (c == 1) & (turn >= 1) & (turn < 1 + G * G)
        two = (c == 0) & (turn >= 9) & (turn < 14)

        @pl.when((job == 2) & (one | two))
        def _():
            low = c * (turn - 1) + (1 - c) * 2 * (turn - 9)
            high = low + 1 + (1 - c) * (1 - turn // 13)

            def body(place, carry):
                relay(0, place)
                return carry

            lax.fori_loop(low, high, body, 0)

    def tiles_of(turn):
        out = []
        for half in range(2):
            row = turn * 2 + half
            for step in range(3):
                out.append((*upper_tile(row, step), step == 0))
        out.append((turn, turn + 3, False))
        return out

    def unit(v, step):
        late = (v + 3) // 6
        half = (v - 3) % 2
        base = G * (1 - (v - 3) // 2)
        row = base + half * (1 + step // 2)
        col = base + (1 - half) * step + half * (1 + (step + 1) // 2)
        return row * late + v * (1 - late), col * late + (G + step) * (1 - late)

    def send_aid(v):
        for row, col, _ in tiles_of(v):
            ref = stage.at[2, slot_of(row, col)]
            pltpu.make_async_remote_copy(
                ref, ref, aid_send, aid_sem, device_id=device(y, x, 0), device_id_type=MESH
            ).start()

    def square(src, job, before, may_aid):
        own_job = (job + 1) // 2

        def turn(v, carry):
            relay_early(job, before + v)
            if may_aid:
                pl.when((job == 0) & (v > 0))(lambda: send_aid(v - 1))
            for row, col, diag in tiles_of(v):
                if diag:
                    cross = chain(src, src, row, col, ((0, 2), (0, 1)))
                    val = chain(src, src, row, col, ((1, 1), (0, 0)))
                    val = val + (cross + cross.T)
                else:
                    val = chain(src, src, row, col, PASSES)
                put(buf_b, row, col, val, diag)
                if may_aid:
                    stage[2, slot_of(row, col) * (1 - own_job) + UPPER * own_job] = val
                sums[2] += fold(val * get(src, row, col)) * (1.0 if diag else 2.0)
            return carry

        sums[2] = jnp.zeros_like(sums[2])
        lax.fori_loop(0, 3, turn, 0)
        if may_aid:
            pl.when(job == 0)(lambda: send_aid(2))

    def absorb():
        wait_for(stage.at[2, pl.ds(0, UPPER)], aid_sem)
        sums[2] = jnp.zeros_like(sums[2])

        def turn(v, carry):
            for step in range(3):
                row, col = unit(v, step)
                val = stage[2, slot_of(row, col)]
                put(buf_b, row, col, val, False)
                sums[2] += fold(val * get(buf_a, row, col)) * jnp.where(row == col, 1.0, 2.0)
            return carry

        lax.fori_loop(0, 7, turn, 0)

    def coefs():
        t1, t2, t3 = total(sums[0]), total(sums[1]), total(sums[2])
        coef = (t2 - t3) / (t1 - t2)
        inv = 1.0 / (1.0 - coef)
        return (1.0 - 2.0 * coef) * inv, (1.0 + coef) * inv, inv

    def count(val, diag):
        if diag:
            sums[0] += fold(val * eye)
        sums[1] += fold(val * val) * (1.0 if diag else 2.0)

    def combine(src, row, col, co):
        acc = chain(buf_b, src, row, col, PASSES)
        return co[0] * get(src, row, col) + co[1] * get(buf_b, row, col) - co[2] * acc

    def cube(src, dst, job, before):
        co = coefs()
        sums[0:2] = jnp.zeros_like(sums[0:2])

        def turn(v, carry):
            relay_early(job, before + v)
            for row, col, diag in tiles_of(v):
                val = combine(src, row, col, co)
                put(dst, row, col, val, diag)
                count(val, diag)
            return carry

        lax.fori_loop(0, 3, turn, 0)

    def cube_last(src, rnd):
        co = coefs()
        sums[0] = jnp.zeros_like(sums[0])

        def turn(v, carry):
            @pl.when(v > 0)
            def _():
                for step in range(3):
                    send_out(rnd, *unit(v - 1, step))

            for step in range(3):
                row, col = unit(v, step)
                val = combine(src, row, col, co)
                slot = slot_of(row, col)
                weight = jnp.where(row == col, 1.0, 2.0)
                sums[0] += fold(val * stage[rnd, slot]) * weight
                stage[rnd, slot] = val
            return carry

        lax.fori_loop(0, 7, turn, 0)
        for step in range(3):
            send_out(rnd, *unit(6, step))

    def one_job(job, carry):
        pl.when((job > 0) | (c == 1))(lambda: run_job(job))
        return carry

    def run_job(job):
        own_job = (job + 1) // 2
        rnd = job - 1
        put_in = (job + 2) % 3
        mat = own_job * (rnd * 8 + own) + (1 - own_job) * (8 + own - 1)
        wait_for(stage.at[put_in, pl.ds(0, 15)], so_sem.at[put_in])
        wait_for(stage.at[put_in, pl.ds(15, 6), pl.ds(0, tile * 7 // 8)], r_sem.at[put_in])
        half = tile // 2
        for i in range(G, NB):
            slot = slot_of(i, i)
            stage[put_in, slot, half:, :half] = stage[put_in, slot, :half, half:].T
        diag_sum = fold(stage[put_in, slot_of(0, 0)] * eye)
        for i in range(1, NB):
            diag_sum += fold(stage[put_in, slot_of(i, i)] * eye)
        mean = total(diag_sum) / order
        filled = occ[mat].astype(F32)
        scale = jnp.minimum(
            filled / (bounds[1, mat] - mean), (order - filled) / (mean - bounds[0, mat])
        )
        on_diag = (scale * mean + filled) / order
        slope = scale / order
        sums[0:2] = jnp.zeros_like(sums[0:2])

        def first(v, c_):
            for step in range(3):
                row, col = unit(v, step)
                one = jnp.where(row == col, 1.0, 0.0)
                val = stage[put_in, slot_of(row, col)] * -slope + (on_diag * one) * eye
                put(buf_a, row, col, val, False)
                sums[0] += fold(val * eye) * one
                sums[1] += fold(val * val) * (2.0 - one)
            return c_

        lax.fori_loop(0, 7, first, 0)
        given = (job == 2) & (c == 0)
        mine = job > 0

        def step(s, c_):
            @pl.when(((s == 0) & ~given) | ((s == 2) & mine))
            def _():
                square(buf_a, job, 6 * s, True)

            pl.when((s == 0) & given)(absorb)
            pl.when((s == 1) & mine)(lambda: square(buf_c, job, 6, False))
            pl.when((s == 0) & mine)(lambda: cube(buf_a, buf_c, job, 3))
            pl.when((s == 1) & mine)(lambda: cube(buf_c, buf_a, job, 9))
            pl.when((s == 2) & mine)(lambda: finish(rnd, mat))
            return c_

        lax.fori_loop(0, STEPS, step, 0)

    def finish(rnd, mat):
        cube_last(buf_a, rnd)
        e_vec[rnd] = jnp.broadcast_to(2.0 * total(sums[0]), e_vec.shape[1:])
        for k in range(1, 8):
            pltpu.make_async_remote_copy(
                e_vec.at[rnd], ener.at[mat], e_send, e_sem,
                device_id=device(flip(y, k // 4), flip(x, (k // 2) % 2), flip(c, k % 2)),
                device_id_type=MESH,
            ).start()
        pltpu.make_async_copy(e_vec.at[rnd], ener.at[mat], e_sem).start()

    lax.fori_loop(0, 3, one_job, 0)

    def relay_late(place, carry):
        relay(1, place)
        return carry

    lax.fori_loop(0, G * G, relay_late, 0)
    wait_for(ener.at[pl.ds(0, 14)], e_send)
    wait_for(ener, e_sem)

    def wait_tiles(quarters, sem):
        lead = 8 if quarters <= 288 else 16
        wait_for(ham.at[pl.ds(0, lead), pl.ds(0, quarters * tile // (12 * lead)), :], sem)

    @pl.when(c == 1)
    def _():
        wait_for(stage.at[2, pl.ds(0, UPPER)], aid_send)

    @pl.when(differ == 0)
    def _():
        pl.when(c == 0)(lambda: wait_tiles(105 + 72, in_send))
        pl.when(c == 1)(lambda: wait_tiles(105 + 48, in_send))
        wait_tiles(4 * 96, out_send)
        wait_tiles(4 * 63, land_sem)

    @pl.when(differ == 1)
    def _():
        pl.when(c == 0)(lambda: wait_tiles(108, in_send))
        pl.when(c == 1)(lambda: wait_tiles(72, in_send))
        wait_tiles(414, out_send)
        wait_tiles(4 * 108, land_sem)


PER = 2


def unpack_kernel(in0, in1, in2, out):
    tile = in0.shape[2]
    half = tile // 2
    x, c = lax.axis_index('row'), lax.axis_index('col')
    differ = flip(x, c)
    tiles = [ref.at[0, k] for ref in (in0, in1, in2) for k in range(3 * PER)]

    for sub in range(PER):
        mat = pl.program_id(0) * PER + sub
        turned = flip((mat // 2) % 2, x)

        def write(i, j, val):
            rows, cols = val.shape
            out[sub, pl.ds(i * half, rows), pl.ds(j * half, cols)] = val

        @pl.when(differ == 0)
        def _():
            for i in range(G):
                for j in range(i, G):
                    ref = tiles[UPPER3 * sub + slot3_of(i, j)]
                    if i == j:
                        top = ref[:half, :]
                        write(2 * i, 2 * i, top)
                        write(2 * i + 1, 2 * i, top[:, half:].T)
                        write(2 * i + 1, 2 * i + 1, ref[half:, half:])
                    else:
                        val = ref[...]
                        write(2 * i, 2 * j, val)
                        write(2 * j, 2 * i, val.T)

        @pl.when(differ * (1 - turned) == 1)
        def _():
            for i in range(G):
                for j in range(G):
                    write(2 * i, 2 * j, tiles[G * G * sub + i * G + j][...])

        @pl.when(differ * turned == 1)
        def _():
            for i in range(G):
                for j in range(G):
                    write(2 * j, 2 * i, tiles[G * G * sub + i * G + j][...].T)


def solution(mesh):
    def local_purify(ham, bounds, occ):
        mats, blk, _ = ham.shape
        tile = blk // G
        any_spec = pl.BlockSpec(memory_space=pltpu.HBM)
        smem = pl.BlockSpec(memory_space=pltpu.SMEM)
        limb = pltpu.VMEM((3, NB, NB, tile, tile), BF16)
        flops = 2 * 6 * 21 * 36 * 2 * tile**3
        land, ener = pl.pallas_call(
            main_kernel,
            out_shape=(
                jax.ShapeDtypeStruct((mats * G * G, tile, tile), F32),
                jax.ShapeDtypeStruct((mats, 8, 128), F32),
            ),
            in_specs=[smem, smem, any_spec],
            out_specs=(any_spec, any_spec),
            scratch_shapes=[
                limb, limb, limb,
                pltpu.VMEM((3, UPPER + 1, tile, tile), F32),
                pltpu.VMEM((3, 8, tile), F32),
                pltpu.VMEM((2, 8, 128), F32),
                pltpu.SemaphoreType.DMA((3,)),
                pltpu.SemaphoreType.DMA((3,)),
                pltpu.SemaphoreType.DMA,
                pltpu.SemaphoreType.DMA,
                pltpu.SemaphoreType.DMA,
                pltpu.SemaphoreType.DMA,
                pltpu.SemaphoreType.DMA((2, 2, G * G)),
                pltpu.SemaphoreType.DMA,
                pltpu.SemaphoreType.DMA,
                pltpu.SemaphoreType.DMA,
            ],
            compiler_params=pltpu.CompilerParams(
                collective_id=0, has_side_effects=True, vmem_limit_bytes=67043328
            ),
            cost_estimate=pl.CostEstimate(flops=flops, bytes_accessed=120 * 2**20, transcendentals=0),
            name='purify',
        )(bounds.T, occ, ham)

        quads = land.reshape(mats * G // PER, G * PER, tile, tile)

        def part(k):
            def index(m):
                off = flip(lax.axis_index('row'), lax.axis_index('col'))
                last = 0 if k == 2 else 2 * m + k
                return off * (3 * m + k) + (1 - off) * last, 0, 0, 0

            return pl.BlockSpec((1, G * PER, tile, tile), index)

        density = pl.pallas_call(
            unpack_kernel,
            out_shape=jax.ShapeDtypeStruct(ham.shape, F32),
            grid=(mats // PER,),
            in_specs=[part(0), part(1), part(2)],
            out_specs=pl.BlockSpec((PER, blk, blk), lambda m: (m, 0, 0)),
            compiler_params=pltpu.CompilerParams(vmem_limit_bytes=40 * 2**20),
            cost_estimate=pl.CostEstimate(flops=10**6, bytes_accessed=75 * 2**20, transcendentals=0),
            name='unpack',
        )(quads, quads, quads)
        return density, ener[:, 0, 0]

    mat_spec = P('spin', 'row', 'col')
    return jax.shard_map(
        local_purify, mesh=mesh,
        in_specs=(mat_spec, P('spin', None), P('spin')),
        out_specs=(mat_spec, P('spin')), check_vma=False,
    )
```

```python
import functools

import jax
import jax.numpy as jnp
from jax import lax
from jax.experimental import pallas as pl
from jax.experimental.pallas import tpu as pltpu
from jax.sharding import PartitionSpec as P

STEPS = 3
G = 3
NB = 2 * G
UPPER = NB * (NB + 1) // 2
UPPER3 = G * (G + 1) // 2
OVER_X = 7
F32 = jnp.float32
BF16 = jnp.bfloat16
PASSES = ((0, 2), (2, 0), (1, 1), (0, 1), (1, 0), (0, 0))
MESH = pl.DeviceIdType.MESH


def slot_of(row, col):
    return row * (2 * NB - 1 - row) // 2 + col


def slot3_of(row, col):
    return row * (2 * G - 1 - row) // 2 + col


def upper_tile(row, step):
    wrap = (row + step) // NB
    other = row + step - NB * wrap
    return row * (1 - wrap) + other * wrap, other * (1 - wrap) + row * wrap


def limbs(val):
    high = val.astype(BF16)
    rest = val - high.astype(F32)
    mid = rest.astype(BF16)
    low = (rest - mid.astype(F32)).astype(BF16)
    return high, mid, low


def put(ref, row, col, val, diag):
    for piece, part in enumerate(limbs(val)):
        ref[piece, row, col] = part
    if not diag:
        for piece, part in enumerate(limbs(val.T)):
            ref[piece, col, row] = part


def get(ref, row, col):
    low = ref[1, row, col].astype(F32) + ref[2, row, col].astype(F32)
    return ref[0, row, col].astype(F32) + low


def chain(left, right, row, col, passes):
    acc = None
    for k in range(NB):
        for p, q in passes:
            part = jnp.dot(left[p, row, k], right[q, k, col], preferred_element_type=F32)
            acc = part if acc is None else acc + part
    return acc


def fold(val):
    size = val.shape[0]
    return jnp.sum(val.reshape(size // 8, 8, val.shape[1]), axis=0)


def total(val):
    return jnp.sum(jnp.sum(val, axis=0, keepdims=True), axis=1, keepdims=True)


def flip(bit, by):
    return bit + by - 2 * bit * by


def main_kernel(
    bounds, occ, ham, land, ener,
    buf_a, buf_b, buf_c, stage, sums, e_vec,
    so_sem, r_sem, in_send, aid_sem, aid_send, land_sem, relay_sem, out_send, e_sem, e_send,
):
    tile = stage.shape[2]
    order = NB * tile
    y, x, c = lax.axis_index('depth'), lax.axis_index('row'), lax.axis_index('col')
    own = y * 4 + x * 2 + c
    differ = flip(x, c)

    def device(dy, dx, cd):
        return {'depth': dy, 'row': dx, 'col': cd}

    barrier = pltpu.get_barrier_semaphore()
    for k in range(1, 8):
        pl.semaphore_signal(
            barrier, inc=1,
            device_id=device(flip(y, k // 4), flip(x, (k // 2) % 2), flip(c, k % 2)),
            device_id_type=MESH,
        )
    pl.semaphore_wait(barrier, 7)

    def h_tile(mat, i, j):
        return ham.at[mat, pl.ds(i * tile, tile), pl.ds(j * tile, tile)]

    def parts(diag):
        half = tile // 2
        if not diag:
            return [(slice(None), slice(None))]
        return [(pl.ds(0, half), slice(None)), (pl.ds(half, half), pl.ds(half, half))]

    diag_tiles = [(i, j) for i in range(G) for j in range(i, G)]

    def send_in(e, carry):
        late = e // 3
        aid = (e % 3) % 2 * (1 - late)
        cd = (1 - late) * ((e + 1) // 2) + late * (e - 3)
        mat = 8 * (aid + late) + cd * (1 - aid) + y * 4
        put_in = 2 * aid + late

        @pl.when(differ == 0)
        def _():
            for i, j in diag_tiles:
                for part in parts(i == j):
                    pltpu.make_async_remote_copy(
                        h_tile(mat + (1 - x) * 2, i, j).at[part],
                        stage.at[put_in, slot_of(G + i, G + j)].at[part],
                        in_send, r_sem.at[put_in],
                        device_id=device(y, 1 - x, cd), device_id_type=MESH,
                    ).start()

        def near(tiles, shift):
            for i, j in tiles:
                near_tile(i, j, shift)

        def near_row(i, carry_):
            for j in range(G):
                near_tile(i, j, G)
            return carry_

        def near_tile(i, j, shift):
            src = h_tile(mat + x * 2, i, j)
            dst = stage.at[put_in, slot_of(i, shift + j)]

            @pl.when(cd == c)
            def _():
                pltpu.make_async_copy(src, dst, so_sem.at[put_in]).start()

            @pl.when(cd != c)
            def _():
                pltpu.make_async_remote_copy(
                    src, dst, in_send, so_sem.at[put_in],
                    device_id=device(y, x, cd), device_id_type=MESH,
                ).start()

        pl.when(differ == 0)(lambda: near(diag_tiles, 0))

        @pl.when(differ == 1)
        def _():
            lax.fori_loop(0, G, near_row, 0)

        return carry

    lax.fori_loop(0, 5, send_in, 0)

    def wait_for(ref, sem):
        pltpu.make_async_copy(ref, ref, sem).wait()

    rows = lax.broadcasted_iota(jnp.int32, (tile, tile), 0)
    cols = lax.broadcasted_iota(jnp.int32, (tile, tile), 1)
    eye = jnp.where(rows == cols, 1.0, 0.0).astype(F32)

    def send_out(rnd, row, col):
        mat = rnd * 8 + own
        src = stage.at[rnd, slot_of(row, col)]
        k_row, k_col = row // G, col // G

        def start(dy, xd, cd, dst, sem, diag=False):
            for part in parts(diag):
                pltpu.make_async_remote_copy(
                    src.at[part], dst.at[part], out_send, sem,
                    device_id=device(flip(y, dy), xd, cd), device_id_type=MESH,
                ).start()

        def keep(dst, diag=False):
            for part in parts(diag):
                pltpu.make_async_copy(src.at[part], dst.at[part], land_sem).start()

        @pl.when(k_row + k_col == 1)
        def _():
            place = row * G + col - G
            dst = land.at[mat * 9 + place]
            sem = relay_sem.at[rnd, c, place]

            @pl.when(place < OVER_X)
            def _():
                start(1, x, 1 - x, dst, sem)
                start(0, 1 - x, x, dst, land_sem)

            @pl.when(place >= OVER_X)
            def _():
                start(0, 1 - x, x, dst, sem)
                start(1, x, 1 - x, dst, land_sem)

            pl.when(differ == 1)(lambda: keep(dst))
            pl.when(differ == 0)(lambda: start(0, x, 1 - x, dst, land_sem))

        for diag in (False, True):
            same = (row == col) if diag else (row != col)

            @pl.when((k_row == 1) & same)
            def _():
                place = slot3_of(row - G, col - G)
                start(0, 1 - x, 1 - x, land.at[mat * 6 + place], relay_sem.at[rnd, c, place], diag)

            @pl.when((k_col == 0) & same)
            def _():
                dst = land.at[mat * 6 + slot3_of(row, col)]
                start(1, x, x, dst, land_sem, diag)
                pl.when(differ == 0)(lambda: keep(dst, diag))
                pl.when(differ == 1)(lambda: start(0, x, x, dst, land_sem, diag))

    def relay(rnd, cd, place):
        over_x = differ * (1 - place // OVER_X)
        owner = over_x * ((1 - y) * 4 + x * 2) + (1 - over_x) * (y * 4 + (1 - x) * 2) + cd
        dev = device(flip(y, 1 - over_x), flip(x, over_x), over_x * x + (1 - over_x) * c)
        tile_ref = land.at[(rnd * 8 + owner) * (UPPER3 + 3 * differ) + place]

        def pass_on(whole, diag):
            wait_for(whole, relay_sem.at[rnd, cd, place])
            for part in parts(diag):
                pltpu.make_async_remote_copy(
                    tile_ref.at[part], tile_ref.at[part], out_send, land_sem,
                    device_id=dev, device_id_type=MESH,
                ).start()

        on_diag = (differ == 0) & ((place == 0) | (place == 3) | (place == 5))
        pl.when(on_diag)(lambda: pass_on(tile_ref.at[pl.ds(0, tile * 3 // 4)], True))
        pl.when(~on_diag & (place < UPPER3 + 3 * differ))(lambda: pass_on(tile_ref, False))

    def relays(rnd, cd, low, count):
        def body(k, carry):
            relay(rnd, cd, low + k)
            return carry

        lax.fori_loop(0, count, body, 0)

    def relay_early(job, turn):
        one = (c == 1) & (turn >= 1) & (turn < 1 + G * G)
        two = (c == 0) & (turn >= 9) & (turn < 14)

        @pl.when((job == 2) & (one | two))
        def _():
            low = c * (turn - 1) + (1 - c) * 2 * (turn - 9)
            count = 1 + (1 - c) * (1 - turn // 13)

            def body(k, carry):
                relay(0, k % 2, low + k // 2)
                return carry

            lax.fori_loop(0, 2 * count, body, 0)

        @pl.when((job == 2) & (c == 1) & (turn >= 12))
        def _():
            later = (turn - 11) // 2
            low = differ * later * (2 * turn - 23)
            relays(1, 0, low, differ * (3 - later) + (1 - differ) * (turn // 14))

    def relay_last(rnd, v):
        @pl.when((rnd == 1) & (c == 1) & (v >= 1) & (v < UPPER3 - 3 * differ))
        def _():
            relays(1, 0, v + 6 * differ, 1)

    def tiles_of(turn):
        out = []
        for half in range(2):
            row = turn * 2 + half
            for step in range(3):
                out.append((*upper_tile(row, step), step == 0))
        out.append((turn, turn + 3, False))
        return out

    def unit(v, step):
        late = (v + 3) // 6
        half = (v - 3) % 2
        base = G * (1 - (v - 3) // 2)
        row = base + half * (1 + step // 2)
        col = base + (1 - half) * step + half * (1 + (step + 1) // 2)
        return row * late + v * (1 - late), col * late + (G + step) * (1 - late)

    def send_aid(v):
        for row, col, _ in tiles_of(v):
            ref = stage.at[2, slot_of(row, col)]
            pltpu.make_async_remote_copy(
                ref, ref, aid_send, aid_sem, device_id=device(y, x, 0), device_id_type=MESH
            ).start()

    def square(src, job, before, may_aid):
        own_job = (job + 1) // 2

        def turn(v, carry):
            relay_early(job, before + v)
            if may_aid:
                pl.when((job == 0) & (v > 0))(lambda: send_aid(v - 1))
            for row, col, diag in tiles_of(v):
                if diag:
                    cross = chain(src, src, row, col, ((0, 2), (0, 1)))
                    val = chain(src, src, row, col, ((1, 1), (0, 0)))
                    val = val + (cross + cross.T)
                else:
                    val = chain(src, src, row, col, PASSES)
                put(buf_b, row, col, val, diag)
                if may_aid:
                    stage[2, slot_of(row, col) * (1 - own_job) + UPPER * own_job] = val
                sums[2] += fold(val * get(src, row, col)) * (1.0 if diag else 2.0)
            return carry

        sums[2] = jnp.zeros_like(sums[2])
        lax.fori_loop(0, 3, turn, 0)
        if may_aid:
            pl.when(job == 0)(lambda: send_aid(2))

    def absorb():
        wait_for(stage.at[2, pl.ds(0, UPPER)], aid_sem)
        sums[2] = jnp.zeros_like(sums[2])

        def turn(v, carry):
            for step in range(3):
                row, col = unit(v, step)
                val = stage[2, slot_of(row, col)]
                put(buf_b, row, col, val, False)
                sums[2] += fold(val * get(buf_a, row, col)) * jnp.where(row == col, 1.0, 2.0)
            return carry

        lax.fori_loop(0, 7, turn, 0)

    def coefs():
        t1, t2, t3 = total(sums[0]), total(sums[1]), total(sums[2])
        coef = (t2 - t3) / (t1 - t2)
        inv = 1.0 / (1.0 - coef)
        return (1.0 - 2.0 * coef) * inv, (1.0 + coef) * inv, inv

    def count(val, diag):
        if diag:
            sums[0] += fold(val * eye)
        sums[1] += fold(val * val) * (1.0 if diag else 2.0)

    def combine(src, row, col, co):
        acc = chain(buf_b, src, row, col, PASSES)
        return co[0] * get(src, row, col) + co[1] * get(buf_b, row, col) - co[2] * acc

    def cube(src, dst, job, before):
        co = coefs()
        sums[0:2] = jnp.zeros_like(sums[0:2])

        def turn(v, carry):
            relay_early(job, before + v)
            for row, col, diag in tiles_of(v):
                val = combine(src, row, col, co)
                put(dst, row, col, val, diag)
                count(val, diag)
            return carry

        lax.fori_loop(0, 3, turn, 0)

    def cube_last(src, rnd):
        co = coefs()
        sums[0] = jnp.zeros_like(sums[0])

        def turn(v, carry):
            @pl.when(v > 0)
            def _():
                for step in range(3):
                    send_out(rnd, *unit(v - 1, step))

            relay_last(rnd, v)

            for step in range(3):
                row, col = unit(v, step)
                val = combine(src, row, col, co)
                slot = slot_of(row, col)
                weight = jnp.where(row == col, 1.0, 2.0)
                sums[0] += fold(val * stage[rnd, slot]) * weight
                stage[rnd, slot] = val
            return carry

        lax.fori_loop(0, 7, turn, 0)
        for step in range(3):
            send_out(rnd, *unit(6, step))

    def one_job(job, carry):
        pl.when((job > 0) | (c == 1))(lambda: run_job(job))
        return carry

    def run_job(job):
        own_job = (job + 1) // 2
        rnd = job - 1
        put_in = (job + 2) % 3
        mat = own_job * (rnd * 8 + own) + (1 - own_job) * (8 + own - 1)
        wait_for(stage.at[put_in, pl.ds(0, 15)], so_sem.at[put_in])
        wait_for(stage.at[put_in, pl.ds(15, 6), pl.ds(0, tile * 7 // 8)], r_sem.at[put_in])
        half = tile // 2
        for i in range(G, NB):
            slot = slot_of(i, i)
            stage[put_in, slot, half:, :half] = stage[put_in, slot, :half, half:].T
        diag_sum = fold(stage[put_in, slot_of(0, 0)] * eye)
        for i in range(1, NB):
            diag_sum += fold(stage[put_in, slot_of(i, i)] * eye)
        mean = total(diag_sum) / order
        filled = occ[mat].astype(F32)
        scale = jnp.minimum(
            filled / (bounds[1, mat] - mean), (order - filled) / (mean - bounds[0, mat])
        )
        on_diag = (scale * mean + filled) / order
        slope = scale / order
        sums[0:2] = jnp.zeros_like(sums[0:2])

        def first(v, c_):
            for step in range(3):
                row, col = unit(v, step)
                one = jnp.where(row == col, 1.0, 0.0)
                val = stage[put_in, slot_of(row, col)] * -slope + (on_diag * one) * eye
                put(buf_a, row, col, val, False)
                sums[0] += fold(val * eye) * one
                sums[1] += fold(val * val) * (2.0 - one)
            return c_

        lax.fori_loop(0, 7, first, 0)
        given = (job == 2) & (c == 0)
        mine = job > 0

        def step(s, c_):
            @pl.when(((s == 0) & ~given) | ((s == 2) & mine))
            def _():
                square(buf_a, job, 6 * s, True)

            pl.when((s == 0) & given)(absorb)
            pl.when((s == 1) & mine)(lambda: square(buf_c, job, 6, False))
            pl.when((s == 0) & mine)(lambda: cube(buf_a, buf_c, job, 3))
            pl.when((s == 1) & mine)(lambda: cube(buf_c, buf_a, job, 9))
            pl.when((s == 2) & mine)(lambda: finish(rnd, mat))
            return c_

        lax.fori_loop(0, STEPS, step, 0)

    def finish(rnd, mat):
        cube_last(buf_a, rnd)
        lane = lax.broadcasted_iota(jnp.int32, e_vec.shape[1:], 1)
        e_vec[rnd] = jnp.where(lane == mat, 2.0 * total(sums[0]), 0.0)
        for k in range(1, 8):
            pltpu.make_async_remote_copy(
                e_vec.at[rnd], ener.at[mat], e_send, e_sem,
                device_id=device(flip(y, k // 4), flip(x, (k // 2) % 2), flip(c, k % 2)),
                device_id_type=MESH,
            ).start()
        pltpu.make_async_copy(e_vec.at[rnd], ener.at[mat], e_sem).start()

    lax.fori_loop(0, 3, one_job, 0)

    pl.when(c == 0)(lambda: relays(1, 0, 0, G * G))
    relays(1, 1, 0, G * G)
    wait_for(ener.at[pl.ds(0, 14)], e_send)
    wait_for(ener, e_sem)

    def wait_tiles(quarters, sem):
        lead = 8 if quarters <= 288 else 16
        wait_for(ham.at[pl.ds(0, lead), pl.ds(0, quarters * tile // (12 * lead)), :], sem)

    @pl.when(c == 1)
    def _():
        wait_for(stage.at[2, pl.ds(0, UPPER)], aid_send)

    @pl.when(differ == 0)
    def _():
        pl.when(c == 0)(lambda: wait_tiles(105 + 72, in_send))
        pl.when(c == 1)(lambda: wait_tiles(105 + 48, in_send))
        wait_tiles(4 * 96, out_send)
        wait_tiles(4 * 63, land_sem)

    @pl.when(differ == 1)
    def _():
        pl.when(c == 0)(lambda: wait_tiles(108, in_send))
        pl.when(c == 1)(lambda: wait_tiles(72, in_send))
        wait_tiles(414, out_send)
        wait_tiles(4 * 108, land_sem)


RING = 4


def unpack_kernel(land, ener, out, energy, held, block, in_sem, out_sem):
    mats, tile = out.shape[0], land.shape[1]
    half = tile // 2
    x, c = lax.axis_index('row'), lax.axis_index('col')
    differ = flip(x, c)

    def load(mat, act):
        slot = mat % RING
        for kind, count in ((0, UPPER3), (1, G * G)):

            @pl.when(differ == kind)
            def _():
                act(
                    pltpu.make_async_copy(
                        land.at[pl.ds(mat * count, count)],
                        held.at[slot, pl.ds(0, count)],
                        in_sem.at[slot],
                    )
                )

    def store(mat):
        slot = mat % RING
        return pltpu.make_async_copy(block.at[slot], out.at[mat], out_sem.at[slot])

    def prime(mat, carry):
        load(mat, lambda copy: copy.start())
        return carry

    lax.fori_loop(0, RING, prime, 0)
    energy[...] = jnp.sum(ener[...], axis=0)[0, : energy.shape[0]]

    def turn(mat, carry):
        slot = mat % RING
        turned = flip((mat // 2) % 2, x)
        load(mat, lambda copy: copy.wait())
        pl.when(mat >= RING)(lambda: store(mat - RING).wait())

        def write(i, j, val):
            rows, cols = val.shape
            block[slot, pl.ds(i * half, rows), pl.ds(j * half, cols)] = val

        @pl.when(differ == 0)
        def _():
            for i in range(G):
                for j in range(i, G):
                    place = slot3_of(i, j)
                    if i == j:
                        top = held[slot, place, :half, :]
                        write(2 * i, 2 * i, top)
                        write(2 * i + 1, 2 * i, top[:, half:].T)
                        write(2 * i + 1, 2 * i + 1, held[slot, place, half:, half:])
                    else:
                        val = held[slot, place]
                        write(2 * i, 2 * j, val)
                        write(2 * j, 2 * i, val.T)

        @pl.when(differ * (1 - turned) == 1)
        def _():
            for i in range(G):
                for j in range(G):
                    write(2 * i, 2 * j, held[slot, i * G + j])

        @pl.when(differ * turned == 1)
        def _():
            for i in range(G):
                for j in range(G):
                    write(2 * j, 2 * i, held[slot, i * G + j].T)

        store(mat).start()
        pl.when(mat + RING < mats)(lambda: load(mat + RING, lambda copy: copy.start()))
        return carry

    lax.fori_loop(0, mats, turn, 0)
    for mat in range(mats - RING, mats):
        store(mat).wait()


def solution(mesh):
    def local_purify(ham, bounds, occ):
        mats, blk, _ = ham.shape
        tile = blk // G
        any_spec = pl.BlockSpec(memory_space=pltpu.HBM)
        smem = pl.BlockSpec(memory_space=pltpu.SMEM)
        limb = pltpu.VMEM((3, NB, NB, tile, tile), BF16)
        flops = 2 * 6 * 21 * 36 * 2 * tile**3
        land, ener = pl.pallas_call(
            main_kernel,
            out_shape=(
                jax.ShapeDtypeStruct((mats * G * G, tile, tile), F32),
                jax.ShapeDtypeStruct((mats, 8, 128), F32),
            ),
            in_specs=[smem, smem, any_spec],
            out_specs=(any_spec, any_spec),
            scratch_shapes=[
                limb, limb, limb,
                pltpu.VMEM((3, UPPER + 1, tile, tile), F32),
                pltpu.VMEM((3, 8, tile), F32),
                pltpu.VMEM((2, 8, 128), F32),
                pltpu.SemaphoreType.DMA((3,)),
                pltpu.SemaphoreType.DMA((3,)),
                pltpu.SemaphoreType.DMA,
                pltpu.SemaphoreType.DMA,
                pltpu.SemaphoreType.DMA,
                pltpu.SemaphoreType.DMA,
                pltpu.SemaphoreType.DMA((2, 2, G * G)),
                pltpu.SemaphoreType.DMA,
                pltpu.SemaphoreType.DMA,
                pltpu.SemaphoreType.DMA,
            ],
            compiler_params=pltpu.CompilerParams(
                collective_id=0, has_side_effects=True, vmem_limit_bytes=67043328
            ),
            cost_estimate=pl.CostEstimate(flops=flops, bytes_accessed=120 * 2**20, transcendentals=0),
            name='purify',
        )(bounds.T, occ, ham)

        return pl.pallas_call(
            unpack_kernel,
            out_shape=(
                jax.ShapeDtypeStruct(ham.shape, F32),
                jax.ShapeDtypeStruct((mats,), F32),
            ),
            in_specs=[any_spec, pl.BlockSpec(memory_space=pltpu.VMEM)],
            out_specs=(any_spec, pl.BlockSpec(memory_space=pltpu.VMEM)),
            scratch_shapes=[
                pltpu.VMEM((RING, G * G, tile, tile), F32),
                pltpu.VMEM((RING, blk, blk), F32),
                pltpu.SemaphoreType.DMA((RING,)),
                pltpu.SemaphoreType.DMA((RING,)),
            ],
            compiler_params=pltpu.CompilerParams(vmem_limit_bytes=40 * 2**20),
            cost_estimate=pl.CostEstimate(flops=10**6, bytes_accessed=75 * 2**20, transcendentals=0),
            name='unpack',
        )(land, ener)

    mat_spec = P('spin', 'row', 'col')
    return jax.shard_map(
        local_purify, mesh=mesh,
        in_specs=(mat_spec, P('spin', None), P('spin')),
        out_specs=(mat_spec, P('spin')), check_vma=False,
    )
```

```python
import functools

import jax
import jax.numpy as jnp
from jax import lax
from jax.experimental import pallas as pl
from jax.experimental.pallas import tpu as pltpu
from jax.sharding import PartitionSpec as P

STEPS = 3
G = 3
NB = 2 * G
UPPER = NB * (NB + 1) // 2
UPPER3 = G * (G + 1) // 2
OVER_X = 8
F32 = jnp.float32
BF16 = jnp.bfloat16
PASSES = ((0, 2), (2, 0), (1, 1), (0, 1), (1, 0), (0, 0))
MESH = pl.DeviceIdType.MESH


def slot_of(row, col):
    return row * (2 * NB - 1 - row) // 2 + col


def slot3_of(row, col):
    return row * (2 * G - 1 - row) // 2 + col


def upper_tile(row, step):
    wrap = (row + step) // NB
    other = row + step - NB * wrap
    return row * (1 - wrap) + other * wrap, other * (1 - wrap) + row * wrap


def limbs(val):
    high = val.astype(BF16)
    rest = val - high.astype(F32)
    mid = rest.astype(BF16)
    low = (rest - mid.astype(F32)).astype(BF16)
    return high, mid, low


def put(ref, row, col, val, diag):
    for piece, part in enumerate(limbs(val)):
        ref[piece, row, col] = part
    if not diag:
        for piece, part in enumerate(limbs(val.T)):
            ref[piece, col, row] = part


def get(ref, row, col):
    low = ref[1, row, col].astype(F32) + ref[2, row, col].astype(F32)
    return ref[0, row, col].astype(F32) + low


def chain(left, right, row, col, passes):
    acc = None
    for k in range(NB):
        for p, q in passes:
            part = jnp.dot(left[p, row, k], right[q, k, col], preferred_element_type=F32)
            acc = part if acc is None else acc + part
    return acc


def fold(val):
    size = val.shape[0]
    return jnp.sum(val.reshape(size // 8, 8, val.shape[1]), axis=0)


def total(val):
    return jnp.sum(jnp.sum(val, axis=0, keepdims=True), axis=1, keepdims=True)


def flip(bit, by):
    return bit + by - 2 * bit * by


def main_kernel(
    bounds, occ, ham, land, ener,
    buf_a, buf_b, buf_c, stage, sums, e_vec,
    so_sem, r_sem, in_send, aid_sem, aid_send, land_sem, relay_sem, out_send, e_sem, e_send,
):
    tile = stage.shape[2]
    order = NB * tile
    y, x, c = lax.axis_index('depth'), lax.axis_index('row'), lax.axis_index('col')
    own = y * 4 + x * 2 + c
    differ = flip(x, c)

    def device(dy, dx, cd):
        return {'depth': dy, 'row': dx, 'col': cd}

    barrier = pltpu.get_barrier_semaphore()
    for k in range(1, 8):
        pl.semaphore_signal(
            barrier, inc=1,
            device_id=device(flip(y, k // 4), flip(x, (k // 2) % 2), flip(c, k % 2)),
            device_id_type=MESH,
        )
    pl.semaphore_wait(barrier, 7)

    def h_tile(mat, i, j):
        return ham.at[mat, pl.ds(i * tile, tile), pl.ds(j * tile, tile)]

    def parts(diag):
        half = tile // 2
        if not diag:
            return [(slice(None), slice(None))]
        return [(pl.ds(0, half), slice(None)), (pl.ds(half, half), pl.ds(half, half))]

    diag_tiles = [(i, j) for i in range(G) for j in range(i, G)]

    def send_in(e, carry):
        late = e // 3
        aid = (e % 3) % 2 * (1 - late)
        cd = (1 - late) * ((e + 1) // 2) + late * (e - 3)
        mat = 8 * (aid + late) + cd * (1 - aid) + y * 4
        put_in = 2 * aid + late

        @pl.when(differ == 0)
        def _():
            for i, j in diag_tiles:
                for part in parts(i == j):
                    pltpu.make_async_remote_copy(
                        h_tile(mat + (1 - x) * 2, i, j).at[part],
                        stage.at[put_in, slot_of(G + i, G + j)].at[part],
                        in_send, r_sem.at[put_in],
                        device_id=device(y, 1 - x, cd), device_id_type=MESH,
                    ).start()

        def near(tiles, shift):
            for i, j in tiles:
                near_tile(i, j, shift)

        def near_row(i, carry_):
            for j in range(G):
                near_tile(i, j, G)
            return carry_

        def near_tile(i, j, shift):
            src = h_tile(mat + x * 2, i, j)
            dst = stage.at[put_in, slot_of(i, shift + j)]

            @pl.when(cd == c)
            def _():
                pltpu.make_async_copy(src, dst, so_sem.at[put_in]).start()

            @pl.when(cd != c)
            def _():
                pltpu.make_async_remote_copy(
                    src, dst, in_send, so_sem.at[put_in],
                    device_id=device(y, x, cd), device_id_type=MESH,
                ).start()

        pl.when(differ == 0)(lambda: near(diag_tiles, 0))

        @pl.when(differ == 1)
        def _():
            lax.fori_loop(0, G, near_row, 0)

        return carry

    lax.fori_loop(0, 5, send_in, 0)

    def wait_for(ref, sem):
        pltpu.make_async_copy(ref, ref, sem).wait()

    rows = lax.broadcasted_iota(jnp.int32, (tile, tile), 0)
    cols = lax.broadcasted_iota(jnp.int32, (tile, tile), 1)
    eye = jnp.where(rows == cols, 1.0, 0.0).astype(F32)

    def send_out(rnd, row, col):
        mat = rnd * 8 + own
        src = stage.at[rnd, slot_of(row, col)]
        k_row, k_col = row // G, col // G

        def start(dy, xd, cd, dst, sem, diag=False):
            for part in parts(diag):
                pltpu.make_async_remote_copy(
                    src.at[part], dst.at[part], out_send, sem,
                    device_id=device(flip(y, dy), xd, cd), device_id_type=MESH,
                ).start()

        def keep(dst, diag=False):
            for part in parts(diag):
                pltpu.make_async_copy(src.at[part], dst.at[part], land_sem).start()

        @pl.when(k_row + k_col == 1)
        def _():
            place = row * G + col - G
            dst = land.at[mat * 9 + place]
            sem = relay_sem.at[rnd, c, place]

            @pl.when(place < OVER_X)
            def _():
                start(1, x, 1 - x, dst, sem)
                start(0, 1 - x, x, dst, land_sem)

            @pl.when(place >= OVER_X)
            def _():
                start(0, 1 - x, x, dst, sem)
                start(1, x, 1 - x, dst, land_sem)

            pl.when(differ == 1)(lambda: keep(dst))
            pl.when(differ == 0)(lambda: start(0, x, 1 - x, dst, land_sem))

        for diag in (False, True):
            same = (row == col) if diag else (row != col)

            @pl.when((k_row == 1) & same)
            def _():
                place = slot3_of(row - G, col - G)
                start(0, 1 - x, 1 - x, land.at[mat * 6 + place], relay_sem.at[rnd, c, place], diag)

            @pl.when((k_col == 0) & same)
            def _():
                dst = land.at[mat * 6 + slot3_of(row, col)]
                start(1, x, x, dst, land_sem, diag)
                pl.when(differ == 0)(lambda: keep(dst, diag))
                pl.when(differ == 1)(lambda: start(0, x, x, dst, land_sem, diag))

    def relay(rnd, cd, place):
        over_x = differ * (1 - place // OVER_X)
        owner = over_x * ((1 - y) * 4 + x * 2) + (1 - over_x) * (y * 4 + (1 - x) * 2) + cd
        dev = device(flip(y, 1 - over_x), flip(x, over_x), over_x * x + (1 - over_x) * c)
        tile_ref = land.at[(rnd * 8 + owner) * (UPPER3 + 3 * differ) + place]

        def pass_on(whole, diag):
            wait_for(whole, relay_sem.at[rnd, cd, place])
            for part in parts(diag):
                pltpu.make_async_remote_copy(
                    tile_ref.at[part], tile_ref.at[part], out_send, land_sem,
                    device_id=dev, device_id_type=MESH,
                ).start()

        on_diag = (differ == 0) & ((place == 0) | (place == 3) | (place == 5))
        pl.when(on_diag)(lambda: pass_on(tile_ref.at[pl.ds(0, tile * 3 // 4)], True))
        pl.when(~on_diag & (place < UPPER3 + 3 * differ))(lambda: pass_on(tile_ref, False))

    def relays(rnd, cd, low, count):
        def body(k, carry):
            relay(rnd, cd, low + k)
            return carry

        lax.fori_loop(0, count, body, 0)

    def relay_early(job, turn):
        one = (c == 1) & (turn >= 1) & (turn < 1 + G * G)
        two = (c == 0) & (turn >= 9) & (turn < 14)

        @pl.when((job == 2) & (one | two))
        def _():
            low = c * (turn - 1) + (1 - c) * 2 * (turn - 9)
            count = 1 + (1 - c) * (1 - turn // 13)

            def body(k, carry):
                relay(0, k % 2, low + k // 2)
                return carry

            lax.fori_loop(0, 2 * count, body, 0)

        @pl.when((job == 2) & (c == 1) & (turn >= 12))
        def _():
            later = (turn - 11) // 2
            low = differ * later * (2 * turn - 23)
            relays(1, 0, low, differ * (3 - later) + (1 - differ) * (turn // 14))

    def relay_last(rnd, v):
        @pl.when((rnd == 1) & (c == 1) & (v >= 1) & (v < UPPER3 - 3 * differ))
        def _():
            relays(1, 0, v + 6 * differ, 1)

    def tiles_of(turn):
        out = []
        for half in range(2):
            row = turn * 2 + half
            for step in range(3):
                out.append((*upper_tile(row, step), step == 0))
        out.append((turn, turn + 3, False))
        return sorted(out, key=lambda item: item[2])

    def unit(v, step):
        late = (v + 3) // 6
        half = (v - 3) % 2
        base = G * (1 - (v - 3) // 2)
        row = base + half * (1 + step // 2)
        col = base + (1 - half) * step + half * (1 + (step + 1) // 2)
        return row * late + v * (1 - late), col * late + (G + step) * (1 - late)

    def send_aid(v):
        for row, col, _ in tiles_of(v):
            ref = stage.at[2, slot_of(row, col)]
            pltpu.make_async_remote_copy(
                ref, ref, aid_send, aid_sem, device_id=device(y, x, 0), device_id_type=MESH
            ).start()

    def square(src, job, before, may_aid):
        own_job = (job + 1) // 2

        def turn(v, carry):
            relay_early(job, before + v)
            if may_aid:
                pl.when((job == 0) & (v > 0))(lambda: send_aid(v - 1))
            for row, col, diag in tiles_of(v):
                if diag:
                    cross = chain(src, src, row, col, ((0, 2), (0, 1)))
                    val = chain(src, src, row, col, ((1, 1), (0, 0)))
                    val = val + (cross + cross.T)
                else:
                    val = chain(src, src, row, col, PASSES)
                put(buf_b, row, col, val, diag)
                if may_aid:
                    stage[2, slot_of(row, col) * (1 - own_job) + UPPER * own_job] = val
                sums[2] += fold(val * get(src, row, col)) * (1.0 if diag else 2.0)
            return carry

        sums[2] = jnp.zeros_like(sums[2])
        lax.fori_loop(0, 3, turn, 0)
        if may_aid:
            pl.when(job == 0)(lambda: send_aid(2))

    def absorb():
        wait_for(stage.at[2, pl.ds(0, UPPER)], aid_sem)
        sums[2] = jnp.zeros_like(sums[2])

        def turn(v, carry):
            for step in range(3):
                row, col = unit(v, step)
                val = stage[2, slot_of(row, col)]
                put(buf_b, row, col, val, False)
                sums[2] += fold(val * get(buf_a, row, col)) * jnp.where(row == col, 1.0, 2.0)
            return carry

        lax.fori_loop(0, 7, turn, 0)

    def coefs():
        t1, t2, t3 = total(sums[0]), total(sums[1]), total(sums[2])
        coef = (t2 - t3) / (t1 - t2)
        inv = 1.0 / (1.0 - coef)
        return (1.0 - 2.0 * coef) * inv, (1.0 + coef) * inv, inv

    def count(val, diag):
        if diag:
            sums[0] += fold(val * eye)
        sums[1] += fold(val * val) * (1.0 if diag else 2.0)

    def combine(src, row, col, co):
        acc = chain(buf_b, src, row, col, PASSES)
        return co[0] * get(src, row, col) + co[1] * get(buf_b, row, col) - co[2] * acc

    def cube(src, dst, job, before):
        co = coefs()
        sums[0:2] = jnp.zeros_like(sums[0:2])

        def turn(v, carry):
            relay_early(job, before + v)
            for row, col, diag in tiles_of(v):
                val = combine(src, row, col, co)
                put(dst, row, col, val, diag)
                count(val, diag)
            return carry

        lax.fori_loop(0, 3, turn, 0)

    def cube_last(src, rnd):
        co = coefs()
        sums[0] = jnp.zeros_like(sums[0])

        def turn(v, carry):
            @pl.when(v > 0)
            def _():
                for step in range(3):
                    send_out(rnd, *unit(v - 1, step))

            relay_last(rnd, v)

            for step in range(3):
                row, col = unit(v, step)
                val = combine(src, row, col, co)
                slot = slot_of(row, col)
                weight = jnp.where(row == col, 1.0, 2.0)
                sums[0] += fold(val * stage[rnd, slot]) * weight
                stage[rnd, slot] = val
            return carry

        lax.fori_loop(0, 7, turn, 0)
        for step in range(3):
            send_out(rnd, *unit(6, step))

    def one_job(job, carry):
        pl.when((job > 0) | (c == 1))(lambda: run_job(job))
        return carry

    def run_job(job):
        own_job = (job + 1) // 2
        rnd = job - 1
        put_in = (job + 2) % 3
        mat = own_job * (rnd * 8 + own) + (1 - own_job) * (8 + own - 1)
        wait_for(stage.at[put_in, pl.ds(0, 15)], so_sem.at[put_in])
        wait_for(stage.at[put_in, pl.ds(15, 6), pl.ds(0, tile * 7 // 8)], r_sem.at[put_in])
        half = tile // 2
        for i in range(G, NB):
            slot = slot_of(i, i)
            stage[put_in, slot, half:, :half] = stage[put_in, slot, :half, half:].T
        diag_sum = fold(stage[put_in, slot_of(0, 0)] * eye)
        for i in range(1, NB):
            diag_sum += fold(stage[put_in, slot_of(i, i)] * eye)
        mean = total(diag_sum) / order
        filled = occ[mat].astype(F32)
        scale = jnp.minimum(
            filled / (bounds[1, mat] - mean), (order - filled) / (mean - bounds[0, mat])
        )
        on_diag = (scale * mean + filled) / order
        slope = scale / order
        sums[0:2] = jnp.zeros_like(sums[0:2])

        def first(v, c_):
            for step in range(3):
                row, col = unit(v, step)
                one = jnp.where(row == col, 1.0, 0.0)
                val = stage[put_in, slot_of(row, col)] * -slope + (on_diag * one) * eye
                put(buf_a, row, col, val, False)
                sums[0] += fold(val * eye) * one
                sums[1] += fold(val * val) * (2.0 - one)
            return c_

        lax.fori_loop(0, 7, first, 0)
        given = (job == 2) & (c == 0)
        mine = job > 0

        def step(s, c_):
            @pl.when(((s == 0) & ~given) | ((s == 2) & mine))
            def _():
                square(buf_a, job, 6 * s, True)

            pl.when((s == 0) & given)(absorb)
            pl.when((s == 1) & mine)(lambda: square(buf_c, job, 6, False))
            pl.when((s == 0) & mine)(lambda: cube(buf_a, buf_c, job, 3))
            pl.when((s == 1) & mine)(lambda: cube(buf_c, buf_a, job, 9))
            pl.when((s == 2) & mine)(lambda: finish(rnd, mat))
            return c_

        lax.fori_loop(0, STEPS, step, 0)

    def finish(rnd, mat):
        cube_last(buf_a, rnd)
        lane = lax.broadcasted_iota(jnp.int32, e_vec.shape[1:], 1)
        e_vec[rnd] = jnp.where(lane == mat, 2.0 * total(sums[0]), 0.0)
        for k in range(1, 8):
            pltpu.make_async_remote_copy(
                e_vec.at[rnd], ener.at[mat], e_send, e_sem,
                device_id=device(flip(y, k // 4), flip(x, (k // 2) % 2), flip(c, k % 2)),
                device_id_type=MESH,
            ).start()
        pltpu.make_async_copy(e_vec.at[rnd], ener.at[mat], e_sem).start()

    lax.fori_loop(0, 3, one_job, 0)

    pl.when(c == 0)(lambda: relays(1, 0, 0, G * G))
    relays(1, 1, 0, G * G)
    wait_for(ener.at[pl.ds(0, 14)], e_send)
    wait_for(ener, e_sem)

    def wait_tiles(quarters, sem):
        lead = 8 if quarters <= 288 else 16
        wait_for(ham.at[pl.ds(0, lead), pl.ds(0, quarters * tile // (12 * lead)), :], sem)

    @pl.when(c == 1)
    def _():
        wait_for(stage.at[2, pl.ds(0, UPPER)], aid_send)

    @pl.when(differ == 0)
    def _():
        pl.when(c == 0)(lambda: wait_tiles(105 + 72, in_send))
        pl.when(c == 1)(lambda: wait_tiles(105 + 48, in_send))
        wait_tiles(4 * 96, out_send)
        wait_tiles(4 * 63, land_sem)

    @pl.when(differ == 1)
    def _():
        pl.when(c == 0)(lambda: wait_tiles(108, in_send))
        pl.when(c == 1)(lambda: wait_tiles(72, in_send))
        wait_tiles(414, out_send)
        wait_tiles(4 * 108, land_sem)


RING = 4


def unpack_kernel(land, ener, out, energy, held, block, in_sem, out_sem):
    mats, tile = out.shape[0], land.shape[1]
    half = tile // 2
    x, c = lax.axis_index('row'), lax.axis_index('col')
    differ = flip(x, c)

    def load(mat, act):
        slot = mat % RING
        for kind, count in ((0, UPPER3), (1, G * G)):

            @pl.when(differ == kind)
            def _():
                act(
                    pltpu.make_async_copy(
                        land.at[pl.ds(mat * count, count)],
                        held.at[slot, pl.ds(0, count)],
                        in_sem.at[slot],
                    )
                )

    def store(mat):
        slot = mat % RING
        return pltpu.make_async_copy(block.at[slot], out.at[mat], out_sem.at[slot])

    def prime(mat, carry):
        load(mat, lambda copy: copy.start())
        return carry

    lax.fori_loop(0, RING, prime, 0)
    energy[...] = jnp.sum(ener[...], axis=0)[0, : energy.shape[0]]

    def turn(mat, carry):
        slot = mat % RING
        turned = flip((mat // 2) % 2, x)
        load(mat, lambda copy: copy.wait())
        pl.when(mat >= RING)(lambda: store(mat - RING).wait())

        def write(i, j, val):
            rows, cols = val.shape
            block[slot, pl.ds(i * half, rows), pl.ds(j * half, cols)] = val

        @pl.when(differ == 0)
        def _():
            for i in range(G):
                for j in range(i, G):
                    place = slot3_of(i, j)
                    if i == j:
                        top = held[slot, place, :half, :]
                        write(2 * i, 2 * i, top)
                        write(2 * i + 1, 2 * i, top[:, half:].T)
                        write(2 * i + 1, 2 * i + 1, held[slot, place, half:, half:])
                    else:
                        val = held[slot, place]
                        write(2 * i, 2 * j, val)
                        write(2 * j, 2 * i, val.T)

        @pl.when(differ * (1 - turned) == 1)
        def _():
            for i in range(G):
                for j in range(G):
                    write(2 * i, 2 * j, held[slot, i * G + j])

        @pl.when(differ * turned == 1)
        def _():
            for i in range(G):
                for j in range(G):
                    write(2 * j, 2 * i, held[slot, i * G + j].T)

        store(mat).start()
        pl.when(mat + RING < mats)(lambda: load(mat + RING, lambda copy: copy.start()))
        return carry

    lax.fori_loop(0, mats, turn, 0)
    for mat in range(mats - RING, mats):
        store(mat).wait()


def solution(mesh):
    def local_purify(ham, bounds, occ):
        mats, blk, _ = ham.shape
        tile = blk // G
        any_spec = pl.BlockSpec(memory_space=pltpu.HBM)
        smem = pl.BlockSpec(memory_space=pltpu.SMEM)
        limb = pltpu.VMEM((3, NB, NB, tile, tile), BF16)
        flops = 2 * 6 * 21 * 36 * 2 * tile**3
        land, ener = pl.pallas_call(
            main_kernel,
            out_shape=(
                jax.ShapeDtypeStruct((mats * G * G, tile, tile), F32),
                jax.ShapeDtypeStruct((mats, 8, 128), F32),
            ),
            in_specs=[smem, smem, any_spec],
            out_specs=(any_spec, any_spec),
            scratch_shapes=[
                limb, limb, limb,
                pltpu.VMEM((3, UPPER + 1, tile, tile), F32),
                pltpu.VMEM((3, 8, tile), F32),
                pltpu.VMEM((2, 8, 128), F32),
                pltpu.SemaphoreType.DMA((3,)),
                pltpu.SemaphoreType.DMA((3,)),
                pltpu.SemaphoreType.DMA,
                pltpu.SemaphoreType.DMA,
                pltpu.SemaphoreType.DMA,
                pltpu.SemaphoreType.DMA,
                pltpu.SemaphoreType.DMA((2, 2, G * G)),
                pltpu.SemaphoreType.DMA,
                pltpu.SemaphoreType.DMA,
                pltpu.SemaphoreType.DMA,
            ],
            compiler_params=pltpu.CompilerParams(
                collective_id=0, has_side_effects=True, vmem_limit_bytes=67043328
            ),
            cost_estimate=pl.CostEstimate(flops=flops, bytes_accessed=120 * 2**20, transcendentals=0),
            name='purify',
        )(bounds.T, occ, ham)

        return pl.pallas_call(
            unpack_kernel,
            out_shape=(
                jax.ShapeDtypeStruct(ham.shape, F32),
                jax.ShapeDtypeStruct((mats,), F32),
            ),
            in_specs=[any_spec, pl.BlockSpec(memory_space=pltpu.VMEM)],
            out_specs=(any_spec, pl.BlockSpec(memory_space=pltpu.VMEM)),
            scratch_shapes=[
                pltpu.VMEM((RING, G * G, tile, tile), F32),
                pltpu.VMEM((RING, blk, blk), F32),
                pltpu.SemaphoreType.DMA((RING,)),
                pltpu.SemaphoreType.DMA((RING,)),
            ],
            compiler_params=pltpu.CompilerParams(vmem_limit_bytes=40 * 2**20),
            cost_estimate=pl.CostEstimate(flops=10**6, bytes_accessed=75 * 2**20, transcendentals=0),
            name='unpack',
        )(land, ener)

    mat_spec = P('spin', 'row', 'col')
    return jax.shard_map(
        local_purify, mesh=mesh,
        in_specs=(mat_spec, P('spin', None), P('spin')),
        out_specs=(mat_spec, P('spin')), check_vma=False,
    )
```

```python
import functools

import jax
import jax.numpy as jnp
from jax import lax
from jax.experimental import pallas as pl
from jax.experimental.pallas import tpu as pltpu
from jax.sharding import PartitionSpec as P

STEPS = 3
G = 3
NB = 2 * G
UPPER = NB * (NB + 1) // 2
UPPER3 = G * (G + 1) // 2
OVER_X = 8
F32 = jnp.float32
BF16 = jnp.bfloat16
PASSES = ((0, 2), (2, 0), (1, 1), (0, 1), (1, 0), (0, 0))
MESH = pl.DeviceIdType.MESH


def slot_of(row, col):
    return row * (2 * NB - 1 - row) // 2 + col


def slot3_of(row, col):
    return row * (2 * G - 1 - row) // 2 + col


def upper_tile(row, step):
    wrap = (row + step) // NB
    other = row + step - NB * wrap
    return row * (1 - wrap) + other * wrap, other * (1 - wrap) + row * wrap


def limbs(val):
    high = val.astype(BF16)
    rest = val - high.astype(F32)
    mid = rest.astype(BF16)
    low = (rest - mid.astype(F32)).astype(BF16)
    return high, mid, low


def put(ref, row, col, val, diag):
    for piece, part in enumerate(limbs(val)):
        ref[piece, row, col] = part
    if not diag:
        for piece, part in enumerate(limbs(val.T)):
            ref[piece, col, row] = part


def get(ref, row, col):
    low = ref[1, row, col].astype(F32) + ref[2, row, col].astype(F32)
    return ref[0, row, col].astype(F32) + low


def chain(left, right, row, col, passes):
    acc = None
    for k in range(NB):
        for p, q in passes:
            part = jnp.dot(left[p, row, k], right[q, k, col], preferred_element_type=F32)
            acc = part if acc is None else acc + part
    return acc


def fold(val):
    size = val.shape[0]
    return jnp.sum(val.reshape(size // 8, 8, val.shape[1]), axis=0)


def total(val):
    return jnp.sum(jnp.sum(val, axis=0, keepdims=True), axis=1, keepdims=True)


def flip(bit, by):
    return bit + by - 2 * bit * by


def main_kernel(
    bounds, occ, ham, land, ener,
    buf_a, buf_b, buf_c, stage, sums, e_vec, corner, t_vec, t_land,
    so_sem, r_sem, corner_sem, t_sem, t_send, in_send, aid_sem, aid_send, land_sem, relay_sem, out_send, e_sem, e_send,
):
    tile = stage.shape[2]
    order = NB * tile
    y, x, c = lax.axis_index('depth'), lax.axis_index('row'), lax.axis_index('col')
    own = y * 4 + x * 2 + c
    differ = flip(x, c)

    def device(dy, dx, cd):
        return {'depth': dy, 'row': dx, 'col': cd}

    barrier = pltpu.get_barrier_semaphore()
    for k in range(1, 8):
        pl.semaphore_signal(
            barrier, inc=1,
            device_id=device(flip(y, k // 4), flip(x, (k // 2) % 2), flip(c, k % 2)),
            device_id_type=MESH,
        )
    pl.semaphore_wait(barrier, 7)

    def h_tile(mat, i, j):
        return ham.at[mat, pl.ds(i * tile, tile), pl.ds(j * tile, tile)]

    def parts(diag):
        half = tile // 2
        if not diag:
            return [(slice(None), slice(None))]
        return [(pl.ds(0, half), slice(None)), (pl.ds(half, half), pl.ds(half, half))]

    diag_tiles = [(i, j) for i in range(G) for j in range(i, G)]

    def send_in(e, carry):
        late = e // 3
        aid = (e % 3) % 2 * (1 - late)
        cd = (1 - late) * ((e + 1) // 2) + late * (e - 3)
        mat = 8 * (aid + late) + cd * (1 - aid) + y * 4
        put_in = 2 * aid + late

        @pl.when(differ == 0)
        def _():
            for i, j in diag_tiles:
                for part in parts(i == j):
                    pltpu.make_async_remote_copy(
                        h_tile(mat + (1 - x) * 2, i, j).at[part],
                        stage.at[put_in, slot_of(G + i, G + j)].at[part],
                        in_send, r_sem.at[put_in],
                        device_id=device(y, 1 - x, cd), device_id_type=MESH,
                    ).start()

        def near(tiles, shift):
            for i, j in tiles:
                near_tile(i, j, shift)

        def near_row(i, carry_):
            for j in range(G):
                near_tile(i, j, G)
            return carry_

        def near_tile(i, j, shift):
            src = h_tile(mat + x * 2, i, j)
            dst = stage.at[put_in, slot_of(i, shift + j)]

            @pl.when(cd == c)
            def _():
                pltpu.make_async_copy(src, dst, so_sem.at[put_in]).start()

            @pl.when(cd != c)
            def _():
                pltpu.make_async_remote_copy(
                    src, dst, in_send, so_sem.at[put_in],
                    device_id=device(y, x, cd), device_id_type=MESH,
                ).start()

        pl.when(differ == 0)(lambda: near(diag_tiles, 0))

        @pl.when(differ == 1)
        def _():
            lax.fori_loop(0, G, near_row, 0)

        return carry

    quarter = tile // 2

    @pl.when(differ == 0)
    def _():
        for e in range(2):
            for i in range(NB):
                spot = pl.ds(i * quarter, quarter)
                pltpu.make_async_copy(
                    ham.at[y * 4 + (1 - x) * 2 + 8 * e, spot, spot], corner.at[e, i], corner_sem.at[e]
                ).start()

    lax.fori_loop(0, 5, send_in, 0)

    def wait_for(ref, sem):
        pltpu.make_async_copy(ref, ref, sem).wait()

    rows = lax.broadcasted_iota(jnp.int32, (tile, tile), 0)
    cols = lax.broadcasted_iota(jnp.int32, (tile, tile), 1)
    eye = jnp.where(rows == cols, 1.0, 0.0).astype(F32)

    @pl.when(differ == 0)
    def _():
        for e in range(2):
            wait_for(corner.at[e], corner_sem.at[e])
            part = fold(corner[e, 0] * eye[:quarter, :quarter])
            for i in range(1, NB):
                part += fold(corner[e, i] * eye[:quarter, :quarter])
            t_vec[e] = part
        for e in range(2):
            pltpu.make_async_remote_copy(
                t_vec.at[e], t_land, t_send, t_sem,
                device_id=device(y, 1 - x, e), device_id_type=MESH,
            ).start()


    def send_out(rnd, row, col):
        mat = rnd * 8 + own
        src = stage.at[rnd, slot_of(row, col)]
        k_row, k_col = row // G, col // G

        def start(dy, xd, cd, dst, sem, diag=False):
            for part in parts(diag):
                pltpu.make_async_remote_copy(
                    src.at[part], dst.at[part], out_send, sem,
                    device_id=device(flip(y, dy), xd, cd), device_id_type=MESH,
                ).start()

        def keep(dst, diag=False):
            for part in parts(diag):
                pltpu.make_async_copy(src.at[part], dst.at[part], land_sem).start()

        @pl.when(k_row + k_col == 1)
        def _():
            place = row * G + col - G
            dst = land.at[mat * 9 + place]
            sem = relay_sem.at[rnd, c, place]

            @pl.when(place < OVER_X)
            def _():
                start(1, x, 1 - x, dst, sem)
                start(0, 1 - x, x, dst, land_sem)

            @pl.when(place >= OVER_X)
            def _():
                start(0, 1 - x, x, dst, sem)
                start(1, x, 1 - x, dst, land_sem)

            pl.when(differ == 1)(lambda: keep(dst))
            pl.when(differ == 0)(lambda: start(0, x, 1 - x, dst, land_sem))

        for diag in (False, True):
            same = (row == col) if diag else (row != col)

            @pl.when((k_row == 1) & same)
            def _():
                place = slot3_of(row - G, col - G)
                start(0, 1 - x, 1 - x, land.at[mat * 6 + place], relay_sem.at[rnd, c, place], diag)

            @pl.when((k_col == 0) & same)
            def _():
                dst = land.at[mat * 6 + slot3_of(row, col)]
                start(1, x, x, dst, land_sem, diag)
                pl.when(differ == 0)(lambda: keep(dst, diag))
                pl.when(differ == 1)(lambda: start(0, x, x, dst, land_sem, diag))

    def relay(rnd, cd, place):
        over_x = differ * (1 - place // OVER_X)
        owner = over_x * ((1 - y) * 4 + x * 2) + (1 - over_x) * (y * 4 + (1 - x) * 2) + cd
        dev = device(flip(y, 1 - over_x), flip(x, over_x), over_x * x + (1 - over_x) * c)
        tile_ref = land.at[(rnd * 8 + owner) * (UPPER3 + 3 * differ) + place]

        def pass_on(whole, diag):
            wait_for(whole, relay_sem.at[rnd, cd, place])
            for part in parts(diag):
                pltpu.make_async_remote_copy(
                    tile_ref.at[part], tile_ref.at[part], out_send, land_sem,
                    device_id=dev, device_id_type=MESH,
                ).start()

        on_diag = (differ == 0) & ((place == 0) | (place == 3) | (place == 5))
        pl.when(on_diag)(lambda: pass_on(tile_ref.at[pl.ds(0, tile * 3 // 4)], True))
        pl.when(~on_diag & (place < UPPER3 + 3 * differ))(lambda: pass_on(tile_ref, False))

    def relays(rnd, cd, low, count):
        def body(k, carry):
            relay(rnd, cd, low + k)
            return carry

        lax.fori_loop(0, count, body, 0)

    def relay_early(job, turn):
        one = (c == 1) & (turn >= 1) & (turn < 1 + G * G)
        two = (c == 0) & (turn >= 9) & (turn < 14)

        @pl.when((job == 2) & (one | two))
        def _():
            low = c * (turn - 1) + (1 - c) * 2 * (turn - 9)
            count = 1 + (1 - c) * (1 - turn // 13)

            def body(k, carry):
                relay(0, k % 2, low + k // 2)
                return carry

            lax.fori_loop(0, 2 * count, body, 0)

        off = (differ == 1) & (turn >= 11) & (turn < 14)
        far = (differ == 0) & (turn >= 13)

        @pl.when((job == 2) & (c == 1) & (off | far))
        def _():
            nth = turn - 13 + 2 * differ
            low = nth * (2 + nth // 2)
            relays(1, 0, low, 2 + 2 * (nth % 2) + nth // 2)

    def tiles_of(turn):
        out = []
        for half in range(2):
            row = turn * 2 + half
            for step in range(3):
                out.append((*upper_tile(row, step), step == 0))
        out.append((turn, turn + 3, False))
        return sorted(out, key=lambda item: item[2])

    def unit(v, step):
        late = (v + 3) // 6
        half = (v - 3) % 2
        base = G * (1 - (v - 3) // 2)
        row = base + half * (1 + step // 2)
        col = base + (1 - half) * step + half * (1 + (step + 1) // 2)
        return row * late + v * (1 - late), col * late + (G + step) * (1 - late)

    def near_tiles(turn):
        return [(turn, turn, True), (turn // 2, 1 + (turn + 1) // 2, False)]

    def other_tiles(turn):
        off = [(turn, G + j, False) for j in range(G)]
        off.append((G + turn // 2, G + 1 + (turn + 1) // 2, False))
        return [*off, (G + turn, G + turn, True)]

    def send_aid(tiles):
        for row, col, _ in tiles:
            ref = stage.at[2, slot_of(row, col)]
            pltpu.make_async_remote_copy(
                ref, ref, aid_send, aid_sem, device_id=device(y, x, 0), device_id_type=MESH
            ).start()

    def square_tiles(src, tiles, keep, early=False):
        def cross(row, col):
            part = chain(src, src, row, col, ((0, 2), (0, 1)))
            return part + part.T

        ready = [cross(row, col) if early and diag else None for row, col, diag in tiles]
        for (row, col, diag), part in zip(tiles, ready):
            if diag:
                part = cross(row, col) if part is None else part
                val = chain(src, src, row, col, ((1, 1), (0, 0))) + part
            else:
                val = chain(src, src, row, col, PASSES)
            put(buf_b, row, col, val, diag)
            if keep is not None:
                stage[2, slot_of(row, col) * (1 - keep) + UPPER * keep] = val
            sums[2] += fold(val * get(src, row, col)) * (1.0 if diag else 2.0)

    def square_a(job, before, between):
        own_job = (job + 1) // 2
        sums[2] = jnp.zeros_like(sums[2])

        def near(v, carry):
            pl.when((job == 0) & (v > 0))(lambda: send_aid(near_tiles(v - 1)))
            square_tiles(buf_a, near_tiles(v), own_job)
            return carry

        def other(v, carry):
            relay_early(job, before + v)
            pl.when((job == 0) & (v == 0))(lambda: send_aid(near_tiles(2)))
            pl.when((job == 0) & (v > 0))(lambda: send_aid(other_tiles(v - 1)))
            square_tiles(buf_a, other_tiles(v), own_job, True)
            return carry

        lax.fori_loop(0, 3, near, 0)
        between()
        lax.fori_loop(0, 3, other, 0)
        pl.when(job == 0)(lambda: send_aid(other_tiles(2)))

    def square_c(job, before):
        sums[2] = jnp.zeros_like(sums[2])

        def turn(v, carry):
            relay_early(job, before + v)
            square_tiles(buf_c, tiles_of(v), None)
            return carry

        lax.fori_loop(0, 3, turn, 0)

    def absorb():
        wait_for(stage.at[2, pl.ds(0, UPPER)], aid_sem)
        sums[2] = jnp.zeros_like(sums[2])

        def turn(v, carry):
            for step in range(3):
                row, col = unit(v, step)
                val = stage[2, slot_of(row, col)]
                put(buf_b, row, col, val, False)
                sums[2] += fold(val * get(buf_a, row, col)) * jnp.where(row == col, 1.0, 2.0)
            return carry

        lax.fori_loop(0, 7, turn, 0)

    def coefs():
        t1, t2, t3 = total(sums[0]), total(sums[1]), total(sums[2])
        coef = (t2 - t3) / (t1 - t2)
        inv = 1.0 / (1.0 - coef)
        return (1.0 - 2.0 * coef) * inv, (1.0 + coef) * inv, inv

    def count(val, diag):
        if diag:
            sums[0] += fold(val * eye)
        sums[1] += fold(val * val) * (1.0 if diag else 2.0)

    def combine(src, row, col, co):
        acc = chain(buf_b, src, row, col, PASSES)
        return co[0] * get(src, row, col) + co[1] * get(buf_b, row, col) - co[2] * acc

    def cube(src, dst, job, before):
        co = coefs()
        sums[0:2] = jnp.zeros_like(sums[0:2])

        def turn(v, carry):
            relay_early(job, before + v)
            for row, col, diag in tiles_of(v):
                val = combine(src, row, col, co)
                put(dst, row, col, val, diag)
                count(val, diag)
            return carry

        lax.fori_loop(0, 3, turn, 0)

    def cube_last(src, rnd):
        co = coefs()
        sums[0] = jnp.zeros_like(sums[0])

        def turn(v, carry):
            @pl.when(v > 0)
            def _():
                for step in range(3):
                    send_out(rnd, *unit(v - 1, step))

            for step in range(3):
                row, col = unit(v, step)
                val = combine(src, row, col, co)
                slot = slot_of(row, col)
                weight = jnp.where(row == col, 1.0, 2.0)
                sums[0] += fold(val * stage[rnd, slot]) * weight
                stage[rnd, slot] = val
            return carry

        lax.fori_loop(0, 7, turn, 0)
        for step in range(3):
            send_out(rnd, *unit(6, step))

    def one_job(job, carry):
        pl.when((job > 0) | (c == 1))(lambda: run_job(job))
        return carry

    def run_job(job):
        own_job = (job + 1) // 2
        rnd = job - 1
        put_in = (job + 2) % 3
        mat = own_job * (rnd * 8 + own) + (1 - own_job) * (8 + own - 1)
        wait_for(stage.at[put_in, pl.ds(0, 15)], so_sem.at[put_in])
        starts = job == 1 - c

        def far_block():
            wait_for(stage.at[put_in, pl.ds(15, 6), pl.ds(0, tile * 7 // 8)], r_sem.at[put_in])
            for i in range(G, NB):
                slot = slot_of(i, i)
                stage[put_in, slot, quarter:, :quarter] = stage[put_in, slot, :quarter, quarter:].T

        @pl.when(starts)
        def _():
            wait_for(t_land, t_sem)

        @pl.when(~starts)
        def _():
            far_block()
            part = fold(stage[put_in, slot_of(G, G)] * eye)
            for i in range(G + 1, NB):
                part += fold(stage[put_in, slot_of(i, i)] * eye)
            t_land[...] = part[:, :quarter] + part[:, quarter:]

        diag_sum = fold(stage[put_in, slot_of(0, 0)] * eye)
        for i in range(1, G):
            diag_sum += fold(stage[put_in, slot_of(i, i)] * eye)
        mean = (total(diag_sum) + total(t_land[...])) / order
        filled = occ[mat].astype(F32)
        scale = jnp.minimum(
            filled / (bounds[1, mat] - mean), (order - filled) / (mean - bounds[0, mat])
        )
        on_diag = (scale * mean + filled) / order
        slope = scale / order
        sums[0:2] = jnp.zeros_like(sums[0:2])

        def first(q, c_):
            v = q + 2 * (q // 3 - q // 6) - 4 * (q // 5)
            for step in range(3):
                row, col = unit(v, step)
                one = jnp.where(row == col, 1.0, 0.0)
                val = stage[put_in, slot_of(row, col)] * -slope + (on_diag * one) * eye
                put(buf_a, row, col, val, False)
                sums[0] += fold(val * eye) * one
                sums[1] += fold(val * val) * (2.0 - one)
            return c_

        lax.fori_loop(0, 5 + 2 * jnp.where(starts, 0, 1), first, 0)
        given = (job == 2) & (c == 0)
        mine = job > 0

        def step(s, c_):
            @pl.when(((s == 0) & ~given) | ((s == 2) & mine))
            def _():
                def between():
                    @pl.when(starts & (s == 0))
                    def _():
                        far_block()
                        lax.fori_loop(5, 7, first, 0)

                square_a(job, 6 * s, between)

            pl.when((s == 0) & given)(absorb)
            pl.when((s == 1) & mine)(lambda: square_c(job, 6))
            pl.when((s == 0) & mine)(lambda: cube(buf_a, buf_c, job, 3))
            pl.when((s == 1) & mine)(lambda: cube(buf_c, buf_a, job, 9))
            pl.when((s == 2) & mine)(lambda: finish(rnd, mat))
            return c_

        lax.fori_loop(0, STEPS, step, 0)

    def finish(rnd, mat):
        cube_last(buf_a, rnd)
        lane = lax.broadcasted_iota(jnp.int32, e_vec.shape[1:], 1)
        e_vec[rnd] = jnp.where(lane == mat, 2.0 * total(sums[0]), 0.0)
        for k in range(1, 8):
            pltpu.make_async_remote_copy(
                e_vec.at[rnd], ener.at[mat], e_send, e_sem,
                device_id=device(flip(y, k // 4), flip(x, (k // 2) % 2), flip(c, k % 2)),
                device_id_type=MESH,
            ).start()
        pltpu.make_async_copy(e_vec.at[rnd], ener.at[mat], e_sem).start()

    lax.fori_loop(0, 3, one_job, 0)

    pl.when(c == 0)(lambda: relays(1, 0, 0, G * G))
    relays(1, 1, 0, G * G)
    wait_for(ener.at[pl.ds(0, 14)], e_send)
    wait_for(ener, e_sem)

    def wait_tiles(quarters, sem):
        lead = 8 if quarters <= 288 else 16
        wait_for(ham.at[pl.ds(0, lead), pl.ds(0, quarters * tile // (12 * lead)), :], sem)

    @pl.when(c == 1)
    def _():
        wait_for(stage.at[2, pl.ds(0, UPPER)], aid_send)

    @pl.when(differ == 0)
    def _():
        pl.when(c == 0)(lambda: wait_tiles(105 + 72, in_send))
        pl.when(c == 1)(lambda: wait_tiles(105 + 48, in_send))
        wait_for(t_vec, t_send)
        wait_tiles(4 * 96, out_send)
        wait_tiles(4 * 63, land_sem)

    @pl.when(differ == 1)
    def _():
        pl.when(c == 0)(lambda: wait_tiles(108, in_send))
        pl.when(c == 1)(lambda: wait_tiles(72, in_send))
        wait_tiles(414, out_send)
        wait_tiles(4 * 108, land_sem)


RING = 4


def unpack_kernel(land, ener, out, energy, held, block, in_sem, out_sem):
    mats, tile = out.shape[0], land.shape[1]
    half = tile // 2
    x, c = lax.axis_index('row'), lax.axis_index('col')
    differ = flip(x, c)

    def load(mat, act):
        slot = mat % RING
        for kind, count in ((0, UPPER3), (1, G * G)):

            @pl.when(differ == kind)
            def _():
                act(
                    pltpu.make_async_copy(
                        land.at[pl.ds(mat * count, count)],
                        held.at[slot, pl.ds(0, count)],
                        in_sem.at[slot],
                    )
                )

    def store(mat):
        slot = mat % RING
        return pltpu.make_async_copy(block.at[slot], out.at[mat], out_sem.at[slot])

    def prime(mat, carry):
        load(mat, lambda copy: copy.start())
        return carry

    lax.fori_loop(0, RING, prime, 0)
    energy[...] = jnp.sum(ener[...], axis=0)[0, : energy.shape[0]]

    def turn(mat, carry):
        slot = mat % RING
        turned = flip((mat // 2) % 2, x)
        load(mat, lambda copy: copy.wait())
        pl.when(mat >= RING)(lambda: store(mat - RING).wait())

        def write(i, j, val):
            rows, cols = val.shape
            block[slot, pl.ds(i * half, rows), pl.ds(j * half, cols)] = val

        @pl.when(differ == 0)
        def _():
            for i in range(G):
                for j in range(i, G):
                    place = slot3_of(i, j)
                    if i == j:
                        top = held[slot, place, :half, :]
                        write(2 * i, 2 * i, top)
                        write(2 * i + 1, 2 * i, top[:, half:].T)
                        write(2 * i + 1, 2 * i + 1, held[slot, place, half:, half:])
                    else:
                        val = held[slot, place]
                        write(2 * i, 2 * j, val)
                        write(2 * j, 2 * i, val.T)

        @pl.when(differ * (1 - turned) == 1)
        def _():
            for i in range(G):
                for j in range(G):
                    write(2 * i, 2 * j, held[slot, i * G + j])

        @pl.when(differ * turned == 1)
        def _():
            for i in range(G):
                for j in range(G):
                    write(2 * j, 2 * i, held[slot, i * G + j].T)

        store(mat).start()
        pl.when(mat + RING < mats)(lambda: load(mat + RING, lambda copy: copy.start()))
        return carry

    lax.fori_loop(0, mats, turn, 0)
    for mat in range(mats - RING, mats):
        store(mat).wait()


def solution(mesh):
    def local_purify(ham, bounds, occ):
        mats, blk, _ = ham.shape
        tile = blk // G
        any_spec = pl.BlockSpec(memory_space=pltpu.HBM)
        smem = pl.BlockSpec(memory_space=pltpu.SMEM)
        limb = pltpu.VMEM((3, NB, NB, tile, tile), BF16)
        flops = 2 * 6 * 21 * 36 * 2 * tile**3
        land, ener = pl.pallas_call(
            main_kernel,
            out_shape=(
                jax.ShapeDtypeStruct((mats * G * G, tile, tile), F32),
                jax.ShapeDtypeStruct((mats, 8, 128), F32),
            ),
            in_specs=[smem, smem, any_spec],
            out_specs=(any_spec, any_spec),
            scratch_shapes=[
                limb, limb, limb,
                pltpu.VMEM((3, UPPER + 1, tile, tile), F32),
                pltpu.VMEM((3, 8, tile), F32),
                pltpu.VMEM((2, 8, 128), F32),
                pltpu.VMEM((2, NB, tile // 2, tile // 2), F32),
                pltpu.VMEM((2, 8, tile // 2), F32),
                pltpu.VMEM((8, tile // 2), F32),
                pltpu.SemaphoreType.DMA((3,)),
                pltpu.SemaphoreType.DMA((3,)),
                pltpu.SemaphoreType.DMA((2,)),
                pltpu.SemaphoreType.DMA,
                pltpu.SemaphoreType.DMA,
                pltpu.SemaphoreType.DMA,
                pltpu.SemaphoreType.DMA,
                pltpu.SemaphoreType.DMA,
                pltpu.SemaphoreType.DMA,
                pltpu.SemaphoreType.DMA((2, 2, G * G)),
                pltpu.SemaphoreType.DMA,
                pltpu.SemaphoreType.DMA,
                pltpu.SemaphoreType.DMA,
            ],
            compiler_params=pltpu.CompilerParams(
                collective_id=0, has_side_effects=True, vmem_limit_bytes=67043328
            ),
            cost_estimate=pl.CostEstimate(flops=flops, bytes_accessed=120 * 2**20, transcendentals=0),
            name='purify',
        )(bounds.T, occ, ham)

        return pl.pallas_call(
            unpack_kernel,
            out_shape=(
                jax.ShapeDtypeStruct(ham.shape, F32),
                jax.ShapeDtypeStruct((mats,), F32),
            ),
            in_specs=[any_spec, pl.BlockSpec(memory_space=pltpu.VMEM)],
            out_specs=(any_spec, pl.BlockSpec(memory_space=pltpu.VMEM)),
            scratch_shapes=[
                pltpu.VMEM((RING, G * G, tile, tile), F32),
                pltpu.VMEM((RING, blk, blk), F32),
                pltpu.SemaphoreType.DMA((RING,)),
                pltpu.SemaphoreType.DMA((RING,)),
            ],
            compiler_params=pltpu.CompilerParams(vmem_limit_bytes=40 * 2**20),
            cost_estimate=pl.CostEstimate(flops=10**6, bytes_accessed=75 * 2**20, transcendentals=0),
            name='unpack',
        )(land, ener)

    mat_spec = P('spin', 'row', 'col')
    return jax.shard_map(
        local_purify, mesh=mesh,
        in_specs=(mat_spec, P('spin', None), P('spin')),
        out_specs=(mat_spec, P('spin')), check_vma=False,
    )
```

```python
import functools

import jax
import jax.numpy as jnp
from jax import lax
from jax.experimental import pallas as pl
from jax.experimental.pallas import tpu as pltpu
from jax.sharding import PartitionSpec as P

STEPS = 3
G = 3
NB = 2 * G
UPPER = NB * (NB + 1) // 2
UPPER3 = G * (G + 1) // 2
OVER_X = 8
F32 = jnp.float32
BF16 = jnp.bfloat16
PASSES = ((0, 2), (2, 0), (1, 1), (0, 1), (1, 0), (0, 0))
MESH = pl.DeviceIdType.MESH


def slot_of(row, col):
    return row * (2 * NB - 1 - row) // 2 + col


def slot3_of(row, col):
    return row * (2 * G - 1 - row) // 2 + col


def upper_tile(row, step):
    wrap = (row + step) // NB
    other = row + step - NB * wrap
    return row * (1 - wrap) + other * wrap, other * (1 - wrap) + row * wrap


def limbs(val):
    high = val.astype(BF16)
    rest = val - high.astype(F32)
    mid = rest.astype(BF16)
    low = (rest - mid.astype(F32)).astype(BF16)
    return high, mid, low


def put(ref, row, col, val, diag):
    for piece, part in enumerate(limbs(val)):
        ref[piece, row, col] = part
    if not diag:
        for piece, part in enumerate(limbs(val.T)):
            ref[piece, col, row] = part


def get(ref, row, col):
    low = ref[1, row, col].astype(F32) + ref[2, row, col].astype(F32)
    return ref[0, row, col].astype(F32) + low


def chain(left, right, row, col, passes):
    acc = None
    for k in range(NB):
        for p, q in passes:
            part = jnp.dot(left[p, row, k], right[q, k, col], preferred_element_type=F32)
            acc = part if acc is None else acc + part
    return acc


def fold(val):
    size = val.shape[0]
    return jnp.sum(val.reshape(size // 8, 8, val.shape[1]), axis=0)


def total(val):
    return jnp.sum(jnp.sum(val, axis=0, keepdims=True), axis=1, keepdims=True)


def flip(bit, by):
    return bit + by - 2 * bit * by


def main_kernel(
    bounds, occ, ham, land, ener,
    buf_a, buf_b, buf_c, stage, sums, e_vec, corner, t_vec, t_land,
    so_sem, r_sem, corner_sem, t_sem, t_send, in_send, aid_sem, aid_send, land_sem, relay_sem, out_send, e_sem, e_send,
):
    tile = stage.shape[2]
    order = NB * tile
    y, x, c = lax.axis_index('depth'), lax.axis_index('row'), lax.axis_index('col')
    own = y * 4 + x * 2 + c
    differ = flip(x, c)

    def device(dy, dx, cd):
        return {'depth': dy, 'row': dx, 'col': cd}

    def wait_for(ref, sem):
        pltpu.make_async_copy(ref, ref, sem).wait()

    quarter = tile // 2
    rows = lax.broadcasted_iota(jnp.int32, (tile, tile), 0)
    cols = lax.broadcasted_iota(jnp.int32, (tile, tile), 1)
    eye = jnp.where(rows == cols, 1.0, 0.0).astype(F32)

    barrier = pltpu.get_barrier_semaphore()
    for k in range(1, 8):
        pl.semaphore_signal(
            barrier, inc=1,
            device_id=device(flip(y, k // 4), flip(x, (k // 2) % 2), flip(c, k % 2)),
            device_id_type=MESH,
        )

    @pl.when(differ == 0)
    def _():
        for e in range(2):
            for i in range(NB):
                spot = pl.ds(i * quarter, quarter)
                pltpu.make_async_copy(
                    ham.at[y * 4 + (1 - x) * 2 + 8 * e, spot, spot], corner.at[e, i], corner_sem.at[e]
                ).start()
        for e in range(2):
            wait_for(corner.at[e], corner_sem.at[e])
            part = fold(corner[e, 0] * eye[:quarter, :quarter])
            for i in range(1, NB):
                part += fold(corner[e, i] * eye[:quarter, :quarter])
            t_vec[e] = part

    pl.semaphore_wait(barrier, 7)

    @pl.when(differ == 0)
    def _():
        for e in range(2):
            pltpu.make_async_remote_copy(
                t_vec.at[e], t_land, t_send, t_sem,
                device_id=device(y, 1 - x, e), device_id_type=MESH,
            ).start()

    def h_tile(mat, i, j):
        return ham.at[mat, pl.ds(i * tile, tile), pl.ds(j * tile, tile)]

    def parts(diag):
        half = tile // 2
        if not diag:
            return [(slice(None), slice(None))]
        return [(pl.ds(0, half), slice(None)), (pl.ds(half, half), pl.ds(half, half))]

    diag_tiles = [(i, j) for i in range(G) for j in range(i, G)]

    def send_in(e, carry):
        late = e // 3
        aid = (e % 3) % 2 * (1 - late)
        cd = (1 - late) * ((e + 1) // 2) + late * (e - 3)
        mat = 8 * (aid + late) + cd * (1 - aid) + y * 4
        put_in = 2 * aid + late

        @pl.when(differ == 0)
        def _():
            for i, j in diag_tiles:
                for part in parts(i == j):
                    pltpu.make_async_remote_copy(
                        h_tile(mat + (1 - x) * 2, i, j).at[part],
                        stage.at[put_in, slot_of(G + i, G + j)].at[part],
                        in_send, r_sem.at[put_in],
                        device_id=device(y, 1 - x, cd), device_id_type=MESH,
                    ).start()

        def near(tiles, shift):
            for i, j in tiles:
                near_tile(i, j, shift)

        def near_row(i, carry_):
            for j in range(G):
                near_tile(i, j, G)
            return carry_

        def near_tile(i, j, shift):
            src = h_tile(mat + x * 2, i, j)
            dst = stage.at[put_in, slot_of(i, shift + j)]

            @pl.when(cd == c)
            def _():
                pltpu.make_async_copy(src, dst, so_sem.at[put_in]).start()

            @pl.when(cd != c)
            def _():
                pltpu.make_async_remote_copy(
                    src, dst, in_send, so_sem.at[put_in],
                    device_id=device(y, x, cd), device_id_type=MESH,
                ).start()

        pl.when(differ == 0)(lambda: near(diag_tiles, 0))

        @pl.when(differ == 1)
        def _():
            lax.fori_loop(0, G, near_row, 0)

        return carry

    lax.fori_loop(0, 5, send_in, 0)

    def send_out(rnd, row, col):
        mat = rnd * 8 + own
        src = stage.at[rnd, slot_of(row, col)]
        k_row, k_col = row // G, col // G

        def start(dy, xd, cd, dst, sem, diag=False):
            for part in parts(diag):
                pltpu.make_async_remote_copy(
                    src.at[part], dst.at[part], out_send, sem,
                    device_id=device(flip(y, dy), xd, cd), device_id_type=MESH,
                ).start()

        def keep(dst, diag=False):
            for part in parts(diag):
                pltpu.make_async_copy(src.at[part], dst.at[part], land_sem).start()

        @pl.when(k_row + k_col == 1)
        def _():
            place = row * G + col - G
            dst = land.at[mat * 9 + place]
            sem = relay_sem.at[rnd, c, place]

            @pl.when(place < OVER_X)
            def _():
                start(1, x, 1 - x, dst, sem)
                start(0, 1 - x, x, dst, land_sem)

            @pl.when(place >= OVER_X)
            def _():
                start(0, 1 - x, x, dst, sem)
                start(1, x, 1 - x, dst, land_sem)

            pl.when(differ == 1)(lambda: keep(dst))
            pl.when(differ == 0)(lambda: start(0, x, 1 - x, dst, land_sem))

        for diag in (False, True):
            same = (row == col) if diag else (row != col)

            @pl.when((k_row == 1) & same)
            def _():
                place = slot3_of(row - G, col - G)
                start(0, 1 - x, 1 - x, land.at[mat * 6 + place], relay_sem.at[rnd, c, place], diag)

            @pl.when((k_col == 0) & same)
            def _():
                dst = land.at[mat * 6 + slot3_of(row, col)]
                start(1, x, x, dst, land_sem, diag)
                pl.when(differ == 0)(lambda: keep(dst, diag))
                pl.when(differ == 1)(lambda: start(0, x, x, dst, land_sem, diag))

    def relay(rnd, cd, place):
        over_x = differ * (1 - place // OVER_X)
        owner = over_x * ((1 - y) * 4 + x * 2) + (1 - over_x) * (y * 4 + (1 - x) * 2) + cd
        dev = device(flip(y, 1 - over_x), flip(x, over_x), over_x * x + (1 - over_x) * c)
        tile_ref = land.at[(rnd * 8 + owner) * (UPPER3 + 3 * differ) + place]

        def pass_on(whole, diag):
            wait_for(whole, relay_sem.at[rnd, cd, place])
            for part in parts(diag):
                pltpu.make_async_remote_copy(
                    tile_ref.at[part], tile_ref.at[part], out_send, land_sem,
                    device_id=dev, device_id_type=MESH,
                ).start()

        on_diag = (differ == 0) & ((place == 0) | (place == 3) | (place == 5))
        pl.when(on_diag)(lambda: pass_on(tile_ref.at[pl.ds(0, tile * 3 // 4)], True))
        pl.when(~on_diag & (place < UPPER3 + 3 * differ))(lambda: pass_on(tile_ref, False))

    def relays(rnd, cd, low, count):
        def body(k, carry):
            relay(rnd, cd, low + k)
            return carry

        lax.fori_loop(0, count, body, 0)

    def relay_early(job, turn):
        one = (c == 1) & (turn >= 1) & (turn < 1 + G * G)
        two = (c == 0) & (turn >= 9) & (turn < 14)

        @pl.when((job == 2) & (one | two))
        def _():
            low = c * (turn - 1) + (1 - c) * 2 * (turn - 9)
            count = 1 + (1 - c) * (1 - turn // 13)

            def body(k, carry):
                relay(0, k % 2, low + k // 2)
                return carry

            lax.fori_loop(0, 2 * count, body, 0)

        off = (differ == 1) & (turn >= 11) & (turn < 14)
        far = (differ == 0) & (turn >= 13)

        @pl.when((job == 2) & (c == 1) & (off | far))
        def _():
            nth = turn - 13 + 2 * differ
            low = nth * (2 + nth // 2)
            relays(1, 0, low, 2 + 2 * (nth % 2) + nth // 2)

    def tiles_of(turn):
        out = []
        for half in range(2):
            row = turn * 2 + half
            for step in range(3):
                out.append((*upper_tile(row, step), step == 0))
        out.append((turn, turn + 3, False))
        return sorted(out, key=lambda item: item[2])

    def unit(v, step):
        late = (v + 3) // 6
        half = (v - 3) % 2
        base = G * (1 - (v - 3) // 2)
        row = base + half * (1 + step // 2)
        col = base + (1 - half) * step + half * (1 + (step + 1) // 2)
        return row * late + v * (1 - late), col * late + (G + step) * (1 - late)

    def near_tiles(turn):
        return [(turn, turn, True), (turn // 2, 1 + (turn + 1) // 2, False)]

    def other_tiles(turn):
        off = [(turn, G + j, False) for j in range(G)]
        off.append((G + turn // 2, G + 1 + (turn + 1) // 2, False))
        return [*off, (G + turn, G + turn, True)]

    def send_aid(tiles):
        for row, col, _ in tiles:
            ref = stage.at[2, slot_of(row, col)]
            pltpu.make_async_remote_copy(
                ref, ref, aid_send, aid_sem, device_id=device(y, x, 0), device_id_type=MESH
            ).start()

    def square_tiles(src, tiles, keep, early=False):
        def cross(row, col):
            part = chain(src, src, row, col, ((0, 2), (0, 1)))
            return part + part.T

        ready = [cross(row, col) if early and diag else None for row, col, diag in tiles]
        for (row, col, diag), part in zip(tiles, ready):
            if diag:
                part = cross(row, col) if part is None else part
                val = chain(src, src, row, col, ((1, 1), (0, 0))) + part
            else:
                val = chain(src, src, row, col, PASSES)
            put(buf_b, row, col, val, diag)
            if keep is not None:
                stage[2, slot_of(row, col) * (1 - keep) + UPPER * keep] = val
            sums[2] += fold(val * get(src, row, col)) * (1.0 if diag else 2.0)

    def square_a(job, before, between):
        own_job = (job + 1) // 2
        sums[2] = jnp.zeros_like(sums[2])

        def near(v, carry):
            pl.when((job == 0) & (v > 0))(lambda: send_aid(near_tiles(v - 1)))
            square_tiles(buf_a, near_tiles(v), own_job)
            return carry

        def other(v, carry):
            relay_early(job, before + v)
            pl.when((job == 0) & (v == 0))(lambda: send_aid(near_tiles(2)))
            pl.when((job == 0) & (v > 0))(lambda: send_aid(other_tiles(v - 1)))
            square_tiles(buf_a, other_tiles(v), own_job, True)
            return carry

        lax.fori_loop(0, 3, near, 0)
        between()
        lax.fori_loop(0, 3, other, 0)
        pl.when(job == 0)(lambda: send_aid(other_tiles(2)))

    def square_c(job, before):
        sums[2] = jnp.zeros_like(sums[2])

        def turn(v, carry):
            relay_early(job, before + v)
            square_tiles(buf_c, tiles_of(v), None)
            return carry

        lax.fori_loop(0, 3, turn, 0)

    def absorb():
        wait_for(stage.at[2, pl.ds(0, UPPER)], aid_sem)
        sums[2] = jnp.zeros_like(sums[2])

        def turn(v, carry):
            for step in range(3):
                row, col = unit(v, step)
                val = stage[2, slot_of(row, col)]
                put(buf_b, row, col, val, False)
                sums[2] += fold(val * get(buf_a, row, col)) * jnp.where(row == col, 1.0, 2.0)
            return carry

        lax.fori_loop(0, 7, turn, 0)

    def coefs():
        t1, t2, t3 = total(sums[0]), total(sums[1]), total(sums[2])
        coef = (t2 - t3) / (t1 - t2)
        inv = 1.0 / (1.0 - coef)
        return (1.0 - 2.0 * coef) * inv, (1.0 + coef) * inv, inv

    def count(val, diag):
        if diag:
            sums[0] += fold(val * eye)
        sums[1] += fold(val * val) * (1.0 if diag else 2.0)

    def combine(src, row, col, co):
        acc = chain(buf_b, src, row, col, PASSES)
        return co[0] * get(src, row, col) + co[1] * get(buf_b, row, col) - co[2] * acc

    def cube(src, dst, job, before):
        co = coefs()
        sums[0:2] = jnp.zeros_like(sums[0:2])

        def turn(v, carry):
            relay_early(job, before + v)
            for row, col, diag in tiles_of(v):
                val = combine(src, row, col, co)
                put(dst, row, col, val, diag)
                count(val, diag)
            return carry

        lax.fori_loop(0, 3, turn, 0)

    def cube_last(src, rnd):
        co = coefs()
        sums[0] = jnp.zeros_like(sums[0])

        def turn(v, carry):
            @pl.when(v > 0)
            def _():
                for step in range(3):
                    send_out(rnd, *unit(v - 1, step))

            for step in range(3):
                row, col = unit(v, step)
                val = combine(src, row, col, co)
                slot = slot_of(row, col)
                weight = jnp.where(row == col, 1.0, 2.0)
                sums[0] += fold(val * stage[rnd, slot]) * weight
                stage[rnd, slot] = val
            return carry

        lax.fori_loop(0, 7, turn, 0)
        for step in range(3):
            send_out(rnd, *unit(6, step))

    def one_job(job, carry):
        pl.when((job > 0) | (c == 1))(lambda: run_job(job))
        return carry

    def run_job(job):
        own_job = (job + 1) // 2
        rnd = job - 1
        put_in = (job + 2) % 3
        mat = own_job * (rnd * 8 + own) + (1 - own_job) * (8 + own - 1)
        wait_for(stage.at[put_in, pl.ds(0, 15)], so_sem.at[put_in])
        starts = job == 1 - c

        def far_block():
            wait_for(stage.at[put_in, pl.ds(15, 6), pl.ds(0, tile * 7 // 8)], r_sem.at[put_in])
            for i in range(G, NB):
                slot = slot_of(i, i)
                stage[put_in, slot, quarter:, :quarter] = stage[put_in, slot, :quarter, quarter:].T

        @pl.when(starts)
        def _():
            wait_for(t_land, t_sem)

        @pl.when(~starts)
        def _():
            far_block()
            part = fold(stage[put_in, slot_of(G, G)] * eye)
            for i in range(G + 1, NB):
                part += fold(stage[put_in, slot_of(i, i)] * eye)
            t_land[...] = part[:, :quarter] + part[:, quarter:]

        diag_sum = fold(stage[put_in, slot_of(0, 0)] * eye)
        for i in range(1, G):
            diag_sum += fold(stage[put_in, slot_of(i, i)] * eye)
        mean = (total(diag_sum) + total(t_land[...])) / order
        filled = occ[mat].astype(F32)
        scale = jnp.minimum(
            filled / (bounds[1, mat] - mean), (order - filled) / (mean - bounds[0, mat])
        )
        on_diag = (scale * mean + filled) / order
        slope = scale / order
        sums[0:2] = jnp.zeros_like(sums[0:2])

        def first(q, c_):
            v = q + 2 * (q // 3 - q // 6) - 4 * (q // 5)
            for step in range(3):
                row, col = unit(v, step)
                one = jnp.where(row == col, 1.0, 0.0)
                val = stage[put_in, slot_of(row, col)] * -slope + (on_diag * one) * eye
                put(buf_a, row, col, val, False)
                sums[0] += fold(val * eye) * one
                sums[1] += fold(val * val) * (2.0 - one)
            return c_

        lax.fori_loop(0, 5 + 2 * jnp.where(starts, 0, 1), first, 0)
        given = (job == 2) & (c == 0)
        mine = job > 0

        def step(s, c_):
            @pl.when(((s == 0) & ~given) | ((s == 2) & mine))
            def _():
                def between():
                    @pl.when(starts & (s == 0))
                    def _():
                        far_block()
                        lax.fori_loop(5, 7, first, 0)

                square_a(job, 6 * s, between)

            pl.when((s == 0) & given)(absorb)
            pl.when((s == 1) & mine)(lambda: square_c(job, 6))
            pl.when((s == 0) & mine)(lambda: cube(buf_a, buf_c, job, 3))
            pl.when((s == 1) & mine)(lambda: cube(buf_c, buf_a, job, 9))
            pl.when((s == 2) & mine)(lambda: finish(rnd, mat))
            return c_

        lax.fori_loop(0, STEPS, step, 0)

    def finish(rnd, mat):
        cube_last(buf_a, rnd)
        lane = lax.broadcasted_iota(jnp.int32, e_vec.shape[1:], 1)
        e_vec[rnd] = jnp.where(lane == mat, 2.0 * total(sums[0]), 0.0)
        for k in range(1, 8):
            pltpu.make_async_remote_copy(
                e_vec.at[rnd], ener.at[mat], e_send, e_sem,
                device_id=device(flip(y, k // 4), flip(x, (k // 2) % 2), flip(c, k % 2)),
                device_id_type=MESH,
            ).start()
        pltpu.make_async_copy(e_vec.at[rnd], ener.at[mat], e_sem).start()

    lax.fori_loop(0, 3, one_job, 0)

    pl.when(c == 0)(lambda: relays(1, 0, 0, G * G))
    relays(1, 1, 0, G * G)
    wait_for(ener.at[pl.ds(0, 14)], e_send)
    wait_for(ener, e_sem)

    def wait_tiles(quarters, sem):
        lead = 8 if quarters <= 288 else 16
        wait_for(ham.at[pl.ds(0, lead), pl.ds(0, quarters * tile // (12 * lead)), :], sem)

    @pl.when(c == 1)
    def _():
        wait_for(stage.at[2, pl.ds(0, UPPER)], aid_send)

    @pl.when(differ == 0)
    def _():
        pl.when(c == 0)(lambda: wait_tiles(105 + 72, in_send))
        pl.when(c == 1)(lambda: wait_tiles(105 + 48, in_send))
        wait_for(t_vec, t_send)
        wait_tiles(4 * 96, out_send)
        wait_tiles(4 * 63, land_sem)

    @pl.when(differ == 1)
    def _():
        pl.when(c == 0)(lambda: wait_tiles(108, in_send))
        pl.when(c == 1)(lambda: wait_tiles(72, in_send))
        wait_tiles(414, out_send)
        wait_tiles(4 * 108, land_sem)


RING = 4


def unpack_kernel(land, ener, out, energy, held, block, in_sem, out_sem):
    mats, tile = out.shape[0], land.shape[1]
    half = tile // 2
    x, c = lax.axis_index('row'), lax.axis_index('col')
    differ = flip(x, c)

    def load(mat, act):
        slot = mat % RING
        for kind, count in ((0, UPPER3), (1, G * G)):

            @pl.when(differ == kind)
            def _():
                act(
                    pltpu.make_async_copy(
                        land.at[pl.ds(mat * count, count)],
                        held.at[slot, pl.ds(0, count)],
                        in_sem.at[slot],
                    )
                )

    def store(mat):
        slot = mat % RING
        return pltpu.make_async_copy(block.at[slot], out.at[mat], out_sem.at[slot])

    def prime(mat, carry):
        load(mat, lambda copy: copy.start())
        return carry

    lax.fori_loop(0, RING, prime, 0)
    energy[...] = jnp.sum(ener[...], axis=0)[0, : energy.shape[0]]

    def turn(mat, carry):
        slot = mat % RING
        turned = flip((mat // 2) % 2, x)
        load(mat, lambda copy: copy.wait())
        pl.when(mat >= RING)(lambda: store(mat - RING).wait())

        def write(i, j, val):
            rows, cols = val.shape
            block[slot, pl.ds(i * half, rows), pl.ds(j * half, cols)] = val

        @pl.when(differ == 0)
        def _():
            for i in range(G):
                for j in range(i, G):
                    place = slot3_of(i, j)
                    if i == j:
                        top = held[slot, place, :half, :]
                        write(2 * i, 2 * i, top)
                        write(2 * i + 1, 2 * i, top[:, half:].T)
                        write(2 * i + 1, 2 * i + 1, held[slot, place, half:, half:])
                    else:
                        val = held[slot, place]
                        write(2 * i, 2 * j, val)
                        write(2 * j, 2 * i, val.T)

        @pl.when(differ * (1 - turned) == 1)
        def _():
            for i in range(G):
                for j in range(G):
                    write(2 * i, 2 * j, held[slot, i * G + j])

        @pl.when(differ * turned == 1)
        def _():
            for i in range(G):
                for j in range(G):
                    write(2 * j, 2 * i, held[slot, i * G + j].T)

        store(mat).start()
        pl.when(mat + RING < mats)(lambda: load(mat + RING, lambda copy: copy.start()))
        return carry

    lax.fori_loop(0, mats, turn, 0)
    for mat in range(mats - RING, mats):
        store(mat).wait()


def solution(mesh):
    def local_purify(ham, bounds, occ):
        mats, blk, _ = ham.shape
        tile = blk // G
        any_spec = pl.BlockSpec(memory_space=pltpu.HBM)
        smem = pl.BlockSpec(memory_space=pltpu.SMEM)
        limb = pltpu.VMEM((3, NB, NB, tile, tile), BF16)
        flops = 2 * 6 * 21 * 36 * 2 * tile**3
        land, ener = pl.pallas_call(
            main_kernel,
            out_shape=(
                jax.ShapeDtypeStruct((mats * G * G, tile, tile), F32),
                jax.ShapeDtypeStruct((mats, 8, 128), F32),
            ),
            in_specs=[smem, smem, any_spec],
            out_specs=(any_spec, any_spec),
            scratch_shapes=[
                limb, limb, limb,
                pltpu.VMEM((3, UPPER + 1, tile, tile), F32),
                pltpu.VMEM((3, 8, tile), F32),
                pltpu.VMEM((2, 8, 128), F32),
                pltpu.VMEM((2, NB, tile // 2, tile // 2), F32),
                pltpu.VMEM((2, 8, tile // 2), F32),
                pltpu.VMEM((8, tile // 2), F32),
                pltpu.SemaphoreType.DMA((3,)),
                pltpu.SemaphoreType.DMA((3,)),
                pltpu.SemaphoreType.DMA((2,)),
                pltpu.SemaphoreType.DMA,
                pltpu.SemaphoreType.DMA,
                pltpu.SemaphoreType.DMA,
                pltpu.SemaphoreType.DMA,
                pltpu.SemaphoreType.DMA,
                pltpu.SemaphoreType.DMA,
                pltpu.SemaphoreType.DMA((2, 2, G * G)),
                pltpu.SemaphoreType.DMA,
                pltpu.SemaphoreType.DMA,
                pltpu.SemaphoreType.DMA,
            ],
            compiler_params=pltpu.CompilerParams(
                collective_id=0, has_side_effects=True, vmem_limit_bytes=67043328
            ),
            cost_estimate=pl.CostEstimate(flops=flops, bytes_accessed=120 * 2**20, transcendentals=0),
            name='purify',
        )(bounds.T, occ, ham)

        return pl.pallas_call(
            unpack_kernel,
            out_shape=(
                jax.ShapeDtypeStruct(ham.shape, F32),
                jax.ShapeDtypeStruct((mats,), F32),
            ),
            in_specs=[any_spec, pl.BlockSpec(memory_space=pltpu.VMEM)],
            out_specs=(any_spec, pl.BlockSpec(memory_space=pltpu.VMEM)),
            scratch_shapes=[
                pltpu.VMEM((RING, G * G, tile, tile), F32),
                pltpu.VMEM((RING, blk, blk), F32),
                pltpu.SemaphoreType.DMA((RING,)),
                pltpu.SemaphoreType.DMA((RING,)),
            ],
            compiler_params=pltpu.CompilerParams(vmem_limit_bytes=40 * 2**20),
            cost_estimate=pl.CostEstimate(flops=10**6, bytes_accessed=75 * 2**20, transcendentals=0),
            name='unpack',
        )(land, ener)

    mat_spec = P('spin', 'row', 'col')
    return jax.shard_map(
        local_purify, mesh=mesh,
        in_specs=(mat_spec, P('spin', None), P('spin')),
        out_specs=(mat_spec, P('spin')), check_vma=False,
    )
```

```python
import functools

import jax
import jax.numpy as jnp
from jax import lax
from jax.experimental import pallas as pl
from jax.experimental.pallas import tpu as pltpu
from jax.sharding import PartitionSpec as P

STEPS = 3
G = 3
NB = 2 * G
UPPER = NB * (NB + 1) // 2
UPPER3 = G * (G + 1) // 2
OVER_X = 8
F32 = jnp.float32
BF16 = jnp.bfloat16
PASSES = ((0, 2), (2, 0), (1, 1), (0, 1), (1, 0), (0, 0))
MESH = pl.DeviceIdType.MESH


def slot_of(row, col):
    return row * (2 * NB - 1 - row) // 2 + col


def slot3_of(row, col):
    return row * (2 * G - 1 - row) // 2 + col


def upper_tile(row, step):
    wrap = (row + step) // NB
    other = row + step - NB * wrap
    return row * (1 - wrap) + other * wrap, other * (1 - wrap) + row * wrap


def limbs(val):
    high = val.astype(BF16)
    rest = val - high.astype(F32)
    mid = rest.astype(BF16)
    low = (rest - mid.astype(F32)).astype(BF16)
    return high, mid, low


def put(ref, row, col, val, diag):
    for piece, part in enumerate(limbs(val)):
        ref[piece, row, col] = part
    if not diag:
        for piece, part in enumerate(limbs(val.T)):
            ref[piece, col, row] = part


def get(ref, row, col):
    low = ref[1, row, col].astype(F32) + ref[2, row, col].astype(F32)
    return ref[0, row, col].astype(F32) + low


def chain(left, right, row, col, passes):
    acc = None
    for k in range(NB):
        for p, q in passes:
            part = jnp.dot(left[p, row, k], right[q, k, col], preferred_element_type=F32)
            acc = part if acc is None else acc + part
    return acc


def fold(val):
    size = val.shape[0]
    return jnp.sum(val.reshape(size // 8, 8, val.shape[1]), axis=0)


def total(val):
    return jnp.sum(jnp.sum(val, axis=0, keepdims=True), axis=1, keepdims=True)


def flip(bit, by):
    return bit + by - 2 * bit * by


def main_kernel(
    bounds, occ, ham, land, ener,
    buf_a, buf_b, buf_c, stage, sums, e_vec, corner, t_vec, t_land,
    so_sem, r_sem, corner_sem, t_sem, t_send, in_send, aid_sem, aid_send, land_sem, relay_sem, out_send, e_sem, e_send,
):
    tile = stage.shape[2]
    order = NB * tile
    y, x, c = lax.axis_index('depth'), lax.axis_index('row'), lax.axis_index('col')
    own = y * 4 + x * 2 + c
    differ = flip(x, c)

    def device(dy, dx, cd):
        return {'depth': dy, 'row': dx, 'col': cd}

    def wait_for(ref, sem):
        pltpu.make_async_copy(ref, ref, sem).wait()

    quarter = tile // 2
    rows = lax.broadcasted_iota(jnp.int32, (tile, tile), 0)
    cols = lax.broadcasted_iota(jnp.int32, (tile, tile), 1)
    eye = jnp.where(rows == cols, 1.0, 0.0).astype(F32)

    barrier = pltpu.get_barrier_semaphore()
    for k in range(1, 8):
        pl.semaphore_signal(
            barrier, inc=1,
            device_id=device(flip(y, k // 4), flip(x, (k // 2) % 2), flip(c, k % 2)),
            device_id_type=MESH,
        )

    @pl.when(differ == 0)
    def _():
        for e in range(2):
            for i in range(NB):
                spot = pl.ds(i * quarter, quarter)
                pltpu.make_async_copy(
                    ham.at[y * 4 + (1 - x) * 2 + 8 * e, spot, spot], corner.at[e, i], corner_sem.at[e]
                ).start()
        for e in range(2):
            wait_for(corner.at[e], corner_sem.at[e])
            part = fold(corner[e, 0] * eye[:quarter, :quarter])
            for i in range(1, NB):
                part += fold(corner[e, i] * eye[:quarter, :quarter])
            t_vec[e] = part

    pl.semaphore_wait(barrier, 7)

    @pl.when(differ == 0)
    def _():
        for e in range(2):
            pltpu.make_async_remote_copy(
                t_vec.at[e], t_land, t_send, t_sem,
                device_id=device(y, 1 - x, e), device_id_type=MESH,
            ).start()

    def h_tile(mat, i, j):
        return ham.at[mat, pl.ds(i * tile, tile), pl.ds(j * tile, tile)]

    def parts(diag):
        half = tile // 2
        if not diag:
            return [(slice(None), slice(None))]
        return [(pl.ds(0, half), slice(None)), (pl.ds(half, half), pl.ds(half, half))]

    diag_tiles = [(i, j) for i in range(G) for j in range(i, G)]

    def send_in(e, carry):
        late = e // 3
        aid = (e % 3) % 2 * (1 - late)
        cd = (1 - late) * ((e + 1) // 2) + late * (e - 3)
        mat = 8 * (aid + late) + cd * (1 - aid) + y * 4
        put_in = 2 * aid + late

        @pl.when(differ == 0)
        def _():
            for i, j in diag_tiles:
                for part in parts(i == j):
                    pltpu.make_async_remote_copy(
                        h_tile(mat + (1 - x) * 2, i, j).at[part],
                        stage.at[put_in, slot_of(G + i, G + j)].at[part],
                        in_send, r_sem.at[put_in],
                        device_id=device(y, 1 - x, cd), device_id_type=MESH,
                    ).start()

        def near(tiles, shift):
            for i, j in tiles:
                near_tile(i, j, shift)

        def near_row(i, carry_):
            for j in range(G):
                near_tile(i, j, G)
            return carry_

        def near_tile(i, j, shift):
            src = h_tile(mat + x * 2, i, j)
            dst = stage.at[put_in, slot_of(i, shift + j)]

            @pl.when(cd == c)
            def _():
                pltpu.make_async_copy(src, dst, so_sem.at[put_in]).start()

            @pl.when(cd != c)
            def _():
                pltpu.make_async_remote_copy(
                    src, dst, in_send, so_sem.at[put_in],
                    device_id=device(y, x, cd), device_id_type=MESH,
                ).start()

        pl.when(differ == 0)(lambda: near(diag_tiles, 0))

        @pl.when(differ == 1)
        def _():
            lax.fori_loop(0, G, near_row, 0)

        return carry

    lax.fori_loop(0, 5, send_in, 0)

    def send_out(rnd, row, col):
        mat = rnd * 8 + own
        src = stage.at[rnd, slot_of(row, col)]
        k_row, k_col = row // G, col // G

        def start(dy, xd, cd, dst, sem, diag=False):
            for part in parts(diag):
                pltpu.make_async_remote_copy(
                    src.at[part], dst.at[part], out_send, sem,
                    device_id=device(flip(y, dy), xd, cd), device_id_type=MESH,
                ).start()

        def keep(dst, diag=False):
            for part in parts(diag):
                pltpu.make_async_copy(src.at[part], dst.at[part], land_sem).start()

        @pl.when(k_row + k_col == 1)
        def _():
            place = row * G + col - G
            dst = land.at[mat * 9 + place]
            sem = relay_sem.at[rnd, c, place]

            @pl.when(place < OVER_X)
            def _():
                start(1, x, 1 - x, dst, sem)
                start(0, 1 - x, x, dst, land_sem)

            @pl.when(place >= OVER_X)
            def _():
                start(0, 1 - x, x, dst, sem)
                start(1, x, 1 - x, dst, land_sem)

            pl.when(differ == 1)(lambda: keep(dst))
            pl.when(differ == 0)(lambda: start(0, x, 1 - x, dst, land_sem))

        for diag in (False, True):
            same = (row == col) if diag else (row != col)

            @pl.when((k_row == 1) & same)
            def _():
                place = slot3_of(row - G, col - G)
                start(0, 1 - x, 1 - x, land.at[mat * 6 + place], relay_sem.at[rnd, c, place], diag)

            @pl.when((k_col == 0) & same)
            def _():
                dst = land.at[mat * 6 + slot3_of(row, col)]
                start(1, x, x, dst, land_sem, diag)
                pl.when(differ == 0)(lambda: keep(dst, diag))
                pl.when(differ == 1)(lambda: start(0, x, x, dst, land_sem, diag))

    def relay(rnd, cd, place):
        over_x = differ * (1 - place // OVER_X)
        owner = over_x * ((1 - y) * 4 + x * 2) + (1 - over_x) * (y * 4 + (1 - x) * 2) + cd
        dev = device(flip(y, 1 - over_x), flip(x, over_x), over_x * x + (1 - over_x) * c)
        tile_ref = land.at[(rnd * 8 + owner) * (UPPER3 + 3 * differ) + place]

        def pass_on(whole, diag):
            wait_for(whole, relay_sem.at[rnd, cd, place])
            for part in parts(diag):
                pltpu.make_async_remote_copy(
                    tile_ref.at[part], tile_ref.at[part], out_send, land_sem,
                    device_id=dev, device_id_type=MESH,
                ).start()

        on_diag = (differ == 0) & ((place == 0) | (place == 3) | (place == 5))
        pl.when(on_diag)(lambda: pass_on(tile_ref.at[pl.ds(0, tile * 3 // 4)], True))
        pl.when(~on_diag & (place < UPPER3 + 3 * differ))(lambda: pass_on(tile_ref, False))

    def relays(rnd, cd, low, count):
        def body(k, carry):
            relay(rnd, cd, low + k)
            return carry

        lax.fori_loop(0, count, body, 0)

    def relay_early(job, turn):
        one = (c == 1) & (turn >= 1) & (turn < 1 + G * G)
        two = (c == 0) & (turn >= 9) & (turn < 14)

        @pl.when((job == 2) & (one | two))
        def _():
            low = c * (turn - 1) + (1 - c) * 2 * (turn - 9)
            count = 1 + (1 - c) * (1 - turn // 13)

            def body(k, carry):
                relay(0, k % 2, low + k // 2)
                return carry

            lax.fori_loop(0, 2 * count, body, 0)

        @pl.when((job == 2) & (c == 1) & (turn >= 11) & (turn < 13 + differ))
        def _():
            nth = turn - 11
            low = differ * (3 * nth - nth // 2) + (1 - differ) * 2 * nth
            count = differ * (3 - nth + 3 * (nth // 2)) + (1 - differ) * (2 + 2 * nth)
            relays(1, 0, low, count)

    def tiles_of(turn):
        out = []
        for half in range(2):
            row = turn * 2 + half
            for step in range(3):
                out.append((*upper_tile(row, step), step == 0))
        out.append((turn, turn + 3, False))
        return sorted(out, key=lambda item: item[2])

    def unit(v, step):
        late = (v + 3) // 6
        half = (v - 3) % 2
        base = G * (1 - (v - 3) // 2)
        row = base + half * (1 + step // 2)
        col = base + (1 - half) * step + half * (1 + (step + 1) // 2)
        return row * late + v * (1 - late), col * late + (G + step) * (1 - late)

    def near_tiles(turn):
        return [(turn, turn, True), (turn // 2, 1 + (turn + 1) // 2, False)]

    def other_tiles(turn):
        off = [(turn, G + j, False) for j in range(G)]
        off.append((G + turn // 2, G + 1 + (turn + 1) // 2, False))
        return [*off, (G + turn, G + turn, True)]

    def send_aid(tiles):
        for row, col, _ in tiles:
            ref = stage.at[2, slot_of(row, col)]
            pltpu.make_async_remote_copy(
                ref, ref, aid_send, aid_sem, device_id=device(y, x, 0), device_id_type=MESH
            ).start()

    def square_tiles(src, tiles, keep, early=False):
        def cross(row, col):
            part = chain(src, src, row, col, ((0, 2), (0, 1)))
            return part + part.T

        ready = [cross(row, col) if early and diag else None for row, col, diag in tiles]
        for (row, col, diag), part in zip(tiles, ready):
            if diag:
                part = cross(row, col) if part is None else part
                val = chain(src, src, row, col, ((1, 1), (0, 0))) + part
            else:
                val = chain(src, src, row, col, PASSES)
            put(buf_b, row, col, val, diag)
            if keep is not None:
                stage[2, slot_of(row, col) * (1 - keep) + UPPER * keep] = val
            sums[2] += fold(val * get(src, row, col)) * (1.0 if diag else 2.0)

    def square_a(job, before, between):
        own_job = (job + 1) // 2
        sums[2] = jnp.zeros_like(sums[2])

        def near(v, carry):
            pl.when((job == 0) & (v > 0))(lambda: send_aid(near_tiles(v - 1)))
            square_tiles(buf_a, near_tiles(v), own_job)
            return carry

        def other(v, carry):
            relay_early(job, before + v)
            pl.when((job == 0) & (v == 0))(lambda: send_aid(near_tiles(2)))
            pl.when((job == 0) & (v > 0))(lambda: send_aid(other_tiles(v - 1)))
            square_tiles(buf_a, other_tiles(v), own_job, True)
            return carry

        lax.fori_loop(0, 3, near, 0)
        between()
        lax.fori_loop(0, 3, other, 0)
        pl.when(job == 0)(lambda: send_aid(other_tiles(2)))

    def square_c(job, before):
        sums[2] = jnp.zeros_like(sums[2])

        def turn(v, carry):
            relay_early(job, before + v)
            square_tiles(buf_c, tiles_of(v), None)
            return carry

        lax.fori_loop(0, 3, turn, 0)

    def absorb():
        wait_for(stage.at[2, pl.ds(0, UPPER)], aid_sem)
        sums[2] = jnp.zeros_like(sums[2])

        def turn(v, carry):
            for step in range(3):
                row, col = unit(v, step)
                val = stage[2, slot_of(row, col)]
                put(buf_b, row, col, val, False)
                sums[2] += fold(val * get(buf_a, row, col)) * jnp.where(row == col, 1.0, 2.0)
            return carry

        lax.fori_loop(0, 7, turn, 0)

    def coefs():
        t1, t2, t3 = total(sums[0]), total(sums[1]), total(sums[2])
        coef = (t2 - t3) / (t1 - t2)
        inv = 1.0 / (1.0 - coef)
        return (1.0 - 2.0 * coef) * inv, (1.0 + coef) * inv, inv

    def count(val, diag):
        if diag:
            sums[0] += fold(val * eye)
        sums[1] += fold(val * val) * (1.0 if diag else 2.0)

    def combine(src, row, col, co):
        acc = chain(buf_b, src, row, col, PASSES)
        return co[0] * get(src, row, col) + co[1] * get(buf_b, row, col) - co[2] * acc

    def cube(src, dst, job, before):
        co = coefs()
        sums[0:2] = jnp.zeros_like(sums[0:2])

        def turn(v, carry):
            relay_early(job, before + v)
            for row, col, diag in tiles_of(v):
                val = combine(src, row, col, co)
                put(dst, row, col, val, diag)
                count(val, diag)
            return carry

        lax.fori_loop(0, 3, turn, 0)

    def cube_last(src, rnd):
        co = coefs()
        sums[0] = jnp.zeros_like(sums[0])

        def when(v):
            pair = (v + 1) // 2 % 3
            return v + pair * (5 - 3 * pair)

        def turn(v, carry):
            @pl.when(v > 0)
            def _():
                for step in range(3):
                    send_out(rnd, *unit(when(v - 1), step))

            for step in range(3):
                row, col = unit(when(v), step)
                val = combine(src, row, col, co)
                slot = slot_of(row, col)
                weight = jnp.where(row == col, 1.0, 2.0)
                sums[0] += fold(val * stage[rnd, slot]) * weight
                stage[rnd, slot] = val
            return carry

        lax.fori_loop(0, 7, turn, 0)
        for step in range(3):
            send_out(rnd, *unit(when(6), step))

    def one_job(job, carry):
        pl.when((job > 0) | (c == 1))(lambda: run_job(job))
        return carry

    def run_job(job):
        own_job = (job + 1) // 2
        rnd = job - 1
        put_in = (job + 2) % 3
        mat = own_job * (rnd * 8 + own) + (1 - own_job) * (8 + own - 1)
        wait_for(stage.at[put_in, pl.ds(0, 15)], so_sem.at[put_in])
        starts = job == 1 - c

        def far_block():
            wait_for(stage.at[put_in, pl.ds(15, 6), pl.ds(0, tile * 7 // 8)], r_sem.at[put_in])
            for i in range(G, NB):
                slot = slot_of(i, i)
                stage[put_in, slot, quarter:, :quarter] = stage[put_in, slot, :quarter, quarter:].T

        @pl.when(starts)
        def _():
            wait_for(t_land, t_sem)

        @pl.when(~starts)
        def _():
            far_block()
            part = fold(stage[put_in, slot_of(G, G)] * eye)
            for i in range(G + 1, NB):
                part += fold(stage[put_in, slot_of(i, i)] * eye)
            t_land[...] = part[:, :quarter] + part[:, quarter:]

        diag_sum = fold(stage[put_in, slot_of(0, 0)] * eye)
        for i in range(1, G):
            diag_sum += fold(stage[put_in, slot_of(i, i)] * eye)
        mean = (total(diag_sum) + total(t_land[...])) / order
        filled = occ[mat].astype(F32)
        scale = jnp.minimum(
            filled / (bounds[1, mat] - mean), (order - filled) / (mean - bounds[0, mat])
        )
        on_diag = (scale * mean + filled) / order
        slope = scale / order
        sums[0:2] = jnp.zeros_like(sums[0:2])

        def first(q, c_):
            v = q + 2 * (q // 3 - q // 6) - 4 * (q // 5)
            for step in range(3):
                row, col = unit(v, step)
                one = jnp.where(row == col, 1.0, 0.0)
                val = stage[put_in, slot_of(row, col)] * -slope + (on_diag * one) * eye
                put(buf_a, row, col, val, False)
                sums[0] += fold(val * eye) * one
                sums[1] += fold(val * val) * (2.0 - one)
            return c_

        lax.fori_loop(0, 5 + 2 * jnp.where(starts, 0, 1), first, 0)
        given = (job == 2) & (c == 0)
        mine = job > 0

        def step(s, c_):
            @pl.when(((s == 0) & ~given) | ((s == 2) & mine))
            def _():
                def between():
                    @pl.when(starts & (s == 0))
                    def _():
                        far_block()
                        lax.fori_loop(5, 7, first, 0)

                square_a(job, 6 * s, between)

            pl.when((s == 0) & given)(absorb)
            pl.when((s == 1) & mine)(lambda: square_c(job, 6))
            pl.when((s == 0) & mine)(lambda: cube(buf_a, buf_c, job, 3))
            pl.when((s == 1) & mine)(lambda: cube(buf_c, buf_a, job, 9))
            pl.when((s == 2) & mine)(lambda: finish(rnd, mat))
            return c_

        lax.fori_loop(0, STEPS, step, 0)

    def finish(rnd, mat):
        cube_last(buf_a, rnd)
        lane = lax.broadcasted_iota(jnp.int32, e_vec.shape[1:], 1)
        e_vec[rnd] = jnp.where(lane == mat, 2.0 * total(sums[0]), 0.0)
        for k in range(1, 8):
            pltpu.make_async_remote_copy(
                e_vec.at[rnd], ener.at[mat], e_send, e_sem,
                device_id=device(flip(y, k // 4), flip(x, (k // 2) % 2), flip(c, k % 2)),
                device_id_type=MESH,
            ).start()
        pltpu.make_async_copy(e_vec.at[rnd], ener.at[mat], e_sem).start()

    lax.fori_loop(0, 3, one_job, 0)

    pl.when(c == 0)(lambda: relays(1, 0, 0, G * G))
    relays(1, 1, 0, G * G)
    wait_for(ener.at[pl.ds(0, 14)], e_send)
    wait_for(ener, e_sem)

    def wait_tiles(quarters, sem):
        lead = 8 if quarters <= 288 else 16
        wait_for(ham.at[pl.ds(0, lead), pl.ds(0, quarters * tile // (12 * lead)), :], sem)

    @pl.when(c == 1)
    def _():
        wait_for(stage.at[2, pl.ds(0, UPPER)], aid_send)

    @pl.when(differ == 0)
    def _():
        pl.when(c == 0)(lambda: wait_tiles(105 + 72, in_send))
        pl.when(c == 1)(lambda: wait_tiles(105 + 48, in_send))
        wait_for(t_vec, t_send)
        wait_tiles(4 * 96, out_send)
        wait_tiles(4 * 63, land_sem)

    @pl.when(differ == 1)
    def _():
        pl.when(c == 0)(lambda: wait_tiles(108, in_send))
        pl.when(c == 1)(lambda: wait_tiles(72, in_send))
        wait_tiles(414, out_send)
        wait_tiles(4 * 108, land_sem)


RING = 4


def unpack_kernel(land, ener, out, energy, held, block, in_sem, out_sem):
    mats, tile = out.shape[0], land.shape[1]
    half = tile // 2
    x, c = lax.axis_index('row'), lax.axis_index('col')
    differ = flip(x, c)

    def load(mat, act):
        slot = mat % RING
        for kind, count in ((0, UPPER3), (1, G * G)):

            @pl.when(differ == kind)
            def _():
                act(
                    pltpu.make_async_copy(
                        land.at[pl.ds(mat * count, count)],
                        held.at[slot, pl.ds(0, count)],
                        in_sem.at[slot],
                    )
                )

    def store(mat):
        slot = mat % RING
        return pltpu.make_async_copy(block.at[slot], out.at[mat], out_sem.at[slot])

    def prime(mat, carry):
        load(mat, lambda copy: copy.start())
        return carry

    lax.fori_loop(0, RING, prime, 0)
    energy[...] = jnp.sum(ener[...], axis=0)[0, : energy.shape[0]]

    def turn(mat, carry):
        slot = mat % RING
        turned = flip((mat // 2) % 2, x)
        load(mat, lambda copy: copy.wait())
        pl.when(mat >= RING)(lambda: store(mat - RING).wait())

        def write(i, j, val):
            rows, cols = val.shape
            block[slot, pl.ds(i * half, rows), pl.ds(j * half, cols)] = val

        @pl.when(differ == 0)
        def _():
            for i in range(G):
                for j in range(i, G):
                    place = slot3_of(i, j)
                    if i == j:
                        top = held[slot, place, :half, :]
                        write(2 * i, 2 * i, top)
                        write(2 * i + 1, 2 * i, top[:, half:].T)
                        write(2 * i + 1, 2 * i + 1, held[slot, place, half:, half:])
                    else:
                        val = held[slot, place]
                        write(2 * i, 2 * j, val)
                        write(2 * j, 2 * i, val.T)

        @pl.when(differ * (1 - turned) == 1)
        def _():
            for i in range(G):
                for j in range(G):
                    write(2 * i, 2 * j, held[slot, i * G + j])

        @pl.when(differ * turned == 1)
        def _():
            for i in range(G):
                for j in range(G):
                    write(2 * j, 2 * i, held[slot, i * G + j].T)

        store(mat).start()
        pl.when(mat + RING < mats)(lambda: load(mat + RING, lambda copy: copy.start()))
        return carry

    lax.fori_loop(0, mats, turn, 0)
    for mat in range(mats - RING, mats):
        store(mat).wait()


def solution(mesh):
    def local_purify(ham, bounds, occ):
        mats, blk, _ = ham.shape
        tile = blk // G
        any_spec = pl.BlockSpec(memory_space=pltpu.HBM)
        smem = pl.BlockSpec(memory_space=pltpu.SMEM)
        limb = pltpu.VMEM((3, NB, NB, tile, tile), BF16)
        flops = 2 * 6 * 21 * 36 * 2 * tile**3
        land, ener = pl.pallas_call(
            main_kernel,
            out_shape=(
                jax.ShapeDtypeStruct((mats * G * G, tile, tile), F32),
                jax.ShapeDtypeStruct((mats, 8, 128), F32),
            ),
            in_specs=[smem, smem, any_spec],
            out_specs=(any_spec, any_spec),
            scratch_shapes=[
                limb, limb, limb,
                pltpu.VMEM((3, UPPER + 1, tile, tile), F32),
                pltpu.VMEM((3, 8, tile), F32),
                pltpu.VMEM((2, 8, 128), F32),
                pltpu.VMEM((2, NB, tile // 2, tile // 2), F32),
                pltpu.VMEM((2, 8, tile // 2), F32),
                pltpu.VMEM((8, tile // 2), F32),
                pltpu.SemaphoreType.DMA((3,)),
                pltpu.SemaphoreType.DMA((3,)),
                pltpu.SemaphoreType.DMA((2,)),
                pltpu.SemaphoreType.DMA,
                pltpu.SemaphoreType.DMA,
                pltpu.SemaphoreType.DMA,
                pltpu.SemaphoreType.DMA,
                pltpu.SemaphoreType.DMA,
                pltpu.SemaphoreType.DMA,
                pltpu.SemaphoreType.DMA((2, 2, G * G)),
                pltpu.SemaphoreType.DMA,
                pltpu.SemaphoreType.DMA,
                pltpu.SemaphoreType.DMA,
            ],
            compiler_params=pltpu.CompilerParams(
                collective_id=0, has_side_effects=True, vmem_limit_bytes=67043328
            ),
            cost_estimate=pl.CostEstimate(flops=flops, bytes_accessed=120 * 2**20, transcendentals=0),
            name='purify',
        )(bounds.T, occ, ham)

        return pl.pallas_call(
            unpack_kernel,
            out_shape=(
                jax.ShapeDtypeStruct(ham.shape, F32),
                jax.ShapeDtypeStruct((mats,), F32),
            ),
            in_specs=[any_spec, pl.BlockSpec(memory_space=pltpu.VMEM)],
            out_specs=(any_spec, pl.BlockSpec(memory_space=pltpu.VMEM)),
            scratch_shapes=[
                pltpu.VMEM((RING, G * G, tile, tile), F32),
                pltpu.VMEM((RING, blk, blk), F32),
                pltpu.SemaphoreType.DMA((RING,)),
                pltpu.SemaphoreType.DMA((RING,)),
            ],
            compiler_params=pltpu.CompilerParams(vmem_limit_bytes=40 * 2**20),
            cost_estimate=pl.CostEstimate(flops=10**6, bytes_accessed=75 * 2**20, transcendentals=0),
            name='unpack',
        )(land, ener)

    mat_spec = P('spin', 'row', 'col')
    return jax.shard_map(
        local_purify, mesh=mesh,
        in_specs=(mat_spec, P('spin', None), P('spin')),
        out_specs=(mat_spec, P('spin')), check_vma=False,
    )
```

```python
import functools

import jax
import jax.numpy as jnp
from jax import lax
from jax.experimental import pallas as pl
from jax.experimental.pallas import tpu as pltpu
from jax.sharding import PartitionSpec as P

STEPS = 3
G = 3
NB = 2 * G
UPPER = NB * (NB + 1) // 2
UPPER3 = G * (G + 1) // 2
OVER_X = 7
F32 = jnp.float32
BF16 = jnp.bfloat16
PASSES = ((0, 2), (2, 0), (1, 1), (0, 1), (1, 0), (0, 0))
MESH = pl.DeviceIdType.MESH


def slot_of(row, col):
    return row * (2 * NB - 1 - row) // 2 + col


def slot3_of(row, col):
    return row * (2 * G - 1 - row) // 2 + col


def upper_tile(row, step):
    wrap = (row + step) // NB
    other = row + step - NB * wrap
    return row * (1 - wrap) + other * wrap, other * (1 - wrap) + row * wrap


def limbs(val):
    high = val.astype(BF16)
    rest = val - high.astype(F32)
    mid = rest.astype(BF16)
    low = (rest - mid.astype(F32)).astype(BF16)
    return high, mid, low


def put(ref, row, col, val, diag):
    for piece, part in enumerate(limbs(val)):
        ref[piece, row, col] = part
    if not diag:
        for piece, part in enumerate(limbs(val.T)):
            ref[piece, col, row] = part


def get(ref, row, col):
    low = ref[1, row, col].astype(F32) + ref[2, row, col].astype(F32)
    return ref[0, row, col].astype(F32) + low


def chain(left, right, row, col, passes):
    acc = None
    for k in range(NB):
        for p, q in passes:
            part = jnp.dot(left[p, row, k], right[q, k, col], preferred_element_type=F32)
            acc = part if acc is None else acc + part
    return acc


def fold(val):
    size = val.shape[0]
    return jnp.sum(val.reshape(size // 8, 8, val.shape[1]), axis=0)


def total(val):
    return jnp.sum(jnp.sum(val, axis=0, keepdims=True), axis=1, keepdims=True)


def flip(bit, by):
    return bit + by - 2 * bit * by


def main_kernel(
    bounds, occ, ham, land, ener,
    buf_a, buf_b, buf_c, stage, sums, e_vec, corner, t_vec, t_land,
    so_sem, r_sem, corner_sem, t_sem, t_send, in_send, aid_sem, aid_send, land_sem, relay_sem, out_send, e_sem, e_send,
):
    tile = stage.shape[2]
    order = NB * tile
    y, x, c = lax.axis_index('depth'), lax.axis_index('row'), lax.axis_index('col')
    own = y * 4 + x * 2 + c
    differ = flip(x, c)

    def device(dy, dx, cd):
        return {'depth': dy, 'row': dx, 'col': cd}

    def wait_for(ref, sem):
        pltpu.make_async_copy(ref, ref, sem).wait()

    quarter = tile // 2
    rows = lax.broadcasted_iota(jnp.int32, (tile, tile), 0)
    cols = lax.broadcasted_iota(jnp.int32, (tile, tile), 1)
    eye = jnp.where(rows == cols, 1.0, 0.0).astype(F32)

    barrier = pltpu.get_barrier_semaphore()
    for k in range(1, 8):
        pl.semaphore_signal(
            barrier, inc=1,
            device_id=device(flip(y, k // 4), flip(x, (k // 2) % 2), flip(c, k % 2)),
            device_id_type=MESH,
        )

    @pl.when(differ == 0)
    def _():
        for e in range(2):
            for i in range(NB):
                spot = pl.ds(i * quarter, quarter)
                pltpu.make_async_copy(
                    ham.at[y * 4 + (1 - x) * 2 + 8 * e, spot, spot], corner.at[e, i], corner_sem.at[e]
                ).start()
        for e in range(2):
            wait_for(corner.at[e], corner_sem.at[e])
            part = fold(corner[e, 0] * eye[:quarter, :quarter])
            for i in range(1, NB):
                part += fold(corner[e, i] * eye[:quarter, :quarter])
            t_vec[e] = part

    pl.semaphore_wait(barrier, 7)

    @pl.when(differ == 0)
    def _():
        for e in range(2):
            pltpu.make_async_remote_copy(
                t_vec.at[e], t_land, t_send, t_sem,
                device_id=device(y, 1 - x, e), device_id_type=MESH,
            ).start()

    def h_tile(mat, i, j):
        return ham.at[mat, pl.ds(i * tile, tile), pl.ds(j * tile, tile)]

    def parts(diag):
        half = tile // 2
        if not diag:
            return [(slice(None), slice(None))]
        return [(pl.ds(0, half), slice(None)), (pl.ds(half, half), pl.ds(half, half))]

    diag_tiles = [(i, j) for i in range(G) for j in range(i, G)]

    def send_in(e, carry):
        late = e // 3
        aid = (e % 3) % 2 * (1 - late)
        cd = (1 - late) * ((e + 1) // 2) + late * (e - 3)
        mat = 8 * (aid + late) + cd * (1 - aid) + y * 4
        put_in = 2 * aid + late

        @pl.when(differ == 0)
        def _():
            for i, j in diag_tiles:
                for part in parts(i == j):
                    pltpu.make_async_remote_copy(
                        h_tile(mat + (1 - x) * 2, i, j).at[part],
                        stage.at[put_in, slot_of(G + i, G + j)].at[part],
                        in_send, r_sem.at[put_in],
                        device_id=device(y, 1 - x, cd), device_id_type=MESH,
                    ).start()

        def near(tiles, shift):
            for i, j in tiles:
                near_tile(i, j, shift)

        def near_row(i, carry_):
            for j in range(G):
                near_tile(i, j, G)
            return carry_

        def near_tile(i, j, shift):
            src = h_tile(mat + x * 2, i, j)
            dst = stage.at[put_in, slot_of(i, shift + j)]

            @pl.when(cd == c)
            def _():
                pltpu.make_async_copy(src, dst, so_sem.at[put_in]).start()

            @pl.when(cd != c)
            def _():
                pltpu.make_async_remote_copy(
                    src, dst, in_send, so_sem.at[put_in],
                    device_id=device(y, x, cd), device_id_type=MESH,
                ).start()

        pl.when(differ == 0)(lambda: near(diag_tiles, 0))

        @pl.when(differ == 1)
        def _():
            lax.fori_loop(0, G, near_row, 0)

        return carry

    lax.fori_loop(0, 5, send_in, 0)

    def send_out(rnd, row, col):
        mat = rnd * 8 + own
        src = stage.at[rnd, slot_of(row, col)]
        k_row, k_col = row // G, col // G

        def start(dy, xd, cd, dst, sem, diag=False):
            for part in parts(diag):
                pltpu.make_async_remote_copy(
                    src.at[part], dst.at[part], out_send, sem,
                    device_id=device(flip(y, dy), xd, cd), device_id_type=MESH,
                ).start()

        def keep(dst, diag=False):
            for part in parts(diag):
                pltpu.make_async_copy(src.at[part], dst.at[part], land_sem).start()

        @pl.when(k_row + k_col == 1)
        def _():
            place = row * G + col - G
            dst = land.at[mat * 9 + place]
            sem = relay_sem.at[rnd, c, place]

            @pl.when(place < OVER_X)
            def _():
                start(1, x, 1 - x, dst, sem)
                start(0, 1 - x, x, dst, land_sem)

            @pl.when(place >= OVER_X)
            def _():
                start(0, 1 - x, x, dst, sem)
                start(1, x, 1 - x, dst, land_sem)

            pl.when(differ == 1)(lambda: keep(dst))
            pl.when(differ == 0)(lambda: start(0, x, 1 - x, dst, land_sem))

        for diag in (False, True):
            same = (row == col) if diag else (row != col)

            @pl.when((k_row == 1) & same)
            def _():
                place = slot3_of(row - G, col - G)
                start(0, 1 - x, 1 - x, land.at[mat * 6 + place], relay_sem.at[rnd, c, place], diag)

            @pl.when((k_col == 0) & same)
            def _():
                dst = land.at[mat * 6 + slot3_of(row, col)]
                start(1, x, x, dst, land_sem, diag)
                pl.when(differ == 0)(lambda: keep(dst, diag))
                pl.when(differ == 1)(lambda: start(0, x, x, dst, land_sem, diag))

    def relay(rnd, cd, place):
        over_x = differ * (1 - place // OVER_X)
        owner = over_x * ((1 - y) * 4 + x * 2) + (1 - over_x) * (y * 4 + (1 - x) * 2) + cd
        dev = device(flip(y, 1 - over_x), flip(x, over_x), over_x * x + (1 - over_x) * c)
        tile_ref = land.at[(rnd * 8 + owner) * (UPPER3 + 3 * differ) + place]

        def pass_on(whole, diag):
            wait_for(whole, relay_sem.at[rnd, cd, place])
            for part in parts(diag):
                pltpu.make_async_remote_copy(
                    tile_ref.at[part], tile_ref.at[part], out_send, land_sem,
                    device_id=dev, device_id_type=MESH,
                ).start()

        on_diag = (differ == 0) & ((place == 0) | (place == 3) | (place == 5))
        pl.when(on_diag)(lambda: pass_on(tile_ref.at[pl.ds(0, tile * 3 // 4)], True))
        pl.when(~on_diag & (place < UPPER3 + 3 * differ))(lambda: pass_on(tile_ref, False))

    def relays(rnd, cd, low, count):
        def body(k, carry):
            relay(rnd, cd, low + k)
            return carry

        lax.fori_loop(0, count, body, 0)

    def relay_early(job, turn):
        one = (c == 1) & (turn >= 1) & (turn < 1 + G * G)
        two = (c == 0) & (turn >= 9) & (turn < 14)

        @pl.when((job == 2) & (one | two))
        def _():
            low = c * (turn - 1) + (1 - c) * 2 * (turn - 9)
            count = 1 + (1 - c) * (1 - turn // 13)

            def body(k, carry):
                relay(0, k % 2, low + k // 2)
                return carry

            lax.fori_loop(0, 2 * count, body, 0)

        @pl.when((job == 2) & (c == 1) & (turn >= 11) & (turn < 13 + differ))
        def _():
            nth = turn - 11
            low = differ * (3 * nth - nth // 2) + (1 - differ) * 2 * nth
            count = differ * (3 - nth + 3 * (nth // 2)) + (1 - differ) * (2 + 2 * nth)
            relays(1, 0, low, count)

    def tiles_of(turn):
        out = []
        for half in range(2):
            row = turn * 2 + half
            for step in range(3):
                out.append((*upper_tile(row, step), step == 0))
        out.append((turn, turn + 3, False))
        return sorted(out, key=lambda item: item[2])

    def unit(v, step):
        late = (v + 3) // 6
        half = (v - 3) % 2
        base = G * (1 - (v - 3) // 2)
        row = base + half * (1 + step // 2)
        col = base + (1 - half) * step + half * (1 + (step + 1) // 2)
        return row * late + v * (1 - late), col * late + (G + step) * (1 - late)

    def near_tiles(turn):
        return [(turn, turn, True), (turn // 2, 1 + (turn + 1) // 2, False)]

    def other_tiles(turn):
        off = [(turn, G + j, False) for j in range(G)]
        off.append((G + turn // 2, G + 1 + (turn + 1) // 2, False))
        return [*off, (G + turn, G + turn, True)]

    def send_aid(tiles):
        for row, col, _ in tiles:
            ref = stage.at[2, slot_of(row, col)]
            pltpu.make_async_remote_copy(
                ref, ref, aid_send, aid_sem, device_id=device(y, x, 0), device_id_type=MESH
            ).start()

    def square_tiles(src, tiles, keep, early=False):
        def cross(row, col):
            part = chain(src, src, row, col, ((0, 2), (0, 1)))
            return part + part.T

        ready = [cross(row, col) if early and diag else None for row, col, diag in tiles]
        for (row, col, diag), part in zip(tiles, ready):
            if diag:
                part = cross(row, col) if part is None else part
                val = chain(src, src, row, col, ((1, 1), (0, 0))) + part
            else:
                val = chain(src, src, row, col, PASSES)
            put(buf_b, row, col, val, diag)
            if keep is not None:
                stage[2, slot_of(row, col) * (1 - keep) + UPPER * keep] = val
            sums[2] += fold(val * get(src, row, col)) * (1.0 if diag else 2.0)

    def square_a(job, before, between, given):
        keep = (job + 1) // 2 * jnp.where(given, 0, 1)
        aid = job == 0
        sums[2] = jnp.zeros_like(sums[2])

        def near(v, carry):
            pl.when(aid & (v > 1))(lambda: send_aid(near_tiles(v - 1)))
            square_tiles(buf_a, near_tiles(v), keep)
            return carry

        def other(v, carry):
            relay_early(job, before + v)
            pl.when(aid & (v == 0))(lambda: send_aid(near_tiles(2)))
            pl.when(aid & (v > 0))(lambda: send_aid(other_tiles(v - 1)))
            square_tiles(buf_a, other_tiles(v), keep)
            return carry

        lax.fori_loop(jnp.where(aid, 1, 0), jnp.where(given, 1, 3), near, 0)
        between()

        @pl.when(~given)
        def _():
            lax.fori_loop(0, 3, other, 0)
            pl.when(aid)(lambda: send_aid(other_tiles(2)))

    def square_c(job, before):
        sums[2] = jnp.zeros_like(sums[2])

        def turn(v, carry):
            relay_early(job, before + v)
            square_tiles(buf_c, tiles_of(v), None)
            return carry

        lax.fori_loop(0, 3, turn, 0)

    def absorb():
        wait_for(stage.at[2, pl.ds(0, UPPER - 2)], aid_sem)
        sums[2] = jnp.zeros_like(sums[2])

        def turn(v, carry):
            for step in range(3):
                row, col = unit(v, step)
                val = stage[2, slot_of(row, col)]
                put(buf_b, row, col, val, False)
                sums[2] += fold(val * get(buf_a, row, col)) * jnp.where(row == col, 1.0, 2.0)
            return carry

        lax.fori_loop(0, 7, turn, 0)

    def coefs():
        t1, t2, t3 = total(sums[0]), total(sums[1]), total(sums[2])
        coef = (t2 - t3) / (t1 - t2)
        inv = 1.0 / (1.0 - coef)
        return (1.0 - 2.0 * coef) * inv, (1.0 + coef) * inv, inv

    def count(val, diag):
        if diag:
            sums[0] += fold(val * eye)
        sums[1] += fold(val * val) * (1.0 if diag else 2.0)

    def combine(src, row, col, co):
        acc = chain(buf_b, src, row, col, PASSES)
        return co[0] * get(src, row, col) + co[1] * get(buf_b, row, col) - co[2] * acc

    def cube(src, dst, job, before):
        co = coefs()
        sums[0:2] = jnp.zeros_like(sums[0:2])

        def turn(v, carry):
            relay_early(job, before + v)
            for row, col, diag in tiles_of(v):
                val = combine(src, row, col, co)
                put(dst, row, col, val, diag)
                count(val, diag)
            return carry

        lax.fori_loop(0, 3, turn, 0)

    def cube_last(src, rnd):
        co = coefs()
        sums[0] = jnp.zeros_like(sums[0])

        def when(v):
            pair = (v + 1) // 2 % 3
            return v + pair * (5 - 3 * pair)

        def turn(v, carry):
            @pl.when(v > 0)
            def _():
                for step in range(3):
                    send_out(rnd, *unit(when(v - 1), step))

            for step in range(3):
                row, col = unit(when(v), step)
                val = combine(src, row, col, co)
                slot = slot_of(row, col)
                weight = jnp.where(row == col, 1.0, 2.0)
                sums[0] += fold(val * stage[rnd, slot]) * weight
                stage[rnd, slot] = val
            return carry

        lax.fori_loop(0, 7, turn, 0)
        for step in range(3):
            send_out(rnd, *unit(when(6), step))

    def one_job(job, carry):
        pl.when((job > 0) | (c == 1))(lambda: run_job(job))
        return carry

    def run_job(job):
        own_job = (job + 1) // 2
        rnd = job - 1
        put_in = (job + 2) % 3
        mat = own_job * (rnd * 8 + own) + (1 - own_job) * (8 + own - 1)
        wait_for(stage.at[put_in, pl.ds(0, 15)], so_sem.at[put_in])
        starts = job == 1 - c

        def far_block():
            wait_for(stage.at[put_in, pl.ds(15, 6), pl.ds(0, tile * 7 // 8)], r_sem.at[put_in])
            for i in range(G, NB):
                slot = slot_of(i, i)
                stage[put_in, slot, quarter:, :quarter] = stage[put_in, slot, :quarter, quarter:].T

        @pl.when(starts)
        def _():
            wait_for(t_land, t_sem)

        @pl.when(~starts)
        def _():
            far_block()
            part = fold(stage[put_in, slot_of(G, G)] * eye)
            for i in range(G + 1, NB):
                part += fold(stage[put_in, slot_of(i, i)] * eye)
            t_land[...] = part[:, :quarter] + part[:, quarter:]

        diag_sum = fold(stage[put_in, slot_of(0, 0)] * eye)
        for i in range(1, G):
            diag_sum += fold(stage[put_in, slot_of(i, i)] * eye)
        mean = (total(diag_sum) + total(t_land[...])) / order
        filled = occ[mat].astype(F32)
        scale = jnp.minimum(
            filled / (bounds[1, mat] - mean), (order - filled) / (mean - bounds[0, mat])
        )
        on_diag = (scale * mean + filled) / order
        slope = scale / order
        sums[0:2] = jnp.zeros_like(sums[0:2])

        def first(q, c_):
            v = q + 2 * (q // 3 - q // 6) - 4 * (q // 5)
            for step in range(3):
                row, col = unit(v, step)
                one = jnp.where(row == col, 1.0, 0.0)
                val = stage[put_in, slot_of(row, col)] * -slope + (on_diag * one) * eye
                put(buf_a, row, col, val, False)
                sums[0] += fold(val * eye) * one
                sums[1] += fold(val * val) * (2.0 - one)
            return c_

        lax.fori_loop(0, 5 + 2 * jnp.where(starts, 0, 1), first, 0)
        given = (job == 2) & (c == 0)
        mine = job > 0

        def step(s, c_):
            @pl.when((s == 0) | ((s == 2) & mine))
            def _():
                def between():
                    @pl.when(starts & (s == 0))
                    def _():
                        far_block()
                        lax.fori_loop(5, 7, first, 0)

                square_a(job, 6 * s, between, given & (s == 0))

            pl.when((s == 0) & given)(absorb)
            pl.when((s == 1) & mine)(lambda: square_c(job, 6))
            pl.when((s == 0) & mine)(lambda: cube(buf_a, buf_c, job, 3))
            pl.when((s == 1) & mine)(lambda: cube(buf_c, buf_a, job, 9))
            pl.when((s == 2) & mine)(lambda: finish(rnd, mat))
            return c_

        lax.fori_loop(0, STEPS, step, 0)

    def finish(rnd, mat):
        cube_last(buf_a, rnd)
        lane = lax.broadcasted_iota(jnp.int32, e_vec.shape[1:], 1)
        e_vec[rnd] = jnp.where(lane == mat, 2.0 * total(sums[0]), 0.0)
        for k in range(1, 8):
            pltpu.make_async_remote_copy(
                e_vec.at[rnd], ener.at[mat], e_send, e_sem,
                device_id=device(flip(y, k // 4), flip(x, (k // 2) % 2), flip(c, k % 2)),
                device_id_type=MESH,
            ).start()
        pltpu.make_async_copy(e_vec.at[rnd], ener.at[mat], e_sem).start()

    lax.fori_loop(0, 3, one_job, 0)

    pl.when(c == 0)(lambda: relays(1, 0, 0, G * G))
    relays(1, 1, 0, G * G)
    wait_for(ener.at[pl.ds(0, 14)], e_send)
    wait_for(ener, e_sem)

    def wait_tiles(quarters, sem):
        lead = 8 if quarters <= 288 else 16
        wait_for(ham.at[pl.ds(0, lead), pl.ds(0, quarters * tile // (12 * lead)), :], sem)

    @pl.when(c == 1)
    def _():
        wait_for(stage.at[2, pl.ds(0, UPPER - 2)], aid_send)

    @pl.when(differ == 0)
    def _():
        pl.when(c == 0)(lambda: wait_tiles(105 + 72, in_send))
        pl.when(c == 1)(lambda: wait_tiles(105 + 48, in_send))
        wait_for(t_vec, t_send)
        wait_tiles(4 * 96, out_send)
        wait_tiles(4 * 63, land_sem)

    @pl.when(differ == 1)
    def _():
        pl.when(c == 0)(lambda: wait_tiles(108, in_send))
        pl.when(c == 1)(lambda: wait_tiles(72, in_send))
        wait_tiles(414, out_send)
        wait_tiles(4 * 108, land_sem)


RING = 4
ROW_RING = 10


def ring(count, depth, load, store, work):
    def prime(unit, carry):
        load(unit, lambda copy: copy.start())
        return carry

    def turn(unit, carry):
        load(unit, None)
        pl.when(unit >= depth)(lambda: store(unit - depth).wait())
        work(unit)
        store(unit).start()
        pl.when(unit + depth < count)(lambda: load(unit + depth, lambda copy: copy.start()))
        return carry

    def drain(unit, carry):
        store(unit).wait()
        return carry

    lax.fori_loop(0, depth, prime, 0)
    lax.fori_loop(0, count, turn, 0)
    lax.fori_loop(count - depth, count, drain, 0)


def unpack_kernel(land, ener, out, energy, held, block, row_held, row_block, in_sem, out_sem, row_in, row_out):
    mats, tile = out.shape[0], land.shape[1]
    half = tile // 2
    x, c = lax.axis_index('row'), lax.axis_index('col')
    differ = flip(x, c)
    energy[...] = jnp.sum(ener[...], axis=0)[0, : energy.shape[0]]

    def load(mat, act):
        slot = mat % RING
        copy = pltpu.make_async_copy(
            land.at[pl.ds(mat * UPPER3, UPPER3)], held.at[slot], in_sem.at[slot]
        )
        copy.wait() if act is None else act(copy)

    def store(mat):
        slot = mat % RING
        return pltpu.make_async_copy(block.at[slot], out.at[mat], out_sem.at[slot])

    def mirror(mat):
        slot = mat % RING

        def write(i, j, val):
            rows, cols = val.shape
            block[slot, pl.ds(i * half, rows), pl.ds(j * half, cols)] = val

        for i in range(G):
            for j in range(i, G):
                place = slot3_of(i, j)
                if i == j:
                    top = held[slot, place, :half, :]
                    write(2 * i, 2 * i, top)
                    write(2 * i + 1, 2 * i, top[:, half:].T)
                    write(2 * i + 1, 2 * i + 1, held[slot, place, half:, half:])
                else:
                    val = held[slot, place]
                    write(2 * i, 2 * j, val)
                    write(2 * j, 2 * i, val.T)

    def turned(mat):
        return flip((mat // 2) % 2, x)

    def load_row(unit, act):
        slot, mat, row = unit % ROW_RING, unit // G, unit % G
        if act is None:
            pltpu.make_async_copy(row_held.at[slot], row_held.at[slot], row_in.at[slot]).wait()
            return
        flipped = turned(mat)
        for k in range(G):
            place = (1 - flipped) * (row * G + k) + flipped * (k * G + row)
            act(pltpu.make_async_copy(land.at[mat * G * G + place], row_held.at[slot, k], row_in.at[slot]))

    def store_row(unit):
        slot, mat, row = unit % ROW_RING, unit // G, unit % G
        return pltpu.make_async_copy(
            row_block.at[slot], out.at[mat, pl.ds(row * tile, tile), :], row_out.at[slot]
        )

    def turn_row(unit):
        slot = unit % ROW_RING
        flipped = turned(unit // G)

        @pl.when(flipped == 0)
        def _():
            for k in range(G):
                row_block[slot, :, pl.ds(k * tile, tile)] = row_held[slot, k]

        @pl.when(flipped == 1)
        def _():
            for k in range(G):
                row_block[slot, :, pl.ds(k * tile, tile)] = row_held[slot, k].T

    pl.when(differ == 0)(lambda: ring(mats, RING, load, store, mirror))
    pl.when(differ == 1)(lambda: ring(mats * G, ROW_RING, load_row, store_row, turn_row))


def solution(mesh):
    def local_purify(ham, bounds, occ):
        mats, blk, _ = ham.shape
        tile = blk // G
        any_spec = pl.BlockSpec(memory_space=pltpu.HBM)
        smem = pl.BlockSpec(memory_space=pltpu.SMEM)
        limb = pltpu.VMEM((3, NB, NB, tile, tile), BF16)
        flops = 2 * 6 * 21 * 36 * 2 * tile**3
        land, ener = pl.pallas_call(
            main_kernel,
            out_shape=(
                jax.ShapeDtypeStruct((mats * G * G, tile, tile), F32),
                jax.ShapeDtypeStruct((mats, 8, 128), F32),
            ),
            in_specs=[smem, smem, any_spec],
            out_specs=(any_spec, any_spec),
            scratch_shapes=[
                limb, limb, limb,
                pltpu.VMEM((3, UPPER + 1, tile, tile), F32),
                pltpu.VMEM((3, 8, tile), F32),
                pltpu.VMEM((2, 8, 128), F32),
                pltpu.VMEM((2, NB, tile // 2, tile // 2), F32),
                pltpu.VMEM((2, 8, tile // 2), F32),
                pltpu.VMEM((8, tile // 2), F32),
                pltpu.SemaphoreType.DMA((3,)),
                pltpu.SemaphoreType.DMA((3,)),
                pltpu.SemaphoreType.DMA((2,)),
                pltpu.SemaphoreType.DMA,
                pltpu.SemaphoreType.DMA,
                pltpu.SemaphoreType.DMA,
                pltpu.SemaphoreType.DMA,
                pltpu.SemaphoreType.DMA,
                pltpu.SemaphoreType.DMA,
                pltpu.SemaphoreType.DMA((2, 2, G * G)),
                pltpu.SemaphoreType.DMA,
                pltpu.SemaphoreType.DMA,
                pltpu.SemaphoreType.DMA,
            ],
            compiler_params=pltpu.CompilerParams(
                collective_id=0, has_side_effects=True, vmem_limit_bytes=67043328
            ),
            cost_estimate=pl.CostEstimate(flops=flops, bytes_accessed=120 * 2**20, transcendentals=0),
            name='purify',
        )(bounds.T, occ, ham)

        return pl.pallas_call(
            unpack_kernel,
            out_shape=(
                jax.ShapeDtypeStruct(ham.shape, F32),
                jax.ShapeDtypeStruct((mats,), F32),
            ),
            in_specs=[any_spec, pl.BlockSpec(memory_space=pltpu.VMEM)],
            out_specs=(any_spec, pl.BlockSpec(memory_space=pltpu.VMEM)),
            scratch_shapes=[
                pltpu.VMEM((RING, UPPER3, tile, tile), F32),
                pltpu.VMEM((RING, blk, blk), F32),
                pltpu.VMEM((ROW_RING, G, tile, tile), F32),
                pltpu.VMEM((ROW_RING, tile, blk), F32),
                pltpu.SemaphoreType.DMA((RING,)),
                pltpu.SemaphoreType.DMA((RING,)),
                pltpu.SemaphoreType.DMA((ROW_RING,)),
                pltpu.SemaphoreType.DMA((ROW_RING,)),
            ],
            compiler_params=pltpu.CompilerParams(vmem_limit_bytes=40 * 2**20),
            cost_estimate=pl.CostEstimate(flops=10**6, bytes_accessed=75 * 2**20, transcendentals=0),
            name='unpack',
        )(land, ener)

    mat_spec = P('spin', 'row', 'col')
    return jax.shard_map(
        local_purify, mesh=mesh,
        in_specs=(mat_spec, P('spin', None), P('spin')),
        out_specs=(mat_spec, P('spin')), check_vma=False,
    )
```

```python
import functools

import jax
import jax.numpy as jnp
from jax import lax
from jax.experimental import pallas as pl
from jax.experimental.pallas import tpu as pltpu
from jax.sharding import PartitionSpec as P

STEPS = 3
G = 3
NB = 2 * G
UPPER = NB * (NB + 1) // 2
UPPER3 = G * (G + 1) // 2
OVER_X = 7
F32 = jnp.float32
BF16 = jnp.bfloat16
PASSES = ((0, 2), (2, 0), (1, 1), (0, 1), (1, 0), (0, 0))
MESH = pl.DeviceIdType.MESH


def slot_of(row, col):
    return row * (2 * NB - 1 - row) // 2 + col


def slot3_of(row, col):
    return row * (2 * G - 1 - row) // 2 + col


def upper_tile(row, step):
    wrap = (row + step) // NB
    other = row + step - NB * wrap
    return row * (1 - wrap) + other * wrap, other * (1 - wrap) + row * wrap


def limbs(val):
    high = val.astype(BF16)
    rest = val - high.astype(F32)
    mid = rest.astype(BF16)
    low = (rest - mid.astype(F32)).astype(BF16)
    return high, mid, low


def put(ref, row, col, val, diag):
    for piece, part in enumerate(limbs(val)):
        ref[piece, row, col] = part
    if not diag:
        for piece, part in enumerate(limbs(val.T)):
            ref[piece, col, row] = part


def get(ref, row, col):
    low = ref[1, row, col].astype(F32) + ref[2, row, col].astype(F32)
    return ref[0, row, col].astype(F32) + low


def chain(left, right, row, col, passes):
    acc = None
    for k in range(NB):
        for p, q in passes:
            part = jnp.dot(left[p, row, k], right[q, k, col], preferred_element_type=F32)
            acc = part if acc is None else acc + part
    return acc


def fold(val):
    size = val.shape[0]
    return jnp.sum(val.reshape(size // 8, 8, val.shape[1]), axis=0)


def total(val):
    return jnp.sum(jnp.sum(val, axis=0, keepdims=True), axis=1, keepdims=True)


def flip(bit, by):
    return bit + by - 2 * bit * by


def main_kernel(
    bounds, occ, ham, land, ener,
    buf_a, buf_b, buf_c, stage, sums, e_vec, corner, t_vec, t_land,
    so_sem, r_sem, corner_sem, t_sem, t_send, in_send, aid_sem, aid_send, land_sem, relay_sem, out_send, e_sem, e_send,
):
    tile = stage.shape[2]
    order = NB * tile
    y, x, c = lax.axis_index('depth'), lax.axis_index('row'), lax.axis_index('col')
    own = y * 4 + x * 2 + c
    differ = flip(x, c)

    def device(dy, dx, cd):
        return {'depth': dy, 'row': dx, 'col': cd}

    def wait_for(ref, sem):
        pltpu.make_async_copy(ref, ref, sem).wait()

    quarter = tile // 2
    rows = lax.broadcasted_iota(jnp.int32, (tile, tile), 0)
    cols = lax.broadcasted_iota(jnp.int32, (tile, tile), 1)
    eye = jnp.where(rows == cols, 1.0, 0.0).astype(F32)

    barrier = pltpu.get_barrier_semaphore()
    for k in range(1, 8):
        pl.semaphore_signal(
            barrier, inc=1,
            device_id=device(flip(y, k // 4), flip(x, (k // 2) % 2), flip(c, k % 2)),
            device_id_type=MESH,
        )

    @pl.when(differ == 0)
    def _():
        for e in range(2):
            for i in range(NB):
                spot = pl.ds(i * quarter, quarter)
                pltpu.make_async_copy(
                    ham.at[y * 4 + (1 - x) * 2 + 8 * e, spot, spot], corner.at[e, i], corner_sem.at[e]
                ).start()
        for e in range(2):
            wait_for(corner.at[e], corner_sem.at[e])
            part = fold(corner[e, 0] * eye[:quarter, :quarter])
            for i in range(1, NB):
                part += fold(corner[e, i] * eye[:quarter, :quarter])
            t_vec[e] = part

    pl.semaphore_wait(barrier, 7)

    @pl.when(differ == 0)
    def _():
        for e in range(2):
            pltpu.make_async_remote_copy(
                t_vec.at[e], t_land, t_send, t_sem,
                device_id=device(y, 1 - x, e), device_id_type=MESH,
            ).start()

    def h_tile(mat, i, j):
        return ham.at[mat, pl.ds(i * tile, tile), pl.ds(j * tile, tile)]

    def parts(diag):
        half = tile // 2
        if not diag:
            return [(slice(None), slice(None))]
        return [(pl.ds(0, half), slice(None)), (pl.ds(half, half), pl.ds(half, half))]

    diag_tiles = [(i, j) for i in range(G) for j in range(i, G)]

    def send_in(e, carry):
        late = e // 3
        aid = (e % 3) % 2 * (1 - late)
        cd = (1 - late) * ((e + 1) // 2) + late * (e - 3)
        mat = 8 * (aid + late) + cd * (1 - aid) + y * 4
        put_in = 2 * aid + late

        @pl.when(differ == 0)
        def _():
            for i, j in diag_tiles:
                for part in parts(i == j):
                    pltpu.make_async_remote_copy(
                        h_tile(mat + (1 - x) * 2, i, j).at[part],
                        stage.at[put_in, slot_of(G + i, G + j)].at[part],
                        in_send, r_sem.at[put_in],
                        device_id=device(y, 1 - x, cd), device_id_type=MESH,
                    ).start()

        def near(tiles, shift):
            for i, j in tiles:
                near_tile(i, j, shift)

        def near_row(i, carry_):
            for j in range(G):
                near_tile(i, j, G)
            return carry_

        def near_tile(i, j, shift):
            src = h_tile(mat + x * 2, i, j)
            dst = stage.at[put_in, slot_of(i, shift + j)]

            @pl.when(cd == c)
            def _():
                pltpu.make_async_copy(src, dst, so_sem.at[put_in]).start()

            @pl.when(cd != c)
            def _():
                pltpu.make_async_remote_copy(
                    src, dst, in_send, so_sem.at[put_in],
                    device_id=device(y, x, cd), device_id_type=MESH,
                ).start()

        pl.when(differ == 0)(lambda: near(diag_tiles, 0))

        @pl.when(differ == 1)
        def _():
            lax.fori_loop(0, G, near_row, 0)

        return carry

    lax.fori_loop(0, 5, send_in, 0)

    def send_out(rnd, row, col):
        mat = rnd * 8 + own
        src = stage.at[rnd, slot_of(row, col)]
        k_row, k_col = row // G, col // G

        def start(dy, xd, cd, dst, sem, diag=False):
            for part in parts(diag):
                pltpu.make_async_remote_copy(
                    src.at[part], dst.at[part], out_send, sem,
                    device_id=device(flip(y, dy), xd, cd), device_id_type=MESH,
                ).start()

        def keep(dst, diag=False):
            for part in parts(diag):
                pltpu.make_async_copy(src.at[part], dst.at[part], land_sem).start()

        @pl.when(k_row + k_col == 1)
        def _():
            place = row * G + col - G
            dst = land.at[mat * 9 + place]
            sem = relay_sem.at[rnd, c, place]

            @pl.when(place < OVER_X)
            def _():
                start(1, x, 1 - x, dst, sem)
                start(0, 1 - x, x, dst, land_sem)

            @pl.when(place >= OVER_X)
            def _():
                start(0, 1 - x, x, dst, sem)
                start(1, x, 1 - x, dst, land_sem)

            pl.when(differ == 1)(lambda: keep(dst))
            pl.when(differ == 0)(lambda: start(0, x, 1 - x, dst, land_sem))

        for diag in (False, True):
            same = (row == col) if diag else (row != col)

            @pl.when((k_row == 1) & same)
            def _():
                place = slot3_of(row - G, col - G)
                start(0, 1 - x, 1 - x, land.at[mat * 6 + place], relay_sem.at[rnd, c, place], diag)

            @pl.when((k_col == 0) & same)
            def _():
                dst = land.at[mat * 6 + slot3_of(row, col)]
                start(1, x, x, dst, land_sem, diag)
                pl.when(differ == 0)(lambda: keep(dst, diag))
                pl.when(differ == 1)(lambda: start(0, x, x, dst, land_sem, diag))

    def relay(rnd, cd, place):
        over_x = differ * (1 - place // OVER_X)
        owner = over_x * ((1 - y) * 4 + x * 2) + (1 - over_x) * (y * 4 + (1 - x) * 2) + cd
        dev = device(flip(y, 1 - over_x), flip(x, over_x), over_x * x + (1 - over_x) * c)
        tile_ref = land.at[(rnd * 8 + owner) * (UPPER3 + 3 * differ) + place]

        def pass_on(whole, diag):
            wait_for(whole, relay_sem.at[rnd, cd, place])
            for part in parts(diag):
                pltpu.make_async_remote_copy(
                    tile_ref.at[part], tile_ref.at[part], out_send, land_sem,
                    device_id=dev, device_id_type=MESH,
                ).start()

        on_diag = (differ == 0) & ((place == 0) | (place == 3) | (place == 5))
        pl.when(on_diag)(lambda: pass_on(tile_ref.at[pl.ds(0, tile * 3 // 4)], True))
        pl.when(~on_diag & (place < UPPER3 + 3 * differ))(lambda: pass_on(tile_ref, False))

    def relays(rnd, cd, low, count):
        def body(k, carry):
            relay(rnd, cd, low + k)
            return carry

        lax.fori_loop(0, count, body, 0)

    def relay_early(job, turn):
        one = (c == 1) & (turn >= 1) & (turn < 1 + G * G)
        two = (c == 0) & (turn >= 9) & (turn < 14)

        @pl.when((job == 2) & (one | two))
        def _():
            low = c * (turn - 1) + (1 - c) * 2 * (turn - 9)
            count = 1 + (1 - c) * (1 - turn // 13)

            def body(k, carry):
                relay(0, k % 2, low + k // 2)
                return carry

            lax.fori_loop(0, 2 * count, body, 0)

        @pl.when((job == 2) & (c == 1) & (turn >= 12))
        def _():
            nth = turn - 12
            low = differ * (3 * nth - nth // 2) + (1 - differ) * 2 * nth
            relays(1, 0, low, differ * (3 - (nth + 1) // 2) + (1 - differ) * 2)

    def tiles_of(turn):
        out = []
        for half in range(2):
            row = turn * 2 + half
            for step in range(3):
                out.append((*upper_tile(row, step), step == 0))
        out.append((turn, turn + 3, False))
        return sorted(out, key=lambda item: item[2])

    def unit(v, step):
        late = (v + 3) // 6
        half = (v - 3) % 2
        base = G * (1 - (v - 3) // 2)
        row = base + half * (1 + step // 2)
        col = base + (1 - half) * step + half * (1 + (step + 1) // 2)
        return row * late + v * (1 - late), col * late + (G + step) * (1 - late)

    def near_tiles(turn):
        return [(turn, turn, True), (turn // 2, 1 + (turn + 1) // 2, False)]

    def other_tiles(turn):
        off = [(turn, G + j, False) for j in range(G)]
        off.append((G + turn // 2, G + 1 + (turn + 1) // 2, False))
        return [*off, (G + turn, G + turn, True)]

    def send_aid(tiles):
        for row, col, _ in tiles:
            ref = stage.at[2, slot_of(row, col)]
            pltpu.make_async_remote_copy(
                ref, ref, aid_send, aid_sem, device_id=device(y, x, 0), device_id_type=MESH
            ).start()

    def square_tiles(src, tiles, keep, early=False):
        def cross(row, col):
            part = chain(src, src, row, col, ((0, 2), (0, 1)))
            return part + part.T

        ready = [cross(row, col) if early and diag else None for row, col, diag in tiles]
        for (row, col, diag), part in zip(tiles, ready):
            if diag:
                part = cross(row, col) if part is None else part
                val = chain(src, src, row, col, ((1, 1), (0, 0))) + part
            else:
                val = chain(src, src, row, col, PASSES)
            put(buf_b, row, col, val, diag)
            if keep is not None:
                stage[2, slot_of(row, col) * (1 - keep) + UPPER * keep] = val
            sums[2] += fold(val * get(src, row, col)) * (1.0 if diag else 2.0)

    def square_a(job, before, between, given):
        keep = (job + 1) // 2 * jnp.where(given, 0, 1)
        aid = job == 0
        sums[2] = jnp.zeros_like(sums[2])

        def near(v, carry):
            pl.when(aid & (v > 1))(lambda: send_aid(near_tiles(v - 1)))
            square_tiles(buf_a, near_tiles(v), keep)
            return carry

        def other(v, carry):
            relay_early(job, before + v)
            pl.when(aid & (v == 0))(lambda: send_aid(near_tiles(2)))
            pl.when(aid & (v > 0))(lambda: send_aid(other_tiles(v - 1)))
            square_tiles(buf_a, other_tiles(v), keep)
            return carry

        lax.fori_loop(jnp.where(aid, 1, 0), jnp.where(given, 1, 3), near, 0)
        between()

        @pl.when(~given)
        def _():
            lax.fori_loop(0, 3, other, 0)
            pl.when(aid)(lambda: send_aid(other_tiles(2)))

    def square_c(job, before):
        sums[2] = jnp.zeros_like(sums[2])

        def turn(v, carry):
            relay_early(job, before + v)
            square_tiles(buf_c, tiles_of(v), None)
            return carry

        lax.fori_loop(0, 3, turn, 0)

    def absorb():
        wait_for(stage.at[2, pl.ds(0, UPPER - 2)], aid_sem)
        sums[2] = jnp.zeros_like(sums[2])

        def turn(v, carry):
            for step in range(3):
                row, col = unit(v, step)
                val = stage[2, slot_of(row, col)]
                put(buf_b, row, col, val, False)
                sums[2] += fold(val * get(buf_a, row, col)) * jnp.where(row == col, 1.0, 2.0)
            return carry

        lax.fori_loop(0, 7, turn, 0)

    def coefs():
        t1, t2, t3 = total(sums[0]), total(sums[1]), total(sums[2])
        coef = (t2 - t3) / (t1 - t2)
        inv = 1.0 / (1.0 - coef)
        return (1.0 - 2.0 * coef) * inv, (1.0 + coef) * inv, inv

    def count(val, diag):
        if diag:
            sums[0] += fold(val * eye)
        sums[1] += fold(val * val) * (1.0 if diag else 2.0)

    def combine(src, row, col, co):
        acc = chain(buf_b, src, row, col, PASSES)
        return co[0] * get(src, row, col) + co[1] * get(buf_b, row, col) - co[2] * acc

    def cube(src, dst, job, before):
        co = coefs()
        sums[0:2] = jnp.zeros_like(sums[0:2])

        def turn(v, carry):
            relay_early(job, before + v)
            for row, col, diag in tiles_of(v):
                val = combine(src, row, col, co)
                put(dst, row, col, val, diag)
                count(val, diag)
            return carry

        lax.fori_loop(0, 3, turn, 0)

    def cube_last(src, rnd):
        co = coefs()
        sums[0] = jnp.zeros_like(sums[0])

        def when(v):
            pair = (v + 1) // 2 % 3
            return v + pair * (5 - 3 * pair)

        def turn(v, carry):
            @pl.when(v > 0)
            def _():
                for step in range(3):
                    send_out(rnd, *unit(when(v - 1), step))

            @pl.when((rnd == 1) & (c * differ == 1) & (v >= 1) & (v < 3))
            def _():
                relays(1, 0, v + 6, 1)

            for step in range(3):
                row, col = unit(when(v), step)
                val = combine(src, row, col, co)
                slot = slot_of(row, col)
                weight = jnp.where(row == col, 1.0, 2.0)
                sums[0] += fold(val * stage[rnd, slot]) * weight
                stage[rnd, slot] = val
            return carry

        lax.fori_loop(0, 7, turn, 0)
        for step in range(3):
            send_out(rnd, *unit(when(6), step))

    def one_job(job, carry):
        pl.when((job > 0) | (c == 1))(lambda: run_job(job))
        return carry

    def run_job(job):
        own_job = (job + 1) // 2
        rnd = job - 1
        put_in = (job + 2) % 3
        mat = own_job * (rnd * 8 + own) + (1 - own_job) * (8 + own - 1)
        wait_for(stage.at[put_in, pl.ds(0, 15)], so_sem.at[put_in])
        starts = job == 1 - c

        def far_block():
            wait_for(stage.at[put_in, pl.ds(15, 6), pl.ds(0, tile * 7 // 8)], r_sem.at[put_in])
            for i in range(G, NB):
                slot = slot_of(i, i)
                stage[put_in, slot, quarter:, :quarter] = stage[put_in, slot, :quarter, quarter:].T

        @pl.when(starts)
        def _():
            wait_for(t_land, t_sem)

        @pl.when(~starts)
        def _():
            far_block()
            part = fold(stage[put_in, slot_of(G, G)] * eye)
            for i in range(G + 1, NB):
                part += fold(stage[put_in, slot_of(i, i)] * eye)
            t_land[...] = part[:, :quarter] + part[:, quarter:]

        diag_sum = fold(stage[put_in, slot_of(0, 0)] * eye)
        for i in range(1, G):
            diag_sum += fold(stage[put_in, slot_of(i, i)] * eye)
        mean = (total(diag_sum) + total(t_land[...])) / order
        filled = occ[mat].astype(F32)
        scale = jnp.minimum(
            filled / (bounds[1, mat] - mean), (order - filled) / (mean - bounds[0, mat])
        )
        on_diag = (scale * mean + filled) / order
        slope = scale / order
        sums[0:2] = jnp.zeros_like(sums[0:2])

        def first(q, c_):
            v = q + 2 * (q // 3 - q // 6) - 4 * (q // 5)
            for step in range(3):
                row, col = unit(v, step)
                one = jnp.where(row == col, 1.0, 0.0)
                val = stage[put_in, slot_of(row, col)] * -slope + (on_diag * one) * eye
                put(buf_a, row, col, val, False)
                sums[0] += fold(val * eye) * one
                sums[1] += fold(val * val) * (2.0 - one)
            return c_

        lax.fori_loop(0, 5 + 2 * jnp.where(starts, 0, 1), first, 0)
        given = (job == 2) & (c == 0)
        mine = job > 0

        def step(s, c_):
            @pl.when((s == 0) | ((s == 2) & mine))
            def _():
                def between():
                    @pl.when(starts & (s == 0))
                    def _():
                        far_block()
                        lax.fori_loop(5, 7, first, 0)

                square_a(job, 6 * s, between, given & (s == 0))

            pl.when((s == 0) & given)(absorb)
            pl.when((s == 1) & mine)(lambda: square_c(job, 6))
            pl.when((s == 0) & mine)(lambda: cube(buf_a, buf_c, job, 3))
            pl.when((s == 1) & mine)(lambda: cube(buf_c, buf_a, job, 9))
            pl.when((s == 2) & mine)(lambda: finish(rnd, mat))
            return c_

        lax.fori_loop(0, STEPS, step, 0)

    def finish(rnd, mat):
        cube_last(buf_a, rnd)
        lane = lax.broadcasted_iota(jnp.int32, e_vec.shape[1:], 1)
        e_vec[rnd] = jnp.where(lane == mat, 2.0 * total(sums[0]), 0.0)
        for k in range(1, 8):
            pltpu.make_async_remote_copy(
                e_vec.at[rnd], ener.at[mat], e_send, e_sem,
                device_id=device(flip(y, k // 4), flip(x, (k // 2) % 2), flip(c, k % 2)),
                device_id_type=MESH,
            ).start()
        pltpu.make_async_copy(e_vec.at[rnd], ener.at[mat], e_sem).start()

    lax.fori_loop(0, 3, one_job, 0)

    pl.when(c == 0)(lambda: relays(1, 0, 0, G * G))
    relays(1, 1, 0, G * G)
    wait_for(ener.at[pl.ds(0, 14)], e_send)
    wait_for(ener, e_sem)

    def wait_tiles(quarters, sem):
        lead = 8 if quarters <= 288 else 16
        wait_for(ham.at[pl.ds(0, lead), pl.ds(0, quarters * tile // (12 * lead)), :], sem)

    @pl.when(c == 1)
    def _():
        wait_for(stage.at[2, pl.ds(0, UPPER - 2)], aid_send)

    @pl.when(differ == 0)
    def _():
        pl.when(c == 0)(lambda: wait_tiles(105 + 72, in_send))
        pl.when(c == 1)(lambda: wait_tiles(105 + 48, in_send))
        wait_for(t_vec, t_send)
        wait_tiles(4 * 96, out_send)
        wait_tiles(4 * 63, land_sem)

    @pl.when(differ == 1)
    def _():
        pl.when(c == 0)(lambda: wait_tiles(108, in_send))
        pl.when(c == 1)(lambda: wait_tiles(72, in_send))
        wait_tiles(414, out_send)
        wait_tiles(4 * 108, land_sem)


RING = 4
ROW_RING = 10


def ring(count, depth, load, store, work):
    def prime(unit, carry):
        load(unit, lambda copy: copy.start())
        return carry

    def turn(unit, carry):
        load(unit, None)
        pl.when(unit >= depth)(lambda: store(unit - depth).wait())
        work(unit)
        store(unit).start()
        pl.when(unit + depth < count)(lambda: load(unit + depth, lambda copy: copy.start()))
        return carry

    def drain(unit, carry):
        store(unit).wait()
        return carry

    lax.fori_loop(0, depth, prime, 0)
    lax.fori_loop(0, count, turn, 0)
    lax.fori_loop(count - depth, count, drain, 0)


def unpack_kernel(land, ener, out, energy, held, block, row_held, row_block, in_sem, out_sem, row_in, row_out):
    mats, tile = out.shape[0], land.shape[1]
    half = tile // 2
    x, c = lax.axis_index('row'), lax.axis_index('col')
    differ = flip(x, c)
    energy[...] = jnp.sum(ener[...], axis=0)[0, : energy.shape[0]]

    def load(mat, act):
        slot = mat % RING
        copy = pltpu.make_async_copy(
            land.at[pl.ds(mat * UPPER3, UPPER3)], held.at[slot], in_sem.at[slot]
        )
        copy.wait() if act is None else act(copy)

    def store(mat):
        slot = mat % RING
        return pltpu.make_async_copy(block.at[slot], out.at[mat], out_sem.at[slot])

    def mirror(mat):
        slot = mat % RING

        def write(i, j, val):
            rows, cols = val.shape
            block[slot, pl.ds(i * half, rows), pl.ds(j * half, cols)] = val

        for i in range(G):
            for j in range(i, G):
                place = slot3_of(i, j)
                if i == j:
                    top = held[slot, place, :half, :]
                    write(2 * i, 2 * i, top)
                    write(2 * i + 1, 2 * i, top[:, half:].T)
                    write(2 * i + 1, 2 * i + 1, held[slot, place, half:, half:])
                else:
                    val = held[slot, place]
                    write(2 * i, 2 * j, val)
                    write(2 * j, 2 * i, val.T)

    def turned(mat):
        return flip((mat // 2) % 2, x)

    def load_row(unit, act):
        slot, mat, row = unit % ROW_RING, unit // G, unit % G
        if act is None:
            pltpu.make_async_copy(row_held.at[slot], row_held.at[slot], row_in.at[slot]).wait()
            return
        flipped = turned(mat)
        for k in range(G):
            place = (1 - flipped) * (row * G + k) + flipped * (k * G + row)
            act(pltpu.make_async_copy(land.at[mat * G * G + place], row_held.at[slot, k], row_in.at[slot]))

    def store_row(unit):
        slot, mat, row = unit % ROW_RING, unit // G, unit % G
        return pltpu.make_async_copy(
            row_block.at[slot], out.at[mat, pl.ds(row * tile, tile), :], row_out.at[slot]
        )

    def turn_row(unit):
        slot = unit % ROW_RING
        flipped = turned(unit // G)

        @pl.when(flipped == 0)
        def _():
            for k in range(G):
                row_block[slot, :, pl.ds(k * tile, tile)] = row_held[slot, k]

        @pl.when(flipped == 1)
        def _():
            for k in range(G):
                row_block[slot, :, pl.ds(k * tile, tile)] = row_held[slot, k].T

    pl.when(differ == 0)(lambda: ring(mats, RING, load, store, mirror))
    pl.when(differ == 1)(lambda: ring(mats * G, ROW_RING, load_row, store_row, turn_row))


def solution(mesh):
    def local_purify(ham, bounds, occ):
        mats, blk, _ = ham.shape
        tile = blk // G
        any_spec = pl.BlockSpec(memory_space=pltpu.HBM)
        smem = pl.BlockSpec(memory_space=pltpu.SMEM)
        limb = pltpu.VMEM((3, NB, NB, tile, tile), BF16)
        flops = 2 * 6 * 21 * 36 * 2 * tile**3
        land, ener = pl.pallas_call(
            main_kernel,
            out_shape=(
                jax.ShapeDtypeStruct((mats * G * G, tile, tile), F32),
                jax.ShapeDtypeStruct((mats, 8, 128), F32),
            ),
            in_specs=[smem, smem, any_spec],
            out_specs=(any_spec, any_spec),
            scratch_shapes=[
                limb, limb, limb,
                pltpu.VMEM((3, UPPER + 1, tile, tile), F32),
                pltpu.VMEM((3, 8, tile), F32),
                pltpu.VMEM((2, 8, 128), F32),
                pltpu.VMEM((2, NB, tile // 2, tile // 2), F32),
                pltpu.VMEM((2, 8, tile // 2), F32),
                pltpu.VMEM((8, tile // 2), F32),
                pltpu.SemaphoreType.DMA((3,)),
                pltpu.SemaphoreType.DMA((3,)),
                pltpu.SemaphoreType.DMA((2,)),
                pltpu.SemaphoreType.DMA,
                pltpu.SemaphoreType.DMA,
                pltpu.SemaphoreType.DMA,
                pltpu.SemaphoreType.DMA,
                pltpu.SemaphoreType.DMA,
                pltpu.SemaphoreType.DMA,
                pltpu.SemaphoreType.DMA((2, 2, G * G)),
                pltpu.SemaphoreType.DMA,
                pltpu.SemaphoreType.DMA,
                pltpu.SemaphoreType.DMA,
            ],
            compiler_params=pltpu.CompilerParams(
                collective_id=0, has_side_effects=True, vmem_limit_bytes=67043328
            ),
            cost_estimate=pl.CostEstimate(flops=flops, bytes_accessed=120 * 2**20, transcendentals=0),
            name='purify',
        )(bounds.T, occ, ham)

        return pl.pallas_call(
            unpack_kernel,
            out_shape=(
                jax.ShapeDtypeStruct(ham.shape, F32),
                jax.ShapeDtypeStruct((mats,), F32),
            ),
            in_specs=[any_spec, pl.BlockSpec(memory_space=pltpu.VMEM)],
            out_specs=(any_spec, pl.BlockSpec(memory_space=pltpu.VMEM)),
            scratch_shapes=[
                pltpu.VMEM((RING, UPPER3, tile, tile), F32),
                pltpu.VMEM((RING, blk, blk), F32),
                pltpu.VMEM((ROW_RING, G, tile, tile), F32),
                pltpu.VMEM((ROW_RING, tile, blk), F32),
                pltpu.SemaphoreType.DMA((RING,)),
                pltpu.SemaphoreType.DMA((RING,)),
                pltpu.SemaphoreType.DMA((ROW_RING,)),
                pltpu.SemaphoreType.DMA((ROW_RING,)),
            ],
            compiler_params=pltpu.CompilerParams(vmem_limit_bytes=40 * 2**20),
            cost_estimate=pl.CostEstimate(flops=10**6, bytes_accessed=75 * 2**20, transcendentals=0),
            name='unpack',
        )(land, ener)

    mat_spec = P('spin', 'row', 'col')
    return jax.shard_map(
        local_purify, mesh=mesh,
        in_specs=(mat_spec, P('spin', None), P('spin')),
        out_specs=(mat_spec, P('spin')), check_vma=False,
    )
```

```python
import functools

import jax
import jax.numpy as jnp
from jax import lax
from jax.experimental import pallas as pl
from jax.experimental.pallas import tpu as pltpu
from jax.sharding import PartitionSpec as P

STEPS = 3
G = 3
NB = 2 * G
UPPER = NB * (NB + 1) // 2
UPPER3 = G * (G + 1) // 2
OVER_X = 8
F32 = jnp.float32
BF16 = jnp.bfloat16
PASSES = ((0, 2), (2, 0), (1, 1), (0, 1), (1, 0), (0, 0))
MESH = pl.DeviceIdType.MESH


def slot_of(row, col):
    return row * (2 * NB - 1 - row) // 2 + col


def slot3_of(row, col):
    return row * (2 * G - 1 - row) // 2 + col


def upper_tile(row, step):
    wrap = (row + step) // NB
    other = row + step - NB * wrap
    return row * (1 - wrap) + other * wrap, other * (1 - wrap) + row * wrap


def limbs(val):
    high = val.astype(BF16)
    rest = val - high.astype(F32)
    mid = rest.astype(BF16)
    low = (rest - mid.astype(F32)).astype(BF16)
    return high, mid, low


def put(ref, row, col, val, diag):
    for piece, part in enumerate(limbs(val)):
        ref[piece, row, col] = part
    if not diag:
        for piece, part in enumerate(limbs(val.T)):
            ref[piece, col, row] = part


def get(ref, row, col):
    low = ref[1, row, col].astype(F32) + ref[2, row, col].astype(F32)
    return ref[0, row, col].astype(F32) + low


def chain(left, right, row, col, passes):
    acc = None
    for k in range(NB):
        for p, q in passes:
            part = jnp.dot(left[p, row, k], right[q, k, col], preferred_element_type=F32)
            acc = part if acc is None else acc + part
    return acc


def fold(val):
    size = val.shape[0]
    return jnp.sum(val.reshape(size // 8, 8, val.shape[1]), axis=0)


def total(val):
    return jnp.sum(jnp.sum(val, axis=0, keepdims=True), axis=1, keepdims=True)


def flip(bit, by):
    return bit + by - 2 * bit * by


def main_kernel(
    bounds, occ, ham, land, ener,
    buf_a, buf_b, buf_c, stage, sums, e_vec, corner, t_vec, t_land,
    so_sem, r_sem, corner_sem, t_sem, t_send, in_send, aid_sem, aid_send, land_sem, relay_sem, out_send, e_sem, e_send,
):
    tile = stage.shape[2]
    order = NB * tile
    y, x, c = lax.axis_index('depth'), lax.axis_index('row'), lax.axis_index('col')
    own = y * 4 + x * 2 + c
    differ = flip(x, c)

    def device(dy, dx, cd):
        return {'depth': dy, 'row': dx, 'col': cd}

    def wait_for(ref, sem):
        pltpu.make_async_copy(ref, ref, sem).wait()

    quarter = tile // 2
    rows = lax.broadcasted_iota(jnp.int32, (tile, tile), 0)
    cols = lax.broadcasted_iota(jnp.int32, (tile, tile), 1)
    eye = jnp.where(rows == cols, 1.0, 0.0).astype(F32)

    barrier = pltpu.get_barrier_semaphore()
    for k in range(1, 8):
        pl.semaphore_signal(
            barrier, inc=1,
            device_id=device(flip(y, k // 4), flip(x, (k // 2) % 2), flip(c, k % 2)),
            device_id_type=MESH,
        )

    @pl.when(differ == 0)
    def _():
        for e in range(2):
            for i in range(NB):
                spot = pl.ds(i * quarter, quarter)
                pltpu.make_async_copy(
                    ham.at[y * 4 + (1 - x) * 2 + 8 * e, spot, spot], corner.at[e, i], corner_sem.at[e]
                ).start()
        for e in range(2):
            wait_for(corner.at[e], corner_sem.at[e])
            part = fold(corner[e, 0] * eye[:quarter, :quarter])
            for i in range(1, NB):
                part += fold(corner[e, i] * eye[:quarter, :quarter])
            t_vec[e] = part

    pl.semaphore_wait(barrier, 7)

    @pl.when(differ == 0)
    def _():
        for e in range(2):
            pltpu.make_async_remote_copy(
                t_vec.at[e], t_land, t_send, t_sem,
                device_id=device(y, 1 - x, e), device_id_type=MESH,
            ).start()

    def h_tile(mat, i, j):
        return ham.at[mat, pl.ds(i * tile, tile), pl.ds(j * tile, tile)]

    def parts(diag):
        half = tile // 2
        if not diag:
            return [(slice(None), slice(None))]
        return [(pl.ds(0, half), slice(None)), (pl.ds(half, half), pl.ds(half, half))]

    diag_tiles = [(i, j) for i in range(G) for j in range(i, G)]

    def send_in(e, carry):
        late = e // 3
        aid = (e % 3) % 2 * (1 - late)
        cd = (1 - late) * ((e + 1) // 2) + late * (e - 3)
        mat = 8 * (aid + late) + cd * (1 - aid) + y * 4
        put_in = 2 * aid + late

        @pl.when(differ == 0)
        def _():
            for i, j in diag_tiles:
                for part in parts(i == j):
                    pltpu.make_async_remote_copy(
                        h_tile(mat + (1 - x) * 2, i, j).at[part],
                        stage.at[put_in, slot_of(G + i, G + j)].at[part],
                        in_send, r_sem.at[put_in],
                        device_id=device(y, 1 - x, cd), device_id_type=MESH,
                    ).start()

        def near(tiles, shift):
            for i, j in tiles:
                near_tile(i, j, shift)

        def near_row(i, carry_):
            for j in range(G):
                near_tile(i, j, G)
            return carry_

        def near_tile(i, j, shift):
            src = h_tile(mat + x * 2, i, j)
            dst = stage.at[put_in, slot_of(i, shift + j)]

            @pl.when(cd == c)
            def _():
                pltpu.make_async_copy(src, dst, so_sem.at[put_in]).start()

            @pl.when(cd != c)
            def _():
                pltpu.make_async_remote_copy(
                    src, dst, in_send, so_sem.at[put_in],
                    device_id=device(y, x, cd), device_id_type=MESH,
                ).start()

        pl.when(differ == 0)(lambda: near(diag_tiles, 0))

        @pl.when(differ == 1)
        def _():
            lax.fori_loop(0, G, near_row, 0)

        return carry

    lax.fori_loop(0, 5, send_in, 0)

    def send_out(rnd, group):
        mat = rnd * 8 + own

        def start(src, dy, xd, cd, dst, sem, diag=False):
            for part in parts(diag):
                pltpu.make_async_remote_copy(
                    src.at[part], dst.at[part], out_send, sem,
                    device_id=device(flip(y, dy), xd, cd), device_id_type=MESH,
                ).start()

        def keep(src, dst, diag=False):
            for part in parts(diag):
                pltpu.make_async_copy(src.at[part], dst.at[part], land_sem).start()

        @pl.when(group < G)
        def _():
            for step in range(3):
                place = group * G + step
                src, dst = stage.at[rnd, slot_of(group, G + step)], land.at[mat * 9 + place]
                sem = relay_sem.at[rnd, c, place]

                def first_over_y(src=src, dst=dst, sem=sem):
                    start(src, 1, x, 1 - x, dst, sem)
                    start(src, 0, 1 - x, x, dst, land_sem)

                def first_over_x(src=src, dst=dst, sem=sem):
                    start(src, 0, 1 - x, x, dst, sem)
                    start(src, 1, x, 1 - x, dst, land_sem)

                if step == 0:
                    first_over_y()
                else:
                    pl.when(place + c < OVER_X)(first_over_y)
                    pl.when(place + c >= OVER_X)(first_over_x)
                pl.when(differ == 1)(functools.partial(keep, src, dst))
                pl.when(differ == 0)(functools.partial(start, src, 0, x, 1 - x, dst, land_sem))

        half = (group - G) % 2
        for step in range(3):
            i, j = half * (1 + step // 2), (1 - half) * step + half * (1 + (step + 1) // 2)
            place = slot3_of(i, j)
            dst = land.at[mat * UPPER3 + place]

            def far(diag, i=i, j=j, place=place, dst=dst):
                src = stage.at[rnd, slot_of(G + i, G + j)]
                start(src, 0, 1 - x, 1 - x, dst, relay_sem.at[rnd, c, place], diag)

            def near(diag, i=i, j=j, dst=dst):
                src = stage.at[rnd, slot_of(i, j)]
                start(src, 1, x, x, dst, land_sem, diag)
                pl.when(differ == 0)(lambda: keep(src, dst, diag))
                pl.when(differ == 1)(lambda: start(src, 0, x, x, dst, land_sem, diag))

            for diag in (False, True):
                if step == (1 if diag else 0):
                    continue
                which = (half == (1 if diag else 0)) if step == 2 else (half >= 0)
                pl.when((group >= G) & (group < G + 2) & which)(functools.partial(far, diag))
                pl.when((group >= G + 2) & which)(functools.partial(near, diag))

    def relay(rnd, cd, place):
        over_x = differ * (1 - (place + cd) // OVER_X)
        owner = over_x * ((1 - y) * 4 + x * 2) + (1 - over_x) * (y * 4 + (1 - x) * 2) + cd
        dev = device(flip(y, 1 - over_x), flip(x, over_x), over_x * x + (1 - over_x) * c)
        tile_ref = land.at[(rnd * 8 + owner) * (UPPER3 + 3 * differ) + place]

        def pass_on(whole, diag):
            wait_for(whole, relay_sem.at[rnd, cd, place])
            for part in parts(diag):
                pltpu.make_async_remote_copy(
                    tile_ref.at[part], tile_ref.at[part], out_send, land_sem,
                    device_id=dev, device_id_type=MESH,
                ).start()

        on_diag = (differ == 0) & ((place == 0) | (place == 3) | (place == 5))
        pl.when(on_diag)(lambda: pass_on(tile_ref.at[pl.ds(0, tile * 3 // 4)], True))
        pl.when(~on_diag & (place < UPPER3 + 3 * differ))(lambda: pass_on(tile_ref, False))

    def relays(rnd, cd, low, count):
        def body(k, carry):
            relay(rnd, cd, low + k)
            return carry

        lax.fori_loop(0, count, body, 0)

    def relay_early(job, turn):
        one = (c == 1) & (turn >= 1) & (turn < 1 + G * G)
        two = (c == 0) & (turn >= 9) & (turn < 14)

        @pl.when((job == 2) & (one | two))
        def _():
            low = c * (turn - 1) + (1 - c) * 2 * (turn - 9)
            count = 1 + (1 - c) * (1 - turn // 13)

            def body(k, carry):
                relay(0, k % 2, low + k // 2)
                return carry

            lax.fori_loop(0, 2 * count, body, 0)

        @pl.when((job == 2) & (c == 1) & (turn >= 12))
        def _():
            nth = turn - 12
            low = differ * (3 * nth - nth // 2) + (1 - differ) * 2 * nth
            relays(1, 0, low, differ * (3 - (nth + 1) // 2) + (1 - differ) * 2)

    def tiles_of(turn):
        out = []
        for half in range(2):
            row = turn * 2 + half
            for step in range(3):
                out.append((*upper_tile(row, step), step == 0))
        out.append((turn, turn + 3, False))
        return sorted(out, key=lambda item: item[2])

    def unit(v, step):
        late = (v + 3) // 6
        half = (v - 3) % 2
        base = G * (1 - (v - 3) // 2)
        row = base + half * (1 + step // 2)
        col = base + (1 - half) * step + half * (1 + (step + 1) // 2)
        return row * late + v * (1 - late), col * late + (G + step) * (1 - late)

    def near_tiles(turn):
        return [(turn, turn, True), (turn // 2, 1 + (turn + 1) // 2, False)]

    def other_tiles(turn):
        off = [(turn, G + j, False) for j in range(G)]
        off.append((G + turn // 2, G + 1 + (turn + 1) // 2, False))
        return [*off, (G + turn, G + turn, True)]

    def send_aid(tiles):
        for row, col, _ in tiles:
            ref = stage.at[2, slot_of(row, col)]
            pltpu.make_async_remote_copy(
                ref, ref, aid_send, aid_sem, device_id=device(y, x, 0), device_id_type=MESH
            ).start()

    def square_tiles(src, tiles, keep, early=False):
        def cross(row, col):
            part = chain(src, src, row, col, ((0, 2), (0, 1)))
            return part + part.T

        ready = [cross(row, col) if early and diag else None for row, col, diag in tiles]
        for (row, col, diag), part in zip(tiles, ready):
            if diag:
                part = cross(row, col) if part is None else part
                val = chain(src, src, row, col, ((1, 1), (0, 0))) + part
            else:
                val = chain(src, src, row, col, PASSES)
            put(buf_b, row, col, val, diag)
            if keep is not None:
                stage[2, slot_of(row, col) * (1 - keep) + UPPER * keep] = val
            sums[2] += fold(val * get(src, row, col)) * (1.0 if diag else 2.0)

    def square_a(job, before, between):
        keep = (job + 1) // 2
        aid = job == 0
        sums[2] = jnp.zeros_like(sums[2])

        def near(v, carry):
            pl.when(aid & (v > 0))(lambda: send_aid(near_tiles(v - 1)))
            square_tiles(buf_a, near_tiles(v), keep)
            return carry

        def other(v, carry):
            relay_early(job, before + v)
            pl.when(aid & (v == 0))(lambda: send_aid(near_tiles(2)))
            pl.when(aid & (v > 0))(lambda: send_aid(other_tiles(v - 1)))
            square_tiles(buf_a, other_tiles(v), keep, True)
            return carry

        lax.fori_loop(0, 3, near, 0)
        between()
        lax.fori_loop(0, 3, other, 0)
        pl.when(aid)(lambda: send_aid(other_tiles(2)))

    def square_c(job, before):
        sums[2] = jnp.zeros_like(sums[2])

        def turn(v, carry):
            relay_early(job, before + v)
            square_tiles(buf_c, tiles_of(v), None)
            return carry

        lax.fori_loop(0, 3, turn, 0)

    def absorb():
        wait_for(stage.at[2, pl.ds(0, UPPER)], aid_sem)
        sums[2] = jnp.zeros_like(sums[2])

        def turn(v, carry):
            for step in range(3):
                row, col = unit(v, step)
                val = stage[2, slot_of(row, col)]
                put(buf_b, row, col, val, False)
                sums[2] += fold(val * get(buf_a, row, col)) * jnp.where(row == col, 1.0, 2.0)
            return carry

        lax.fori_loop(0, 7, turn, 0)

    def coefs():
        t1, t2, t3 = total(sums[0]), total(sums[1]), total(sums[2])
        coef = (t2 - t3) / (t1 - t2)
        inv = 1.0 / (1.0 - coef)
        return (1.0 - 2.0 * coef) * inv, (1.0 + coef) * inv, inv

    def count(val, diag):
        if diag:
            sums[0] += fold(val * eye)
        sums[1] += fold(val * val) * (1.0 if diag else 2.0)

    def combine(src, row, col, co):
        acc = chain(buf_b, src, row, col, PASSES)
        return co[0] * get(src, row, col) + co[1] * get(buf_b, row, col) - co[2] * acc

    def cube(src, dst, job, before):
        co = coefs()
        sums[0:2] = jnp.zeros_like(sums[0:2])

        def turn(v, carry):
            relay_early(job, before + v)
            for row, col, diag in tiles_of(v):
                val = combine(src, row, col, co)
                put(dst, row, col, val, diag)
                count(val, diag)
            return carry

        lax.fori_loop(0, 3, turn, 0)

    def cube_last(src, rnd):
        co = coefs()
        sums[0] = jnp.zeros_like(sums[0])

        def when(v):
            pair = (v + 1) // 2 % 3
            return v + pair * (5 - 3 * pair)

        def turn(v, carry):
            @pl.when(v > 0)
            def _():
                send_out(rnd, when(v - 1))

            @pl.when((rnd == 1) & (c * differ == 1) & (v >= 1) & (v < 3))
            def _():
                relays(1, 0, v + 6, 1)

            for step in range(3):
                row, col = unit(when(v), step)
                val = combine(src, row, col, co)
                slot = slot_of(row, col)
                weight = jnp.where(row == col, 1.0, 2.0)
                sums[0] += fold(val * stage[rnd, slot]) * weight
                stage[rnd, slot] = val
            return carry

        lax.fori_loop(0, 7, turn, 0)
        send_out(rnd, when(6))

    def one_job(job, carry):
        pl.when((job > 0) | (c == 1))(lambda: run_job(job))
        return carry

    def run_job(job):
        own_job = (job + 1) // 2
        rnd = job - 1
        put_in = (job + 2) % 3
        mat = own_job * (rnd * 8 + own) + (1 - own_job) * (8 + own - 1)
        wait_for(stage.at[put_in, pl.ds(0, 15)], so_sem.at[put_in])
        starts = job == 1 - c

        def far_block():
            wait_for(stage.at[put_in, pl.ds(15, 6), pl.ds(0, tile * 7 // 8)], r_sem.at[put_in])
            for i in range(G, NB):
                slot = slot_of(i, i)
                stage[put_in, slot, quarter:, :quarter] = stage[put_in, slot, :quarter, quarter:].T

        @pl.when(starts)
        def _():
            wait_for(t_land, t_sem)

        @pl.when(~starts)
        def _():
            far_block()
            part = fold(stage[put_in, slot_of(G, G)] * eye)
            for i in range(G + 1, NB):
                part += fold(stage[put_in, slot_of(i, i)] * eye)
            t_land[...] = part[:, :quarter] + part[:, quarter:]

        diag_sum = fold(stage[put_in, slot_of(0, 0)] * eye)
        for i in range(1, G):
            diag_sum += fold(stage[put_in, slot_of(i, i)] * eye)
        mean = (total(diag_sum) + total(t_land[...])) / order
        filled = occ[mat].astype(F32)
        scale = jnp.minimum(
            filled / (bounds[1, mat] - mean), (order - filled) / (mean - bounds[0, mat])
        )
        on_diag = (scale * mean + filled) / order
        slope = scale / order
        sums[0:2] = jnp.zeros_like(sums[0:2])

        def first(q, c_):
            v = q + 2 * (q // 3 - q // 6) - 4 * (q // 5)
            for step in range(3):
                row, col = unit(v, step)
                one = jnp.where(row == col, 1.0, 0.0)
                val = stage[put_in, slot_of(row, col)] * -slope + (on_diag * one) * eye
                put(buf_a, row, col, val, False)
                sums[0] += fold(val * eye) * one
                sums[1] += fold(val * val) * (2.0 - one)
            return c_

        lax.fori_loop(0, 5 + 2 * jnp.where(starts, 0, 1), first, 0)
        given = (job == 2) & (c == 0)
        mine = job > 0

        def step(s, c_):
            @pl.when(((s == 0) & ~given) | ((s == 2) & mine))
            def _():
                def between():
                    @pl.when(starts & (s == 0))
                    def _():
                        far_block()
                        lax.fori_loop(5, 7, first, 0)

                square_a(job, 6 * s, between)

            pl.when((s == 0) & given)(absorb)
            pl.when((s == 1) & mine)(lambda: square_c(job, 6))
            pl.when((s == 0) & mine)(lambda: cube(buf_a, buf_c, job, 3))
            pl.when((s == 1) & mine)(lambda: cube(buf_c, buf_a, job, 9))
            pl.when((s == 2) & mine)(lambda: finish(rnd, mat))
            return c_

        lax.fori_loop(0, STEPS, step, 0)

    def finish(rnd, mat):
        cube_last(buf_a, rnd)
        lane = lax.broadcasted_iota(jnp.int32, e_vec.shape[1:], 1)
        e_vec[rnd] = jnp.where(lane == mat, 2.0 * total(sums[0]), 0.0)
        for k in range(1, 8):
            pltpu.make_async_remote_copy(
                e_vec.at[rnd], ener.at[mat], e_send, e_sem,
                device_id=device(flip(y, k // 4), flip(x, (k // 2) % 2), flip(c, k % 2)),
                device_id_type=MESH,
            ).start()
        pltpu.make_async_copy(e_vec.at[rnd], ener.at[mat], e_sem).start()

    lax.fori_loop(0, 3, one_job, 0)

    pl.when(c == 0)(lambda: relays(1, 0, 0, G * G))
    relays(1, 1, 0, G * G)
    wait_for(ener.at[pl.ds(0, 14)], e_send)
    wait_for(ener, e_sem)

    def wait_tiles(quarters, sem):
        lead = 8 if quarters <= 288 else 16
        wait_for(ham.at[pl.ds(0, lead), pl.ds(0, quarters * tile // (12 * lead)), :], sem)

    @pl.when(c == 1)
    def _():
        wait_for(stage.at[2, pl.ds(0, UPPER)], aid_send)

    @pl.when(differ == 0)
    def _():
        pl.when(c == 0)(lambda: wait_tiles(105 + 72, in_send))
        pl.when(c == 1)(lambda: wait_tiles(105 + 48, in_send))
        wait_for(t_vec, t_send)
        wait_tiles(4 * 96, out_send)
        wait_tiles(4 * 63, land_sem)

    @pl.when(differ == 1)
    def _():
        pl.when(c == 0)(lambda: wait_tiles(108, in_send))
        pl.when(c == 1)(lambda: wait_tiles(72, in_send))
        wait_tiles(414, out_send)
        wait_tiles(4 * 108, land_sem)


RING = 4
ROW_RING = 10


def ring(count, depth, load, store, work):
    def prime(unit, carry):
        load(unit, lambda copy: copy.start())
        return carry

    def turn(unit, carry):
        load(unit, None)
        pl.when(unit >= depth)(lambda: store(unit - depth).wait())
        work(unit)
        store(unit).start()
        pl.when(unit + depth < count)(lambda: load(unit + depth, lambda copy: copy.start()))
        return carry

    def drain(unit, carry):
        store(unit).wait()
        return carry

    lax.fori_loop(0, depth, prime, 0)
    lax.fori_loop(0, count, turn, 0)
    lax.fori_loop(count - depth, count, drain, 0)


def unpack_kernel(land, ener, out, energy, held, block, row_held, row_block, in_sem, out_sem, row_in, row_out):
    mats, tile = out.shape[0], land.shape[1]
    half = tile // 2
    x, c = lax.axis_index('row'), lax.axis_index('col')
    differ = flip(x, c)
    energy[...] = jnp.sum(ener[...], axis=0)[0, : energy.shape[0]]

    def load(mat, act):
        slot = mat % RING
        copy = pltpu.make_async_copy(
            land.at[pl.ds(mat * UPPER3, UPPER3)], held.at[slot], in_sem.at[slot]
        )
        copy.wait() if act is None else act(copy)

    def store(mat):
        slot = mat % RING
        return pltpu.make_async_copy(block.at[slot], out.at[mat], out_sem.at[slot])

    def mirror(mat):
        slot = mat % RING

        def write(i, j, val):
            rows, cols = val.shape
            block[slot, pl.ds(i * half, rows), pl.ds(j * half, cols)] = val

        for i in range(G):
            for j in range(i, G):
                place = slot3_of(i, j)
                if i == j:
                    top = held[slot, place, :half, :]
                    write(2 * i, 2 * i, top)
                    write(2 * i + 1, 2 * i, top[:, half:].T)
                    write(2 * i + 1, 2 * i + 1, held[slot, place, half:, half:])
                else:
                    val = held[slot, place]
                    write(2 * i, 2 * j, val)
                    write(2 * j, 2 * i, val.T)

    def turned(mat):
        return flip((mat // 2) % 2, x)

    def load_row(unit, act):
        slot, mat, row = unit % ROW_RING, unit // G, unit % G
        if act is None:
            pltpu.make_async_copy(row_held.at[slot], row_held.at[slot], row_in.at[slot]).wait()
            return
        flipped = turned(mat)
        for k in range(G):
            place = (1 - flipped) * (row * G + k) + flipped * (k * G + row)
            act(pltpu.make_async_copy(land.at[mat * G * G + place], row_held.at[slot, k], row_in.at[slot]))

    def store_row(unit):
        slot, mat, row = unit % ROW_RING, unit // G, unit % G
        return pltpu.make_async_copy(
            row_block.at[slot], out.at[mat, pl.ds(row * tile, tile), :], row_out.at[slot]
        )

    def turn_row(unit):
        slot = unit % ROW_RING
        flipped = turned(unit // G)

        @pl.when(flipped == 0)
        def _():
            for k in range(G):
                row_block[slot, :, pl.ds(k * tile, tile)] = row_held[slot, k]

        @pl.when(flipped == 1)
        def _():
            for k in range(G):
                row_block[slot, :, pl.ds(k * tile, tile)] = row_held[slot, k].T

    pl.when(differ == 0)(lambda: ring(mats, RING, load, store, mirror))
    pl.when(differ == 1)(lambda: ring(mats * G, ROW_RING, load_row, store_row, turn_row))


def solution(mesh):
    def local_purify(ham, bounds, occ):
        mats, blk, _ = ham.shape
        tile = blk // G
        any_spec = pl.BlockSpec(memory_space=pltpu.HBM)
        smem = pl.BlockSpec(memory_space=pltpu.SMEM)
        limb = pltpu.VMEM((3, NB, NB, tile, tile), BF16)
        flops = 2 * 6 * 21 * 36 * 2 * tile**3
        land, ener = pl.pallas_call(
            main_kernel,
            out_shape=(
                jax.ShapeDtypeStruct((mats * G * G, tile, tile), F32),
                jax.ShapeDtypeStruct((mats, 8, 128), F32),
            ),
            in_specs=[smem, smem, any_spec],
            out_specs=(any_spec, any_spec),
            scratch_shapes=[
                limb, limb, limb,
                pltpu.VMEM((3, UPPER + 1, tile, tile), F32),
                pltpu.VMEM((3, 8, tile), F32),
                pltpu.VMEM((2, 8, 128), F32),
                pltpu.VMEM((2, NB, tile // 2, tile // 2), F32),
                pltpu.VMEM((2, 8, tile // 2), F32),
                pltpu.VMEM((8, tile // 2), F32),
                pltpu.SemaphoreType.DMA((3,)),
                pltpu.SemaphoreType.DMA((3,)),
                pltpu.SemaphoreType.DMA((2,)),
                pltpu.SemaphoreType.DMA,
                pltpu.SemaphoreType.DMA,
                pltpu.SemaphoreType.DMA,
                pltpu.SemaphoreType.DMA,
                pltpu.SemaphoreType.DMA,
                pltpu.SemaphoreType.DMA,
                pltpu.SemaphoreType.DMA((2, 2, G * G)),
                pltpu.SemaphoreType.DMA,
                pltpu.SemaphoreType.DMA,
                pltpu.SemaphoreType.DMA,
            ],
            compiler_params=pltpu.CompilerParams(
                collective_id=0,
                has_side_effects=True,
                vmem_limit_bytes=67043328,
            ),
            cost_estimate=pl.CostEstimate(flops=flops, bytes_accessed=120 * 2**20, transcendentals=0),
            name='purify',
        )(bounds.T, occ, ham)

        return pl.pallas_call(
            unpack_kernel,
            out_shape=(
                jax.ShapeDtypeStruct(ham.shape, F32),
                jax.ShapeDtypeStruct((mats,), F32),
            ),
            in_specs=[any_spec, pl.BlockSpec(memory_space=pltpu.VMEM)],
            out_specs=(any_spec, pl.BlockSpec(memory_space=pltpu.VMEM)),
            scratch_shapes=[
                pltpu.VMEM((RING, UPPER3, tile, tile), F32),
                pltpu.VMEM((RING, blk, blk), F32),
                pltpu.VMEM((ROW_RING, G, tile, tile), F32),
                pltpu.VMEM((ROW_RING, tile, blk), F32),
                pltpu.SemaphoreType.DMA((RING,)),
                pltpu.SemaphoreType.DMA((RING,)),
                pltpu.SemaphoreType.DMA((ROW_RING,)),
                pltpu.SemaphoreType.DMA((ROW_RING,)),
            ],
            compiler_params=pltpu.CompilerParams(vmem_limit_bytes=40 * 2**20),
            cost_estimate=pl.CostEstimate(flops=10**6, bytes_accessed=75 * 2**20, transcendentals=0),
            name='unpack',
        )(land, ener)

    mat_spec = P('spin', 'row', 'col')
    return jax.shard_map(
        local_purify, mesh=mesh,
        in_specs=(mat_spec, P('spin', None), P('spin')),
        out_specs=(mat_spec, P('spin')), check_vma=False,
    )
```

```python
import functools

import jax
import jax.numpy as jnp
from jax import lax
from jax.experimental import pallas as pl
from jax.experimental.pallas import tpu as pltpu
from jax.sharding import PartitionSpec as P

STEPS = 3
G = 3
NB = 2 * G
UPPER = NB * (NB + 1) // 2
UPPER3 = G * (G + 1) // 2
OVER_X = 8
F32 = jnp.float32
BF16 = jnp.bfloat16
PASSES = ((0, 2), (2, 0), (1, 1), (0, 1), (1, 0), (0, 0))
MESH = pl.DeviceIdType.MESH


def slot_of(row, col):
    return row * (2 * NB - 1 - row) // 2 + col


def slot3_of(row, col):
    return row * (2 * G - 1 - row) // 2 + col


def upper_tile(row, step):
    wrap = (row + step) // NB
    other = row + step - NB * wrap
    return row * (1 - wrap) + other * wrap, other * (1 - wrap) + row * wrap


def limbs(val):
    high = val.astype(BF16)
    rest = val - high.astype(F32)
    mid = rest.astype(BF16)
    low = (rest - mid.astype(F32)).astype(BF16)
    return high, mid, low


def put(ref, row, col, val, diag):
    for piece, part in enumerate(limbs(val)):
        ref[piece, row, col] = part
    if not diag:
        for piece, part in enumerate(limbs(val.T)):
            ref[piece, col, row] = part


def get(ref, row, col):
    low = ref[1, row, col].astype(F32) + ref[2, row, col].astype(F32)
    return ref[0, row, col].astype(F32) + low


def chain(left, right, row, col, passes):
    acc = None
    for k in range(NB):
        for p, q in passes:
            part = jnp.dot(left[p, row, k], right[q, k, col], preferred_element_type=F32)
            acc = part if acc is None else acc + part
    return acc


def fold(val):
    size = val.shape[0]
    return jnp.sum(val.reshape(size // 8, 8, val.shape[1]), axis=0)


def total(val):
    return jnp.sum(jnp.sum(val, axis=0, keepdims=True), axis=1, keepdims=True)


def flip(bit, by):
    return bit + by - 2 * bit * by


def main_kernel(
    bounds, occ, ham, land, ener,
    buf_a, buf_b, buf_c, stage, sums, e_vec, corner, t_vec, t_land, t3_vec, t3_land,
    so_sem, r_sem, corner_sem, t_sem, t_send, t3_sem, t3_send, in_send, aid_sem, aid_send, land_sem, relay_sem, out_send, e_sem, e_send,
):
    tile = stage.shape[2]
    order = NB * tile
    y, x, c = lax.axis_index('depth'), lax.axis_index('row'), lax.axis_index('col')
    own = y * 4 + x * 2 + c
    differ = flip(x, c)

    def device(dy, dx, cd):
        return {'depth': dy, 'row': dx, 'col': cd}

    def wait_for(ref, sem):
        pltpu.make_async_copy(ref, ref, sem).wait()

    quarter = tile // 2
    rows = lax.broadcasted_iota(jnp.int32, (tile, tile), 0)
    cols = lax.broadcasted_iota(jnp.int32, (tile, tile), 1)
    eye = jnp.where(rows == cols, 1.0, 0.0).astype(F32)

    barrier = pltpu.get_barrier_semaphore()
    for k in range(1, 8):
        pl.semaphore_signal(
            barrier, inc=1,
            device_id=device(flip(y, k // 4), flip(x, (k // 2) % 2), flip(c, k % 2)),
            device_id_type=MESH,
        )

    @pl.when(differ == 0)
    def _():
        for e in range(2):
            for i in range(NB):
                spot = pl.ds(i * quarter, quarter)
                pltpu.make_async_copy(
                    ham.at[y * 4 + (1 - x) * 2 + 8 * e, spot, spot], corner.at[e, i], corner_sem.at[e]
                ).start()
        for e in range(2):
            wait_for(corner.at[e], corner_sem.at[e])
            part = fold(corner[e, 0] * eye[:quarter, :quarter])
            for i in range(1, NB):
                part += fold(corner[e, i] * eye[:quarter, :quarter])
            t_vec[e] = part

    pl.semaphore_wait(barrier, 7)

    @pl.when(differ == 0)
    def _():
        for e in range(2):
            pltpu.make_async_remote_copy(
                t_vec.at[e], t_land, t_send, t_sem,
                device_id=device(y, 1 - x, e), device_id_type=MESH,
            ).start()

    def h_tile(mat, i, j):
        return ham.at[mat, pl.ds(i * tile, tile), pl.ds(j * tile, tile)]

    def parts(diag):
        half = tile // 2
        if not diag:
            return [(slice(None), slice(None))]
        return [(pl.ds(0, half), slice(None)), (pl.ds(half, half), pl.ds(half, half))]

    diag_tiles = [(i, j) for i in range(G) for j in range(i, G)]

    def send_in(e, carry):
        late = e // 3
        aid = (e % 3) % 2 * (1 - late)
        cd = (1 - late) * ((e + 1) // 2) + late * (e - 3)
        mat = 8 * (aid + late) + cd * (1 - aid) + y * 4
        put_in = 2 * aid + late

        @pl.when(differ == 0)
        def _():
            for i, j in diag_tiles:
                for part in parts(i == j):
                    pltpu.make_async_remote_copy(
                        h_tile(mat + (1 - x) * 2, i, j).at[part],
                        stage.at[put_in, slot_of(G + i, G + j)].at[part],
                        in_send, r_sem.at[put_in],
                        device_id=device(y, 1 - x, cd), device_id_type=MESH,
                    ).start()

        def near(tiles, shift):
            for i, j in tiles:
                near_tile(i, j, shift)

        def near_row(i, carry_):
            for j in range(G):
                near_tile(i, j, G)
            return carry_

        def near_tile(i, j, shift):
            src = h_tile(mat + x * 2, i, j)
            dst = stage.at[put_in, slot_of(i, shift + j)]

            @pl.when(cd == c)
            def _():
                pltpu.make_async_copy(src, dst, so_sem.at[put_in]).start()

            @pl.when(cd != c)
            def _():
                pltpu.make_async_remote_copy(
                    src, dst, in_send, so_sem.at[put_in],
                    device_id=device(y, x, cd), device_id_type=MESH,
                ).start()

        pl.when(differ == 0)(lambda: near(diag_tiles, 0))

        @pl.when(differ == 1)
        def _():
            lax.fori_loop(0, G, near_row, 0)

        return carry

    lax.fori_loop(0, 5, send_in, 0)

    def send_out(rnd, group):
        mat = rnd * 8 + own

        def start(src, dy, xd, cd, dst, sem, diag=False):
            for part in parts(diag):
                pltpu.make_async_remote_copy(
                    src.at[part], dst.at[part], out_send, sem,
                    device_id=device(flip(y, dy), xd, cd), device_id_type=MESH,
                ).start()

        def keep(src, dst, diag=False):
            for part in parts(diag):
                pltpu.make_async_copy(src.at[part], dst.at[part], land_sem).start()

        @pl.when(group < G)
        def _():
            for step in range(3):
                place = group * G + step
                src, dst = stage.at[rnd, slot_of(group, G + step)], land.at[mat * 9 + place]
                sem = relay_sem.at[rnd, c, place]

                def first_over_y(src=src, dst=dst, sem=sem):
                    start(src, 1, x, 1 - x, dst, sem)
                    start(src, 0, 1 - x, x, dst, land_sem)

                def first_over_x(src=src, dst=dst, sem=sem):
                    start(src, 0, 1 - x, x, dst, sem)
                    start(src, 1, x, 1 - x, dst, land_sem)

                if step == 0:
                    first_over_y()
                else:
                    pl.when(place + c < OVER_X)(first_over_y)
                    pl.when(place + c >= OVER_X)(first_over_x)
                pl.when(differ == 1)(functools.partial(keep, src, dst))
                pl.when(differ == 0)(functools.partial(start, src, 0, x, 1 - x, dst, land_sem))

        half = (group - G) % 2
        for step in range(3):
            i, j = half * (1 + step // 2), (1 - half) * step + half * (1 + (step + 1) // 2)
            place = slot3_of(i, j)
            dst = land.at[mat * UPPER3 + place]

            def far(diag, i=i, j=j, place=place, dst=dst):
                src = stage.at[rnd, slot_of(G + i, G + j)]
                start(src, 0, 1 - x, 1 - x, dst, relay_sem.at[rnd, c, place], diag)

            def near(diag, i=i, j=j, dst=dst):
                src = stage.at[rnd, slot_of(i, j)]
                start(src, 1, x, x, dst, land_sem, diag)
                pl.when(differ == 0)(lambda: keep(src, dst, diag))
                pl.when(differ == 1)(lambda: start(src, 0, x, x, dst, land_sem, diag))

            for diag in (False, True):
                if step == (1 if diag else 0):
                    continue
                which = (half == (1 if diag else 0)) if step == 2 else (half >= 0)
                pl.when((group >= G) & (group < G + 2) & which)(functools.partial(far, diag))
                pl.when((group >= G + 2) & which)(functools.partial(near, diag))

    def relay(rnd, cd, place):
        over_x = differ * (1 - (place + cd) // OVER_X)
        owner = over_x * ((1 - y) * 4 + x * 2) + (1 - over_x) * (y * 4 + (1 - x) * 2) + cd
        dev = device(flip(y, 1 - over_x), flip(x, over_x), over_x * x + (1 - over_x) * c)
        tile_ref = land.at[(rnd * 8 + owner) * (UPPER3 + 3 * differ) + place]

        def pass_on(whole, diag):
            wait_for(whole, relay_sem.at[rnd, cd, place])
            for part in parts(diag):
                pltpu.make_async_remote_copy(
                    tile_ref.at[part], tile_ref.at[part], out_send, land_sem,
                    device_id=dev, device_id_type=MESH,
                ).start()

        on_diag = (differ == 0) & ((place == 0) | (place == 3) | (place == 5))
        pl.when(on_diag)(lambda: pass_on(tile_ref.at[pl.ds(0, tile * 3 // 4)], True))
        pl.when(~on_diag & (place < UPPER3 + 3 * differ))(lambda: pass_on(tile_ref, False))

    def relays(rnd, cd, low, count):
        def body(k, carry):
            relay(rnd, cd, low + k)
            return carry

        lax.fori_loop(0, count, body, 0)

    def relay_row(rnd, cd, row):
        first = (rnd * 8 + (1 - y) * 4 + x * 2 + cd) * (G * G) + row * G
        for k in range(G):
            wait_for(land.at[first + k], relay_sem.at[rnd, cd, row * G + k])
        ref = land.at[pl.ds(first, G)]
        pltpu.make_async_remote_copy(
            ref, ref, out_send, land_sem, device_id=device(y, 1 - x, x), device_id_type=MESH
        ).start()

    def relay_early(job, turn):
        one = (c == 1) & (turn >= 1 + 6 * differ) & (turn < 7 + 3 * differ)
        two = (c == 0) & (turn >= 9 + 3 * differ) & (turn < 12 + 2 * differ)

        @pl.when((job == 2) & (one | two))
        def _():
            low = c * (turn - 1) + (1 - c) * 2 * (turn - 9)
            count = 1 + (1 - c) * (1 - turn // 13)

            def body(k, carry):
                relay(0, k % 2, low + k // 2)
                return carry

            lax.fori_loop(0, 2 * count, body, 0)

        row_1 = turn == 11 - 5 * c

        @pl.when((job == 2) & (differ == 1) & ((turn == 10 - 7 * c) | row_1))
        def _():
            for cd in range(2):
                relay_row(0, cd, jnp.where(row_1, 1, 0))

        @pl.when((job == 2) & (c * differ == 1) & ((turn == 12) | (turn == 14)))
        def _():
            relay_row(1, 0, turn // 14)

        @pl.when((job == 2) & (c == 1) & (turn >= 12 + 2 * differ))
        def _():
            relays(1, 0, 6 * differ + (1 - differ) * 2 * (turn - 12), 2 - differ)

    def tiles_of(turn):
        out = []
        for half in range(2):
            row = turn * 2 + half
            for step in range(3):
                out.append((*upper_tile(row, step), step == 0))
        out.append((turn, turn + 3, False))
        return sorted(out, key=lambda item: item[2])

    def unit(v, step):
        late = (v + 3) // 6
        half = (v - 3) % 2
        base = G * (1 - (v - 3) // 2)
        row = base + half * (1 + step // 2)
        col = base + (1 - half) * step + half * (1 + (step + 1) // 2)
        return row * late + v * (1 - late), col * late + (G + step) * (1 - late)

    def near_tiles(turn):
        return [(turn, turn, True), (turn // 2, 1 + (turn + 1) // 2, False)]

    def other_tiles(turn):
        off = [(turn, G + j, False) for j in range(G)]
        off.append((G + turn // 2, G + 1 + (turn + 1) // 2, False))
        return [*off, (G + turn, G + turn, True)]

    def send_aid(tiles):
        for row, col, _ in tiles:
            ref = stage.at[2, slot_of(row, col)]
            pltpu.make_async_remote_copy(
                ref, ref, aid_send, aid_sem, device_id=device(y, x, 0), device_id_type=MESH
            ).start()

    def square_tiles(src, tiles, keep, early=False):
        def cross(row, col):
            part = chain(src, src, row, col, ((0, 2), (0, 1)))
            return part + part.T

        ready = [cross(row, col) if early and diag else None for row, col, diag in tiles]
        for (row, col, diag), part in zip(tiles, ready):
            if diag:
                part = cross(row, col) if part is None else part
                val = chain(src, src, row, col, ((1, 1), (0, 0))) + part
            else:
                val = chain(src, src, row, col, PASSES)
            put(buf_b, row, col, val, diag)
            if keep is not None:
                stage[2, slot_of(row, col) * (1 - keep) + UPPER * keep] = val
            sums[2] += fold(val * get(src, row, col)) * (1.0 if diag else 2.0)

    def square_a(job, before, between):
        keep = (job + 1) // 2
        aid = job == 0
        sums[2] = jnp.zeros_like(sums[2])

        def near(v, carry):
            pl.when(aid & (v > 0))(lambda: send_aid(near_tiles(v - 1)))
            square_tiles(buf_a, near_tiles(v), keep)
            return carry

        def other(v, carry):
            relay_early(job, before + v)
            pl.when(aid & (v == 0))(lambda: send_aid(near_tiles(2)))
            pl.when(aid & (v > 0))(lambda: send_aid(other_tiles(v - 1)))
            square_tiles(buf_a, other_tiles(v), keep, True)
            return carry

        lax.fori_loop(0, 3 - job // 3, near, 0)
        between()
        lax.fori_loop(0, 3, other, 0)

        @pl.when(aid)
        def _():
            t3_vec[...] = sums[2]
            send_aid(other_tiles(2))
            pltpu.make_async_remote_copy(
                t3_vec, t3_land, t3_send, t3_sem, device_id=device(y, x, 0), device_id_type=MESH
            ).start()

    def square_c(job, before):
        sums[2] = jnp.zeros_like(sums[2])

        def turn(v, carry):
            relay_early(job, before + v)
            square_tiles(buf_c, tiles_of(v), None)
            return carry

        lax.fori_loop(0, 3, turn, 0)

    def absorb():
        wait_for(stage.at[2, pl.ds(0, UPPER)], aid_sem)
        wait_for(t3_land, t3_sem)
        sums[2] = t3_land[...]

        def turn(v, carry):
            for step in range(3):
                row, col = unit(v, step)
                put(buf_b, row, col, stage[2, slot_of(row, col)], False)
            return carry

        lax.fori_loop(0, 7, turn, 0)

    def coefs():
        t1, t2, t3 = total(sums[0]), total(sums[1]), total(sums[2])
        coef = (t2 - t3) / (t1 - t2)
        inv = 1.0 / (1.0 - coef)
        return (1.0 - 2.0 * coef) * inv, (1.0 + coef) * inv, inv

    def count(val, diag):
        if diag:
            sums[0] += fold(val * eye)
        sums[1] += fold(val * val) * (1.0 if diag else 2.0)

    def combine(src, row, col, co):
        acc = chain(buf_b, src, row, col, PASSES)
        return co[0] * get(src, row, col) + co[1] * get(buf_b, row, col) - co[2] * acc

    def cube(src, dst, job, before):
        co = coefs()
        sums[0:2] = jnp.zeros_like(sums[0:2])

        def turn(v, carry):
            relay_early(job, before + v)
            for row, col, diag in tiles_of(v):
                val = combine(src, row, col, co)
                put(dst, row, col, val, diag)
                count(val, diag)
            return carry

        lax.fori_loop(0, 3, turn, 0)

    def cube_last(src, rnd):
        co = coefs()
        sums[0] = jnp.zeros_like(sums[0])

        def when(v):
            pair = (v + 1) // 2 % 3
            return v + pair * (5 - 3 * pair)

        def turn(v, carry):
            @pl.when(v > 0)
            def _():
                send_out(rnd, when(v - 1))

            @pl.when((rnd == 1) & (c * differ == 1) & (v >= 1) & (v < 3))
            def _():
                relays(1, 0, v + 6, 1)

            for step in range(3):
                row, col = unit(when(v), step)
                val = combine(src, row, col, co)
                slot = slot_of(row, col)
                weight = jnp.where(row == col, 1.0, 2.0)
                sums[0] += fold(val * stage[rnd, slot]) * weight
                stage[rnd, slot] = val
            return carry

        lax.fori_loop(0, 7, turn, 0)
        send_out(rnd, when(6))

    def one_job(job, carry):
        pl.when((job > 0) | (c == 1))(lambda: run_job(job))
        return carry

    def run_job(job):
        own_job = (job + 1) // 2
        rnd = job - 1
        put_in = (job + 2) % 3
        mat = own_job * (rnd * 8 + own) + (1 - own_job) * (8 + own - 1)
        wait_for(stage.at[put_in, pl.ds(0, 15)], so_sem.at[put_in])
        starts = job == 1 - c

        def far_block():
            wait_for(stage.at[put_in, pl.ds(15, 6), pl.ds(0, tile * 7 // 8)], r_sem.at[put_in])
            for i in range(G, NB):
                slot = slot_of(i, i)
                stage[put_in, slot, quarter:, :quarter] = stage[put_in, slot, :quarter, quarter:].T

        @pl.when(starts)
        def _():
            wait_for(t_land, t_sem)

        @pl.when(~starts)
        def _():
            far_block()
            part = fold(stage[put_in, slot_of(G, G)] * eye)
            for i in range(G + 1, NB):
                part += fold(stage[put_in, slot_of(i, i)] * eye)
            t_land[...] = part[:, :quarter] + part[:, quarter:]

        diag_sum = fold(stage[put_in, slot_of(0, 0)] * eye)
        for i in range(1, G):
            diag_sum += fold(stage[put_in, slot_of(i, i)] * eye)
        mean = (total(diag_sum) + total(t_land[...])) / order
        filled = occ[mat].astype(F32)
        scale = jnp.minimum(
            filled / (bounds[1, mat] - mean), (order - filled) / (mean - bounds[0, mat])
        )
        on_diag = (scale * mean + filled) / order
        slope = scale / order
        sums[0] = jnp.where((rows[:8] == 0) & (cols[:8] == 0), filled, 0.0)
        sums[1] = jnp.zeros_like(sums[1])

        def first_off(v, c_):
            for step in range(3):
                val = stage[put_in, slot_of(v, G + step)] * -slope
                put(buf_a, v, G + step, val, False)
                sums[1] += fold(val * val) * 2.0
            return c_

        def first(q, c_):
            v = (q + 2) % 4 + 3
            for step in range(3):
                row, col = unit(v, step)
                one = jnp.where(row == col, 1.0, 0.0)
                val = stage[put_in, slot_of(row, col)] * -slope + (on_diag * one) * eye
                put(buf_a, row, col, val, False)
                sums[1] += fold(val * val) * (2.0 - one)
            return c_

        lax.fori_loop(0, 3, first_off, 0)
        lax.fori_loop(0, 2 + 2 * jnp.where(starts, 0, 1), first, 0)
        given = (job == 2) & (c == 0)
        mine = job > 0

        def step(s, c_):
            @pl.when(((s == 0) & ~given) | ((s == 2) & mine))
            def _():
                def between():
                    @pl.when(starts & (s == 0))
                    def _():
                        far_block()
                        lax.fori_loop(2, 4, first, 0)

                square_a(job, 6 * s, between)

            pl.when((s == 0) & given)(absorb)
            pl.when((s == 1) & mine)(lambda: square_c(job, 6))
            pl.when((s == 0) & mine)(lambda: cube(buf_a, buf_c, job, 3))
            pl.when((s == 1) & mine)(lambda: cube(buf_c, buf_a, job, 9))
            pl.when((s == 2) & mine)(lambda: finish(rnd, mat))
            return c_

        lax.fori_loop(0, STEPS, step, 0)

    def finish(rnd, mat):
        cube_last(buf_a, rnd)
        lane = lax.broadcasted_iota(jnp.int32, e_vec.shape[1:], 1)
        e_vec[rnd] = jnp.where(lane == mat, 2.0 * total(sums[0]), 0.0)
        for k in range(1, 8):
            pltpu.make_async_remote_copy(
                e_vec.at[rnd], ener.at[mat], e_send, e_sem,
                device_id=device(flip(y, k // 4), flip(x, (k // 2) % 2), flip(c, k % 2)),
                device_id_type=MESH,
            ).start()
        pltpu.make_async_copy(e_vec.at[rnd], ener.at[mat], e_sem).start()

    lax.fori_loop(0, 3, one_job, 0)

    pl.when(c == 0)(lambda: relays(1, 0, 0, G * G))
    relays(1, 1, 0, G * G)
    wait_for(ener.at[pl.ds(0, 14)], e_send)
    wait_for(ener, e_sem)

    def wait_tiles(quarters, sem):
        lead = 8 if quarters <= 288 else 16
        wait_for(ham.at[pl.ds(0, lead), pl.ds(0, quarters * tile // (12 * lead)), :], sem)

    @pl.when(c == 1)
    def _():
        wait_for(stage.at[2, pl.ds(0, UPPER)], aid_send)
        wait_for(t3_vec, t3_send)

    @pl.when(differ == 0)
    def _():
        pl.when(c == 0)(lambda: wait_tiles(105 + 72, in_send))
        pl.when(c == 1)(lambda: wait_tiles(105 + 48, in_send))
        wait_for(t_vec, t_send)
        wait_tiles(4 * 96, out_send)
        wait_tiles(4 * 63, land_sem)

    @pl.when(differ == 1)
    def _():
        pl.when(c == 0)(lambda: wait_tiles(108, in_send))
        pl.when(c == 1)(lambda: wait_tiles(72, in_send))
        wait_tiles(414, out_send)
        wait_tiles(4 * 108, land_sem)


RING = 4
ROW_RING = 10


def ring(count, depth, load, store, work):
    def prime(unit, carry):
        load(unit, lambda copy: copy.start())
        return carry

    def turn(unit, carry):
        load(unit, None)
        pl.when(unit >= depth)(lambda: store(unit - depth).wait())
        work(unit)
        store(unit).start()
        pl.when(unit + depth < count)(lambda: load(unit + depth, lambda copy: copy.start()))
        return carry

    def drain(unit, carry):
        store(unit).wait()
        return carry

    lax.fori_loop(0, depth, prime, 0)
    lax.fori_loop(0, count, turn, 0)
    lax.fori_loop(count - depth, count, drain, 0)


def unpack_kernel(land, ener, out, energy, held, block, row_held, row_block, in_sem, out_sem, row_in, row_out):
    mats, tile = out.shape[0], land.shape[1]
    half = tile // 2
    x, c = lax.axis_index('row'), lax.axis_index('col')
    differ = flip(x, c)
    energy[...] = jnp.sum(ener[...], axis=0)[0, : energy.shape[0]]

    def load(mat, act):
        slot = mat % RING
        copy = pltpu.make_async_copy(
            land.at[pl.ds(mat * UPPER3, UPPER3)], held.at[slot], in_sem.at[slot]
        )
        copy.wait() if act is None else act(copy)

    def store(mat):
        slot = mat % RING
        return pltpu.make_async_copy(block.at[slot], out.at[mat], out_sem.at[slot])

    def mirror(mat):
        slot = mat % RING

        def write(i, j, val):
            rows, cols = val.shape
            block[slot, pl.ds(i * half, rows), pl.ds(j * half, cols)] = val

        for i in range(G):
            for j in range(i, G):
                place = slot3_of(i, j)
                if i == j:
                    top = held[slot, place, :half, :]
                    write(2 * i, 2 * i, top)
                    write(2 * i + 1, 2 * i, top[:, half:].T)
                    write(2 * i + 1, 2 * i + 1, held[slot, place, half:, half:])
                else:
                    val = held[slot, place]
                    write(2 * i, 2 * j, val)
                    write(2 * j, 2 * i, val.T)

    def turned(mat):
        return flip((mat // 2) % 2, x)

    def load_row(unit, act):
        slot, mat, row = unit % ROW_RING, unit // G, unit % G
        if act is None:
            pltpu.make_async_copy(row_held.at[slot], row_held.at[slot], row_in.at[slot]).wait()
            return
        flipped = turned(mat)
        for k in range(G):
            place = (1 - flipped) * (row * G + k) + flipped * (k * G + row)
            act(pltpu.make_async_copy(land.at[mat * G * G + place], row_held.at[slot, k], row_in.at[slot]))

    def store_row(unit):
        slot, mat, row = unit % ROW_RING, unit // G, unit % G
        return pltpu.make_async_copy(
            row_block.at[slot], out.at[mat, pl.ds(row * tile, tile), :], row_out.at[slot]
        )

    def turn_row(unit):
        slot = unit % ROW_RING
        flipped = turned(unit // G)

        @pl.when(flipped == 0)
        def _():
            for k in range(G):
                row_block[slot, :, pl.ds(k * tile, tile)] = row_held[slot, k]

        @pl.when(flipped == 1)
        def _():
            for k in range(G):
                row_block[slot, :, pl.ds(k * tile, tile)] = row_held[slot, k].T

    pl.when(differ == 0)(lambda: ring(mats, RING, load, store, mirror))
    pl.when(differ == 1)(lambda: ring(mats * G, ROW_RING, load_row, store_row, turn_row))


def solution(mesh):
    def local_purify(ham, bounds, occ):
        mats, blk, _ = ham.shape
        tile = blk // G
        any_spec = pl.BlockSpec(memory_space=pltpu.HBM)
        smem = pl.BlockSpec(memory_space=pltpu.SMEM)
        limb = pltpu.VMEM((3, NB, NB, tile, tile), BF16)
        flops = 2 * 6 * 21 * 36 * 2 * tile**3
        land, ener = pl.pallas_call(
            main_kernel,
            out_shape=(
                jax.ShapeDtypeStruct((mats * G * G, tile, tile), F32),
                jax.ShapeDtypeStruct((mats, 8, 128), F32),
            ),
            in_specs=[smem, smem, any_spec],
            out_specs=(any_spec, any_spec),
            scratch_shapes=[
                limb, limb, limb,
                pltpu.VMEM((3, UPPER + 1, tile, tile), F32),
                pltpu.VMEM((3, 8, tile), F32),
                pltpu.VMEM((2, 8, 128), F32),
                pltpu.VMEM((2, NB, tile // 2, tile // 2), F32),
                pltpu.VMEM((2, 8, tile // 2), F32),
                pltpu.VMEM((8, tile // 2), F32),
                pltpu.VMEM((8, tile), F32),
                pltpu.VMEM((8, tile), F32),
                pltpu.SemaphoreType.DMA((3,)),
                pltpu.SemaphoreType.DMA((3,)),
                pltpu.SemaphoreType.DMA((2,)),
                pltpu.SemaphoreType.DMA,
                pltpu.SemaphoreType.DMA,
                pltpu.SemaphoreType.DMA,
                pltpu.SemaphoreType.DMA,
                pltpu.SemaphoreType.DMA,
                pltpu.SemaphoreType.DMA,
                pltpu.SemaphoreType.DMA,
                pltpu.SemaphoreType.DMA,
                pltpu.SemaphoreType.DMA((2, 2, G * G)),
                pltpu.SemaphoreType.DMA,
                pltpu.SemaphoreType.DMA,
                pltpu.SemaphoreType.DMA,
            ],
            compiler_params=pltpu.CompilerParams(
                collective_id=0,
                has_side_effects=True,
                vmem_limit_bytes=67043328,
            ),
            cost_estimate=pl.CostEstimate(flops=flops, bytes_accessed=120 * 2**20, transcendentals=0),
            name='purify',
        )(bounds.T, occ, ham)

        return pl.pallas_call(
            unpack_kernel,
            out_shape=(
                jax.ShapeDtypeStruct(ham.shape, F32),
                jax.ShapeDtypeStruct((mats,), F32),
            ),
            in_specs=[any_spec, pl.BlockSpec(memory_space=pltpu.VMEM)],
            out_specs=(any_spec, pl.BlockSpec(memory_space=pltpu.VMEM)),
            scratch_shapes=[
                pltpu.VMEM((RING, UPPER3, tile, tile), F32),
                pltpu.VMEM((RING, blk, blk), F32),
                pltpu.VMEM((ROW_RING, G, tile, tile), F32),
                pltpu.VMEM((ROW_RING, tile, blk), F32),
                pltpu.SemaphoreType.DMA((RING,)),
                pltpu.SemaphoreType.DMA((RING,)),
                pltpu.SemaphoreType.DMA((ROW_RING,)),
                pltpu.SemaphoreType.DMA((ROW_RING,)),
            ],
            compiler_params=pltpu.CompilerParams(vmem_limit_bytes=40 * 2**20),
            cost_estimate=pl.CostEstimate(flops=10**6, bytes_accessed=75 * 2**20, transcendentals=0),
            name='unpack',
        )(land, ener)

    mat_spec = P('spin', 'row', 'col')
    return jax.shard_map(
        local_purify, mesh=mesh,
        in_specs=(mat_spec, P('spin', None), P('spin')),
        out_specs=(mat_spec, P('spin')), check_vma=False,
    )
```

```python
import functools

import jax
import jax.numpy as jnp
from jax import lax
from jax.experimental import pallas as pl
from jax.experimental.pallas import tpu as pltpu
from jax.sharding import PartitionSpec as P

STEPS = 3
G = 3
NB = 2 * G
UPPER = NB * (NB + 1) // 2
UPPER3 = G * (G + 1) // 2
OVER_X = 8
F32 = jnp.float32
BF16 = jnp.bfloat16
PASSES = ((0, 2), (2, 0), (1, 1), (0, 1), (1, 0), (0, 0))
MESH = pl.DeviceIdType.MESH


def slot_of(row, col):
    return row * (2 * NB - 1 - row) // 2 + col


def slot3_of(row, col):
    return row * (2 * G - 1 - row) // 2 + col


def upper_tile(row, step):
    wrap = (row + step) // NB
    other = row + step - NB * wrap
    return row * (1 - wrap) + other * wrap, other * (1 - wrap) + row * wrap


def limbs(val):
    high = val.astype(BF16)
    rest = val - high.astype(F32)
    mid = rest.astype(BF16)
    low = (rest - mid.astype(F32)).astype(BF16)
    return high, mid, low


def put(ref, row, col, val, diag):
    for piece, part in enumerate(limbs(val)):
        ref[piece, row, col] = part
    if not diag:
        for piece, part in enumerate(limbs(val.T)):
            ref[piece, col, row] = part


def get(ref, row, col):
    low = ref[1, row, col].astype(F32) + ref[2, row, col].astype(F32)
    return ref[0, row, col].astype(F32) + low


def chain(left, right, row, col, passes):
    acc = None
    for k in range(NB):
        for p, q in passes:
            part = jnp.dot(left[p, row, k], right[q, k, col], preferred_element_type=F32)
            acc = part if acc is None else acc + part
    return acc


def fold(val):
    size = val.shape[0]
    return jnp.sum(val.reshape(size // 8, 8, val.shape[1]), axis=0)


def total(val):
    return jnp.sum(jnp.sum(val, axis=0, keepdims=True), axis=1, keepdims=True)


def flip(bit, by):
    return bit + by - 2 * bit * by


def main_kernel(
    bounds, occ, ham, land, ener,
    buf_a, buf_b, buf_c, stage, sums, e_vec, corner, t_vec, t_land, t3_vec, t3_land,
    so_sem, r_sem, corner_sem, t_sem, t_send, t3_sem, t3_send, in_send, aid_sem, aid_send, land_sem, relay_sem, out_send, e_sem, e_send,
):
    tile = stage.shape[2]
    order = NB * tile
    y, x, c = lax.axis_index('depth'), lax.axis_index('row'), lax.axis_index('col')
    own = y * 4 + x * 2 + c
    differ = flip(x, c)

    def device(dy, dx, cd):
        return {'depth': dy, 'row': dx, 'col': cd}

    def wait_for(ref, sem):
        pltpu.make_async_copy(ref, ref, sem).wait()

    quarter = tile // 2
    rows = lax.broadcasted_iota(jnp.int32, (tile, tile), 0)
    cols = lax.broadcasted_iota(jnp.int32, (tile, tile), 1)
    eye = jnp.where(rows == cols, 1.0, 0.0).astype(F32)

    barrier = pltpu.get_barrier_semaphore()
    for k in range(1, 8):
        pl.semaphore_signal(
            barrier, inc=1,
            device_id=device(flip(y, k // 4), flip(x, (k // 2) % 2), flip(c, k % 2)),
            device_id_type=MESH,
        )

    @pl.when(differ == 0)
    def _():
        for e in range(2):
            for i in range(NB):
                spot = pl.ds(i * quarter, quarter)
                pltpu.make_async_copy(
                    ham.at[y * 4 + (1 - x) * 2 + 8 * e, spot, spot], corner.at[e, i], corner_sem.at[e]
                ).start()
        for e in range(2):
            wait_for(corner.at[e], corner_sem.at[e])
            part = fold(corner[e, 0] * eye[:quarter, :quarter])
            for i in range(1, NB):
                part += fold(corner[e, i] * eye[:quarter, :quarter])
            t_vec[e] = part

    pl.semaphore_wait(barrier, 7)

    @pl.when(differ == 0)
    def _():
        for e in range(2):
            pltpu.make_async_remote_copy(
                t_vec.at[e], t_land, t_send, t_sem,
                device_id=device(y, 1 - x, e), device_id_type=MESH,
            ).start()

    def h_tile(mat, i, j):
        return ham.at[mat, pl.ds(i * tile, tile), pl.ds(j * tile, tile)]

    def parts(diag):
        half = tile // 2
        if not diag:
            return [(slice(None), slice(None))]
        return [(pl.ds(0, half), slice(None)), (pl.ds(half, half), pl.ds(half, half))]

    diag_tiles = [(i, j) for i in range(G) for j in range(i, G)]

    def send_in(e, carry):
        late = e // 3
        aid = (e % 3) % 2 * (1 - late)
        cd = (1 - late) * ((e + 1) // 2) + late * (e - 3)
        mat = 8 * (aid + late) + cd * (1 - aid) + y * 4
        put_in = 2 * aid + late

        @pl.when(differ == 0)
        def _():
            for i, j in diag_tiles:
                for part in parts(i == j):
                    pltpu.make_async_remote_copy(
                        h_tile(mat + (1 - x) * 2, i, j).at[part],
                        stage.at[put_in, slot_of(G + i, G + j)].at[part],
                        in_send, r_sem.at[put_in],
                        device_id=device(y, 1 - x, cd), device_id_type=MESH,
                    ).start()

        def near(tiles, shift):
            for i, j in tiles:
                near_tile(i, j, shift)

        def near_row(i, carry_):
            for j in range(G):
                near_tile(i, j, G)
            return carry_

        def near_tile(i, j, shift):
            src = h_tile(mat + x * 2, i, j)
            dst = stage.at[put_in, slot_of(i, shift + j)]

            @pl.when(cd == c)
            def _():
                pltpu.make_async_copy(src, dst, so_sem.at[put_in]).start()

            @pl.when(cd != c)
            def _():
                pltpu.make_async_remote_copy(
                    src, dst, in_send, so_sem.at[put_in],
                    device_id=device(y, x, cd), device_id_type=MESH,
                ).start()

        pl.when(differ == 0)(lambda: near(diag_tiles, 0))

        @pl.when(differ == 1)
        def _():
            lax.fori_loop(0, G, near_row, 0)

        return carry

    lax.fori_loop(0, 5, send_in, 0)

    def send_out(rnd, group):
        mat = rnd * 8 + own

        def start(src, dy, xd, cd, dst, sem, diag=False):
            for part in parts(diag):
                pltpu.make_async_remote_copy(
                    src.at[part], dst.at[part], out_send, sem,
                    device_id=device(flip(y, dy), xd, cd), device_id_type=MESH,
                ).start()

        def keep(src, dst, diag=False):
            for part in parts(diag):
                pltpu.make_async_copy(src.at[part], dst.at[part], land_sem).start()

        @pl.when(group < G)
        def _():
            for step in range(3):
                place = group * G + step
                src, dst = stage.at[rnd, slot_of(group, G + step)], land.at[mat * 9 + place]
                sem = relay_sem.at[rnd, c, place]

                def first_over_y(src=src, dst=dst, sem=sem):
                    start(src, 1, x, 1 - x, dst, sem)
                    start(src, 0, 1 - x, x, dst, land_sem)

                def first_over_x(src=src, dst=dst, sem=sem):
                    start(src, 0, 1 - x, x, dst, sem)
                    start(src, 1, x, 1 - x, dst, land_sem)

                if step == 0:
                    first_over_y()
                else:
                    pl.when(place + c < OVER_X)(first_over_y)
                    pl.when(place + c >= OVER_X)(first_over_x)
                pl.when(differ == 1)(functools.partial(keep, src, dst))
                pl.when(differ == 0)(functools.partial(start, src, 0, x, 1 - x, dst, land_sem))

        half = (group - G) % 2
        for step in range(3):
            i, j = half * (1 + step // 2), (1 - half) * step + half * (1 + (step + 1) // 2)
            place = slot3_of(i, j)
            dst = land.at[mat * UPPER3 + place]

            def far(diag, i=i, j=j, place=place, dst=dst):
                src = stage.at[rnd, slot_of(G + i, G + j)]
                start(src, 0, 1 - x, 1 - x, dst, relay_sem.at[rnd, c, place], diag)

            def near(diag, i=i, j=j, dst=dst):
                src = stage.at[rnd, slot_of(i, j)]
                start(src, 1, x, x, dst, land_sem, diag)
                pl.when(differ == 0)(lambda: keep(src, dst, diag))
                pl.when(differ == 1)(lambda: start(src, 0, x, x, dst, land_sem, diag))

            for diag in (False, True):
                if step == (1 if diag else 0):
                    continue
                which = (half == (1 if diag else 0)) if step == 2 else (half >= 0)
                pl.when((group >= G) & (group < G + 2) & which)(functools.partial(far, diag))
                pl.when((group >= G + 2) & which)(functools.partial(near, diag))

    def relay(rnd, cd, place):
        over_x = differ * (1 - (place + cd) // OVER_X)
        owner = over_x * ((1 - y) * 4 + x * 2) + (1 - over_x) * (y * 4 + (1 - x) * 2) + cd
        dev = device(flip(y, 1 - over_x), flip(x, over_x), over_x * x + (1 - over_x) * c)
        tile_ref = land.at[(rnd * 8 + owner) * (UPPER3 + 3 * differ) + place]

        def pass_on(whole, diag):
            wait_for(whole, relay_sem.at[rnd, cd, place])
            for part in parts(diag):
                pltpu.make_async_remote_copy(
                    tile_ref.at[part], tile_ref.at[part], out_send, land_sem,
                    device_id=dev, device_id_type=MESH,
                ).start()

        on_diag = (differ == 0) & ((place == 0) | (place == 3) | (place == 5))
        pl.when(on_diag)(lambda: pass_on(tile_ref.at[pl.ds(0, tile * 3 // 4)], True))
        pl.when(~on_diag & (place < UPPER3 + 3 * differ))(lambda: pass_on(tile_ref, False))

    def relays(rnd, cd, low, count):
        def body(k, carry):
            relay(rnd, cd, low + k)
            return carry

        lax.fori_loop(0, count, body, 0)

    def relay_row(rnd, cd, row):
        first = (rnd * 8 + (1 - y) * 4 + x * 2 + cd) * (G * G) + row * G
        for k in range(G):
            wait_for(land.at[first + k], relay_sem.at[rnd, cd, row * G + k])
        ref = land.at[pl.ds(first, G)]
        pltpu.make_async_remote_copy(
            ref, ref, out_send, land_sem, device_id=device(y, 1 - x, x), device_id_type=MESH
        ).start()

    def relay_three(rnd, cd, row):
        pl.when(differ == 1)(lambda: relay_row(rnd, cd, row))
        pl.when(differ == 0)(lambda: relays(rnd, cd, row * G, G))

    def relay_early(job, turn):
        k = c * turn + (1 - c) * ((turn - 4) // 2)
        ahead = (c == 0) & ((turn == 4) | (turn == 6) | (turn == 9) | (turn == 10))
        first = ahead | ((c == 1) & (turn < 4))
        last = (c == 1) & (turn >= 12 - differ) & (turn < 14 - differ)

        @pl.when((job == 2) & (first | last))
        def _():
            rnd = jnp.where(last, 1, 0)
            nth = rnd * (turn - 12 + differ) + (1 - rnd) * k
            relay_three(rnd, nth // 2, nth % 2)

        third = ((c == 0) & ((turn == 7) | (turn == 11))) | ((c == 1) & ((turn == 2) | (turn == 4)))
        final = (c == 1) & (turn == 13)

        @pl.when((job == 2) & (differ == 1) & (third | final))
        def _():
            cd = c * ((turn - 2) // 2) + (1 - c) * ((turn - 7) // 4)
            relays(jnp.where(final, 1, 0), jnp.where(final, 0, cd), 2 * G, G)

    def tiles_of(turn):
        out = []
        for half in range(2):
            row = turn * 2 + half
            for step in range(3):
                out.append((*upper_tile(row, step), step == 0))
        out.append((turn, turn + 3, False))
        return sorted(out, key=lambda item: item[2])

    def unit(v, step):
        late = (v + 3) // 6
        half = (v - 3) % 2
        base = G * (1 - (v - 3) // 2)
        row = base + half * (1 + step // 2)
        col = base + (1 - half) * step + half * (1 + (step + 1) // 2)
        return row * late + v * (1 - late), col * late + (G + step) * (1 - late)

    def near_tiles(turn):
        return [(turn, turn, True), (turn // 2, 1 + (turn + 1) // 2, False)]

    def other_tiles(turn):
        off = [(turn, G + j, False) for j in range(G)]
        off.append((G + turn // 2, G + 1 + (turn + 1) // 2, False))
        return [*off, (G + turn, G + turn, True)]

    def send_aid(tiles):
        for row, col, _ in tiles:
            ref = stage.at[2, slot_of(row, col)]
            pltpu.make_async_remote_copy(
                ref, ref, aid_send, aid_sem, device_id=device(y, x, 0), device_id_type=MESH
            ).start()

    def square_tiles(src, tiles, keep, early=False):
        def cross(row, col):
            part = chain(src, src, row, col, ((0, 2), (0, 1)))
            return part + part.T

        ready = [cross(row, col) if early and diag else None for row, col, diag in tiles]
        for (row, col, diag), part in zip(tiles, ready):
            if diag:
                part = cross(row, col) if part is None else part
                val = chain(src, src, row, col, ((1, 1), (0, 0))) + part
            else:
                val = chain(src, src, row, col, PASSES)
            put(buf_b, row, col, val, diag)
            if keep is not None:
                stage[2, slot_of(row, col) * (1 - keep) + UPPER * keep] = val
            sums[2] += fold(val * get(src, row, col)) * (1.0 if diag else 2.0)

    def square_a(job, before, between):
        keep = (job + 1) // 2
        aid = job == 0
        sums[2] = jnp.zeros_like(sums[2])

        def near(v, carry):
            pl.when(aid & (v > 0))(lambda: send_aid(near_tiles(v - 1)))
            square_tiles(buf_a, near_tiles(v), keep)
            return carry

        def other(v, carry):
            relay_early(job, before + v)
            pl.when(aid & (v == 0))(lambda: send_aid(near_tiles(2)))
            pl.when(aid & (v > 0))(lambda: send_aid(other_tiles(v - 1)))
            square_tiles(buf_a, other_tiles(v), keep, True)
            return carry

        lax.fori_loop(0, 3 - job // 3, near, 0)
        between()
        lax.fori_loop(0, 3, other, 0)

        @pl.when(aid)
        def _():
            t3_vec[...] = sums[2]
            send_aid(other_tiles(2))
            pltpu.make_async_remote_copy(
                t3_vec, t3_land, t3_send, t3_sem, device_id=device(y, x, 0), device_id_type=MESH
            ).start()

    def square_c(job, before):
        sums[2] = jnp.zeros_like(sums[2])

        def turn(v, carry):
            relay_early(job, before + v)
            square_tiles(buf_c, tiles_of(v), None)
            return carry

        lax.fori_loop(0, 3, turn, 0)

    def absorb():
        wait_for(stage.at[2, pl.ds(0, UPPER)], aid_sem)
        wait_for(t3_land, t3_sem)
        sums[2] = t3_land[...]

        def turn(v, carry):
            for step in range(3):
                row, col = unit(v, step)
                put(buf_b, row, col, stage[2, slot_of(row, col)], False)
            return carry

        lax.fori_loop(0, 7, turn, 0)

    def coefs():
        t1, t2, t3 = total(sums[0]), total(sums[1]), total(sums[2])
        coef = (t2 - t3) / (t1 - t2)
        inv = 1.0 / (1.0 - coef)
        return (1.0 - 2.0 * coef) * inv, (1.0 + coef) * inv, inv

    def count(val, diag):
        if diag:
            sums[0] += fold(val * eye)
        sums[1] += fold(val * val) * (1.0 if diag else 2.0)

    def combine(src, row, col, co):
        acc = chain(buf_b, src, row, col, PASSES)
        return co[0] * get(src, row, col) + co[1] * get(buf_b, row, col) - co[2] * acc

    def cube(src, dst, job, before):
        co = coefs()
        sums[0:2] = jnp.zeros_like(sums[0:2])

        def turn(v, carry):
            relay_early(job, before + v)
            for row, col, diag in tiles_of(v):
                val = combine(src, row, col, co)
                put(dst, row, col, val, diag)
                count(val, diag)
            return carry

        lax.fori_loop(0, 3, turn, 0)

    def cube_last(src, rnd):
        co = coefs()
        sums[0] = jnp.zeros_like(sums[0])

        def when(v):
            pair = (v + 1) // 2 % 3
            return v + pair * (5 - 3 * pair)

        def turn(v, carry):
            @pl.when(v > 0)
            def _():
                send_out(rnd, when(v - 1))

            for step in range(3):
                row, col = unit(when(v), step)
                val = combine(src, row, col, co)
                slot = slot_of(row, col)
                weight = jnp.where(row == col, 1.0, 2.0)
                sums[0] += fold(val * stage[rnd, slot]) * weight
                stage[rnd, slot] = val
            return carry

        lax.fori_loop(0, 7, turn, 0)
        send_out(rnd, when(6))

    def one_job(job, carry):
        pl.when((job > 0) | (c == 1))(lambda: run_job(job))
        return carry

    def run_job(job):
        own_job = (job + 1) // 2
        rnd = job - 1
        put_in = (job + 2) % 3
        mat = own_job * (rnd * 8 + own) + (1 - own_job) * (8 + own - 1)
        wait_for(stage.at[put_in, pl.ds(0, 15)], so_sem.at[put_in])
        starts = job == 1 - c

        def far_block():
            wait_for(stage.at[put_in, pl.ds(15, 6), pl.ds(0, tile * 7 // 8)], r_sem.at[put_in])
            for i in range(G, NB):
                slot = slot_of(i, i)
                stage[put_in, slot, quarter:, :quarter] = stage[put_in, slot, :quarter, quarter:].T

        @pl.when(starts)
        def _():
            wait_for(t_land, t_sem)

        @pl.when(~starts)
        def _():
            far_block()
            part = fold(stage[put_in, slot_of(G, G)] * eye)
            for i in range(G + 1, NB):
                part += fold(stage[put_in, slot_of(i, i)] * eye)
            t_land[...] = part[:, :quarter] + part[:, quarter:]

        diag_sum = fold(stage[put_in, slot_of(0, 0)] * eye)
        for i in range(1, G):
            diag_sum += fold(stage[put_in, slot_of(i, i)] * eye)
        mean = (total(diag_sum) + total(t_land[...])) / order
        filled = occ[mat].astype(F32)
        scale = jnp.minimum(
            filled / (bounds[1, mat] - mean), (order - filled) / (mean - bounds[0, mat])
        )
        on_diag = (scale * mean + filled) / order
        slope = scale / order
        sums[0] = jnp.where((rows[:8] == 0) & (cols[:8] == 0), filled, 0.0)
        sums[1] = jnp.zeros_like(sums[1])

        def first_off(v, c_):
            for step in range(3):
                val = stage[put_in, slot_of(v, G + step)] * -slope
                put(buf_a, v, G + step, val, False)
                sums[1] += fold(val * val) * 2.0
            return c_

        def first(q, c_):
            v = (q + 2) % 4 + 3
            for step in range(3):
                row, col = unit(v, step)
                one = jnp.where(row == col, 1.0, 0.0)
                val = stage[put_in, slot_of(row, col)] * -slope + (on_diag * one) * eye
                put(buf_a, row, col, val, False)
                sums[1] += fold(val * val) * (2.0 - one)
            return c_

        lax.fori_loop(0, 3, first_off, 0)
        lax.fori_loop(0, 2 + 2 * jnp.where(starts, 0, 1), first, 0)
        given = (job == 2) & (c == 0)
        mine = job > 0

        def step(s, c_):
            @pl.when(((s == 0) & ~given) | ((s == 2) & mine))
            def _():
                def between():
                    @pl.when(starts & (s == 0))
                    def _():
                        far_block()
                        lax.fori_loop(2, 4, first, 0)

                square_a(job, 6 * s, between)

            pl.when((s == 0) & given)(absorb)
            pl.when((s == 1) & mine)(lambda: square_c(job, 6))
            pl.when((s == 0) & mine)(lambda: cube(buf_a, buf_c, job, 3))
            pl.when((s == 1) & mine)(lambda: cube(buf_c, buf_a, job, 9))
            pl.when((s == 2) & mine)(lambda: finish(rnd, mat))
            return c_

        lax.fori_loop(0, STEPS, step, 0)

    def finish(rnd, mat):
        cube_last(buf_a, rnd)
        lane = lax.broadcasted_iota(jnp.int32, e_vec.shape[1:], 1)
        e_vec[rnd] = jnp.where(lane == mat, 2.0 * total(sums[0]), 0.0)
        for k in range(1, 8):
            pltpu.make_async_remote_copy(
                e_vec.at[rnd], ener.at[mat], e_send, e_sem,
                device_id=device(flip(y, k // 4), flip(x, (k // 2) % 2), flip(c, k % 2)),
                device_id_type=MESH,
            ).start()
        pltpu.make_async_copy(e_vec.at[rnd], ener.at[mat], e_sem).start()

    lax.fori_loop(0, 3, one_job, 0)

    pl.when(c == 0)(lambda: relays(1, 0, 0, G * G))
    relays(1, 1, 0, G * G)
    wait_for(ener.at[pl.ds(0, 14)], e_send)
    wait_for(ener, e_sem)

    def wait_tiles(quarters, sem):
        lead = 8 if quarters <= 288 else 16
        wait_for(ham.at[pl.ds(0, lead), pl.ds(0, quarters * tile // (12 * lead)), :], sem)

    @pl.when(c == 1)
    def _():
        wait_for(stage.at[2, pl.ds(0, UPPER)], aid_send)
        wait_for(t3_vec, t3_send)

    @pl.when(differ == 0)
    def _():
        pl.when(c == 0)(lambda: wait_tiles(105 + 72, in_send))
        pl.when(c == 1)(lambda: wait_tiles(105 + 48, in_send))
        wait_for(t_vec, t_send)
        wait_tiles(4 * 96, out_send)
        wait_tiles(4 * 63, land_sem)

    @pl.when(differ == 1)
    def _():
        pl.when(c == 0)(lambda: wait_tiles(108, in_send))
        pl.when(c == 1)(lambda: wait_tiles(72, in_send))
        wait_tiles(414, out_send)
        wait_tiles(4 * 108, land_sem)


RING = 4
ROW_RING = 10


def ring(count, depth, load, store, work):
    def prime(unit, carry):
        load(unit, lambda copy: copy.start())
        return carry

    def turn(unit, carry):
        load(unit, None)
        pl.when(unit >= depth)(lambda: store(unit - depth).wait())
        work(unit)
        store(unit).start()
        pl.when(unit + depth < count)(lambda: load(unit + depth, lambda copy: copy.start()))
        return carry

    def drain(unit, carry):
        store(unit).wait()
        return carry

    lax.fori_loop(0, depth, prime, 0)
    lax.fori_loop(0, count, turn, 0)
    lax.fori_loop(count - depth, count, drain, 0)


def unpack_kernel(land, ener, out, energy, held, block, row_held, row_block, in_sem, out_sem, row_in, row_out):
    mats, tile = out.shape[0], land.shape[1]
    half = tile // 2
    x, c = lax.axis_index('row'), lax.axis_index('col')
    differ = flip(x, c)
    energy[...] = jnp.sum(ener[...], axis=0)[0, : energy.shape[0]]

    def load(mat, act):
        slot = mat % RING
        copy = pltpu.make_async_copy(
            land.at[pl.ds(mat * UPPER3, UPPER3)], held.at[slot], in_sem.at[slot]
        )
        copy.wait() if act is None else act(copy)

    def store(mat):
        slot = mat % RING
        return pltpu.make_async_copy(block.at[slot], out.at[mat], out_sem.at[slot])

    def mirror(mat):
        slot = mat % RING

        def write(i, j, val):
            rows, cols = val.shape
            block[slot, pl.ds(i * half, rows), pl.ds(j * half, cols)] = val

        for i in range(G):
            for j in range(i, G):
                place = slot3_of(i, j)
                if i == j:
                    top = held[slot, place, :half, :]
                    write(2 * i, 2 * i, top)
                    write(2 * i + 1, 2 * i, top[:, half:].T)
                    write(2 * i + 1, 2 * i + 1, held[slot, place, half:, half:])
                else:
                    val = held[slot, place]
                    write(2 * i, 2 * j, val)
                    write(2 * j, 2 * i, val.T)

    def turned(mat):
        return flip((mat // 2) % 2, x)

    def load_row(unit, act):
        slot, mat, row = unit % ROW_RING, unit // G, unit % G
        if act is None:
            pltpu.make_async_copy(row_held.at[slot], row_held.at[slot], row_in.at[slot]).wait()
            return
        flipped = turned(mat)
        for k in range(G):
            place = (1 - flipped) * (row * G + k) + flipped * (k * G + row)
            act(pltpu.make_async_copy(land.at[mat * G * G + place], row_held.at[slot, k], row_in.at[slot]))

    def store_row(unit):
        slot, mat, row = unit % ROW_RING, unit // G, unit % G
        return pltpu.make_async_copy(
            row_block.at[slot], out.at[mat, pl.ds(row * tile, tile), :], row_out.at[slot]
        )

    def turn_row(unit):
        slot = unit % ROW_RING
        flipped = turned(unit // G)

        @pl.when(flipped == 0)
        def _():
            for k in range(G):
                row_block[slot, :, pl.ds(k * tile, tile)] = row_held[slot, k]

        @pl.when(flipped == 1)
        def _():
            for k in range(G):
                row_block[slot, :, pl.ds(k * tile, tile)] = row_held[slot, k].T

    pl.when(differ == 0)(lambda: ring(mats, RING, load, store, mirror))
    pl.when(differ == 1)(lambda: ring(mats * G, ROW_RING, load_row, store_row, turn_row))


def solution(mesh):
    def local_purify(ham, bounds, occ):
        mats, blk, _ = ham.shape
        tile = blk // G
        any_spec = pl.BlockSpec(memory_space=pltpu.HBM)
        smem = pl.BlockSpec(memory_space=pltpu.SMEM)
        limb = pltpu.VMEM((3, NB, NB, tile, tile), BF16)
        flops = 2 * 6 * 21 * 36 * 2 * tile**3
        land, ener = pl.pallas_call(
            main_kernel,
            out_shape=(
                jax.ShapeDtypeStruct((mats * G * G, tile, tile), F32),
                jax.ShapeDtypeStruct((mats, 8, 128), F32),
            ),
            in_specs=[smem, smem, any_spec],
            out_specs=(any_spec, any_spec),
            scratch_shapes=[
                limb, limb, limb,
                pltpu.VMEM((3, UPPER + 1, tile, tile), F32),
                pltpu.VMEM((3, 8, tile), F32),
                pltpu.VMEM((2, 8, 128), F32),
                pltpu.VMEM((2, NB, tile // 2, tile // 2), F32),
                pltpu.VMEM((2, 8, tile // 2), F32),
                pltpu.VMEM((8, tile // 2), F32),
                pltpu.VMEM((8, tile), F32),
                pltpu.VMEM((8, tile), F32),
                pltpu.SemaphoreType.DMA((3,)),
                pltpu.SemaphoreType.DMA((3,)),
                pltpu.SemaphoreType.DMA((2,)),
                pltpu.SemaphoreType.DMA,
                pltpu.SemaphoreType.DMA,
                pltpu.SemaphoreType.DMA,
                pltpu.SemaphoreType.DMA,
                pltpu.SemaphoreType.DMA,
                pltpu.SemaphoreType.DMA,
                pltpu.SemaphoreType.DMA,
                pltpu.SemaphoreType.DMA,
                pltpu.SemaphoreType.DMA((2, 2, G * G)),
                pltpu.SemaphoreType.DMA,
                pltpu.SemaphoreType.DMA,
                pltpu.SemaphoreType.DMA,
            ],
            compiler_params=pltpu.CompilerParams(
                collective_id=0,
                has_side_effects=True,
                vmem_limit_bytes=67043328,
            ),
            cost_estimate=pl.CostEstimate(flops=flops, bytes_accessed=120 * 2**20, transcendentals=0),
            name='purify',
        )(bounds.T, occ, ham)

        return pl.pallas_call(
            unpack_kernel,
            out_shape=(
                jax.ShapeDtypeStruct(ham.shape, F32),
                jax.ShapeDtypeStruct((mats,), F32),
            ),
            in_specs=[any_spec, pl.BlockSpec(memory_space=pltpu.VMEM)],
            out_specs=(any_spec, pl.BlockSpec(memory_space=pltpu.VMEM)),
            scratch_shapes=[
                pltpu.VMEM((RING, UPPER3, tile, tile), F32),
                pltpu.VMEM((RING, blk, blk), F32),
                pltpu.VMEM((ROW_RING, G, tile, tile), F32),
                pltpu.VMEM((ROW_RING, tile, blk), F32),
                pltpu.SemaphoreType.DMA((RING,)),
                pltpu.SemaphoreType.DMA((RING,)),
                pltpu.SemaphoreType.DMA((ROW_RING,)),
                pltpu.SemaphoreType.DMA((ROW_RING,)),
            ],
            compiler_params=pltpu.CompilerParams(vmem_limit_bytes=40 * 2**20),
            cost_estimate=pl.CostEstimate(flops=10**6, bytes_accessed=75 * 2**20, transcendentals=0),
            name='unpack',
        )(land, ener)

    mat_spec = P('spin', 'row', 'col')
    return jax.shard_map(
        local_purify, mesh=mesh,
        in_specs=(mat_spec, P('spin', None), P('spin')),
        out_specs=(mat_spec, P('spin')), check_vma=False,
    )
```

```python
import functools

import jax
import jax.numpy as jnp
from jax import lax
from jax.experimental import pallas as pl
from jax.experimental.pallas import tpu as pltpu
from jax.sharding import PartitionSpec as P

STEPS = 3
G = 3
NB = 2 * G
UPPER = NB * (NB + 1) // 2
UPPER3 = G * (G + 1) // 2
F32 = jnp.float32
BF16 = jnp.bfloat16
PASSES = ((0, 2), (2, 0), (1, 1), (0, 1), (1, 0), (0, 0))
MESH = pl.DeviceIdType.MESH


def slot_of(row, col):
    return row * (2 * NB - 1 - row) // 2 + col


def slot3_of(row, col):
    return row * (2 * G - 1 - row) // 2 + col


def upper_tile(row, step):
    wrap = (row + step) // NB
    other = row + step - NB * wrap
    return row * (1 - wrap) + other * wrap, other * (1 - wrap) + row * wrap


def limbs(val):
    high = val.astype(BF16)
    rest = val - high.astype(F32)
    mid = rest.astype(BF16)
    low = (rest - mid.astype(F32)).astype(BF16)
    return high, mid, low


def put(ref, row, col, val, diag):
    for piece, part in enumerate(limbs(val)):
        ref[piece, row, col] = part
    if not diag:
        for piece, part in enumerate(limbs(val.T)):
            ref[piece, col, row] = part


def get(ref, row, col):
    low = ref[1, row, col].astype(F32) + ref[2, row, col].astype(F32)
    return ref[0, row, col].astype(F32) + low


def chain(left, right, row, col, passes):
    acc = None
    for k in range(NB):
        for p, q in passes:
            part = jnp.dot(left[p, row, k], right[q, k, col], preferred_element_type=F32)
            acc = part if acc is None else acc + part
    return acc


def fold(val):
    size = val.shape[0]
    return jnp.sum(val.reshape(size // 8, 8, val.shape[1]), axis=0)


def total(val):
    return jnp.sum(jnp.sum(val, axis=0, keepdims=True), axis=1, keepdims=True)


def flip(bit, by):
    return bit + by - 2 * bit * by


def main_kernel(
    bounds, occ, ham, land, ener,
    buf_a, buf_b, buf_c, stage, sums, e_vec, corner, t_vec, t_land, t3_vec, t3_land,
    so_sem, r_sem, corner_sem, t_sem, t_send, t3_sem, t3_send, in_send, aid_sem, aid_send, land_sem, relay_sem, out_send, e_sem, e_send,
):
    tile = stage.shape[2]
    order = NB * tile
    y, x, c = lax.axis_index('depth'), lax.axis_index('row'), lax.axis_index('col')
    own = y * 4 + x * 2 + c
    differ = flip(x, c)

    def device(dy, dx, cd):
        return {'depth': dy, 'row': dx, 'col': cd}

    def wait_for(ref, sem):
        pltpu.make_async_copy(ref, ref, sem).wait()

    quarter = tile // 2
    rows = lax.broadcasted_iota(jnp.int32, (tile, tile), 0)
    cols = lax.broadcasted_iota(jnp.int32, (tile, tile), 1)
    eye = jnp.where(rows == cols, 1.0, 0.0).astype(F32)

    barrier = pltpu.get_barrier_semaphore()
    for k in range(1, 8):
        pl.semaphore_signal(
            barrier, inc=1,
            device_id=device(flip(y, k // 4), flip(x, (k // 2) % 2), flip(c, k % 2)),
            device_id_type=MESH,
        )

    @pl.when(differ == 0)
    def _():
        for e in range(2):
            for i in range(NB):
                spot = pl.ds(i * quarter, quarter)
                pltpu.make_async_copy(
                    ham.at[y * 4 + (1 - x) * 2 + 8 * e, spot, spot], corner.at[e, i], corner_sem.at[e]
                ).start()
        for e in range(2):
            wait_for(corner.at[e], corner_sem.at[e])
            part = fold(corner[e, 0] * eye[:quarter, :quarter])
            for i in range(1, NB):
                part += fold(corner[e, i] * eye[:quarter, :quarter])
            t_vec[e] = part

    pl.semaphore_wait(barrier, 7)

    @pl.when(differ == 0)
    def _():
        for e in range(2):
            pltpu.make_async_remote_copy(
                t_vec.at[e], t_land, t_send, t_sem,
                device_id=device(y, 1 - x, e), device_id_type=MESH,
            ).start()

    def h_tile(mat, i, j):
        return ham.at[mat, pl.ds(i * tile, tile), pl.ds(j * tile, tile)]

    def parts(diag):
        half = tile // 2
        if not diag:
            return [(slice(None), slice(None))]
        return [(pl.ds(0, half), slice(None)), (pl.ds(half, half), pl.ds(half, half))]

    diag_tiles = [(i, j) for i in range(G) for j in range(i, G)]

    def send_in(e, carry):
        late = e // 3
        aid = (e % 3) % 2 * (1 - late)
        cd = (1 - late) * ((e + 1) // 2) + late * (e - 3)
        mat = 8 * (aid + late) + cd * (1 - aid) + y * 4
        put_in = 2 * aid + late

        @pl.when(differ == 0)
        def _():
            for i, j in diag_tiles:
                for part in parts(i == j):
                    pltpu.make_async_remote_copy(
                        h_tile(mat + (1 - x) * 2, i, j).at[part],
                        stage.at[put_in, slot_of(G + i, G + j)].at[part],
                        in_send, r_sem.at[put_in],
                        device_id=device(y, 1 - x, cd), device_id_type=MESH,
                    ).start()

        def near(tiles, shift):
            for i, j in tiles:
                near_tile(i, j, shift)

        def near_row(i, carry_):
            for j in range(G):
                near_tile(i, j, G)
            return carry_

        def near_tile(i, j, shift):
            src = h_tile(mat + x * 2, i, j)
            dst = stage.at[put_in, slot_of(i, shift + j)]

            @pl.when(cd == c)
            def _():
                pltpu.make_async_copy(src, dst, so_sem.at[put_in]).start()

            @pl.when(cd != c)
            def _():
                pltpu.make_async_remote_copy(
                    src, dst, in_send, so_sem.at[put_in],
                    device_id=device(y, x, cd), device_id_type=MESH,
                ).start()

        pl.when(differ == 0)(lambda: near(diag_tiles, 0))

        @pl.when(differ == 1)
        def _():
            lax.fori_loop(0, G, near_row, 0)

        return carry

    lax.fori_loop(0, 5, send_in, 0)

    def send_out(rnd, group):
        mat = rnd * 8 + own

        def start(src, dy, xd, cd, dst, sem, diag=False):
            for part in parts(diag):
                pltpu.make_async_remote_copy(
                    src.at[part], dst.at[part], out_send, sem,
                    device_id=device(flip(y, dy), xd, cd), device_id_type=MESH,
                ).start()

        def keep(src, dst, diag=False):
            for part in parts(diag):
                pltpu.make_async_copy(src.at[part], dst.at[part], land_sem).start()

        @pl.when(group < G)
        def _():
            src, dst = stage.at[rnd, pl.ds(slot_of(group, G), G)], land.at[pl.ds(mat * 9 + group * G, G)]
            sem = relay_sem.at[rnd, c, group * G]

            @pl.when((group // 2) * c == 0)
            def _():
                start(src, 1, x, 1 - x, dst, sem)
                start(src, 0, 1 - x, x, dst, land_sem)

            @pl.when((group // 2) * c == 1)
            def _():
                start(src, 0, 1 - x, x, dst, sem)
                start(src, 1, x, 1 - x, dst, land_sem)

            pl.when(differ == 1)(lambda: keep(src, dst))
            pl.when(differ == 0)(lambda: start(src, 0, x, 1 - x, dst, land_sem))

        half = (group - G) % 2
        for step in range(3):
            i, j = half * (1 + step // 2), (1 - half) * step + half * (1 + (step + 1) // 2)
            place = slot3_of(i, j)
            dst = land.at[mat * UPPER3 + place]

            def far(diag, i=i, j=j, place=place, dst=dst):
                src = stage.at[rnd, slot_of(G + i, G + j)]
                start(src, 0, 1 - x, 1 - x, dst, relay_sem.at[rnd, c, place], diag)

            def near(diag, i=i, j=j, dst=dst):
                src = stage.at[rnd, slot_of(i, j)]
                start(src, 1, x, x, dst, land_sem, diag)
                pl.when(differ == 0)(lambda: keep(src, dst, diag))
                pl.when(differ == 1)(lambda: start(src, 0, x, x, dst, land_sem, diag))

            for diag in (False, True):
                if step == (1 if diag else 0):
                    continue
                which = (half == (1 if diag else 0)) if step == 2 else (half >= 0)
                pl.when((group >= G) & (group < G + 2) & which)(functools.partial(far, diag))
                pl.when((group >= G + 2) & which)(functools.partial(near, diag))

    def relay(rnd, cd, place):
        tile_ref = land.at[(rnd * 8 + y * 4 + (1 - x) * 2 + cd) * UPPER3 + place]

        def pass_on(whole, diag):
            wait_for(whole, relay_sem.at[rnd, cd, place])
            for part in parts(diag):
                pltpu.make_async_remote_copy(
                    tile_ref.at[part], tile_ref.at[part], out_send, land_sem,
                    device_id=device(1 - y, x, x), device_id_type=MESH,
                ).start()

        on_diag = (place == 0) | (place == 3) | (place == 5)
        pl.when(on_diag)(lambda: pass_on(tile_ref.at[pl.ds(0, tile * 3 // 4)], True))
        pl.when(~on_diag)(lambda: pass_on(tile_ref, False))

    def relays(rnd, cd, low, count):
        def body(k, carry):
            relay(rnd, cd, low + k)
            return carry

        lax.fori_loop(0, count, body, 0)

    def relay_row(rnd, cd, row):
        over_x = 1 - (row // 2) * cd
        owner = over_x * ((1 - y) * 4 + x * 2) + (1 - over_x) * (y * 4 + (1 - x) * 2) + cd
        ref = land.at[pl.ds((rnd * 8 + owner) * (G * G) + row * G, G)]
        wait_for(ref, relay_sem.at[rnd, cd, row * G])
        pltpu.make_async_remote_copy(
            ref, ref, out_send, land_sem,
            device_id=device(flip(y, 1 - over_x), flip(x, over_x), over_x * x + (1 - over_x) * c),
            device_id_type=MESH,
        ).start()

    def relay_rest(cd):
        def body(row, carry):
            relay_row(1, cd, row)
            return carry

        @pl.when(differ == 1)
        def _():
            lax.fori_loop(0, G, body, 0)

        pl.when(differ == 0)(lambda: relays(1, cd, 0, UPPER3))

    def relay_early(job, turn):
        one = (c == 1) & (turn >= 1) & (turn < 7)
        two = (c == 0) & (turn >= 9) & (turn < 12)

        @pl.when((job == 2) & (differ == 0) & (one | two))
        def _():
            low = c * (turn - 1) + (1 - c) * 2 * (turn - 9)

            def body(k, carry):
                relay(0, k % 2, low + k // 2)
                return carry

            lax.fori_loop(0, 2 * (2 - c), body, 0)

        row_1, row_2 = turn == 11 - 5 * c, turn == 13 - 4 * c

        @pl.when((job == 2) & (differ == 1) & ((turn == 10 - 7 * c) | row_1 | row_2))
        def _():
            for cd in range(2):
                relay_row(0, cd, jnp.where(row_2, 2, jnp.where(row_1, 1, 0)))

        @pl.when((job == 2) & (c * differ == 1) & ((turn == 12) | (turn == 14)))
        def _():
            relay_row(1, 0, turn // 14)

        @pl.when((job == 2) & (c == 1) & (differ == 0) & (turn >= 12))
        def _():
            relays(1, 0, 2 * (turn - 12), 2)

    def tiles_of(turn):
        out = []
        for half in range(2):
            row = turn * 2 + half
            for step in range(3):
                out.append((*upper_tile(row, step), step == 0))
        out.append((turn, turn + 3, False))
        return sorted(out, key=lambda item: item[2])

    def unit(v, step):
        late = (v + 3) // 6
        half = (v - 3) % 2
        base = G * (1 - (v - 3) // 2)
        row = base + half * (1 + step // 2)
        col = base + (1 - half) * step + half * (1 + (step + 1) // 2)
        return row * late + v * (1 - late), col * late + (G + step) * (1 - late)

    def near_tiles(turn):
        return [(turn, turn, True), (turn // 2, 1 + (turn + 1) // 2, False)]

    def other_tiles(turn):
        off = [(turn, G + j, False) for j in range(G)]
        off.append((G + turn // 2, G + 1 + (turn + 1) // 2, False))
        return [*off, (G + turn, G + turn, True)]

    def send_aid(tiles):
        for row, col, _ in tiles:
            ref = stage.at[2, slot_of(row, col)]
            pltpu.make_async_remote_copy(
                ref, ref, aid_send, aid_sem, device_id=device(y, x, 0), device_id_type=MESH
            ).start()

    def square_tiles(src, tiles, keep, early=False):
        def cross(row, col):
            part = chain(src, src, row, col, ((0, 2), (0, 1)))
            return part + part.T

        ready = [cross(row, col) if early and diag else None for row, col, diag in tiles]
        for (row, col, diag), part in zip(tiles, ready):
            if diag:
                part = cross(row, col) if part is None else part
                val = chain(src, src, row, col, ((1, 1), (0, 0))) + part
            else:
                val = chain(src, src, row, col, PASSES)
            put(buf_b, row, col, val, diag)
            if keep is not None:
                stage[2, slot_of(row, col) * (1 - keep) + UPPER * keep] = val
            sums[2] += fold(val * get(src, row, col)) * (1.0 if diag else 2.0)

    def square_a(job, before, between):
        keep = (job + 1) // 2
        aid = job == 0
        sums[2] = jnp.zeros_like(sums[2])

        def near(v, carry):
            pl.when(aid & (v > 0))(lambda: send_aid(near_tiles(v - 1)))
            square_tiles(buf_a, near_tiles(v), keep)
            return carry

        def other(v, carry):
            relay_early(job, before + v)
            pl.when(aid & (v == 0))(lambda: send_aid(near_tiles(2)))
            pl.when(aid & (v > 0))(lambda: send_aid(other_tiles(v - 1)))
            square_tiles(buf_a, other_tiles(v), keep, True)
            return carry

        lax.fori_loop(0, 3 - job // 3, near, 0)
        between()
        lax.fori_loop(0, 3, other, 0)

        @pl.when(aid)
        def _():
            t3_vec[...] = sums[2]
            send_aid(other_tiles(2))
            pltpu.make_async_remote_copy(
                t3_vec, t3_land, t3_send, t3_sem, device_id=device(y, x, 0), device_id_type=MESH
            ).start()

    def square_c(job, before):
        sums[2] = jnp.zeros_like(sums[2])

        def turn(v, carry):
            relay_early(job, before + v)
            square_tiles(buf_c, tiles_of(v), None)
            return carry

        lax.fori_loop(0, 3, turn, 0)

    def absorb():
        wait_for(stage.at[2, pl.ds(0, UPPER)], aid_sem)
        wait_for(t3_land, t3_sem)
        sums[2] = t3_land[...]

        def turn(v, carry):
            for step in range(3):
                row, col = unit(v, step)
                put(buf_b, row, col, stage[2, slot_of(row, col)], False)
            return carry

        lax.fori_loop(0, 7, turn, 0)

    def coefs():
        t1, t2, t3 = total(sums[0]), total(sums[1]), total(sums[2])
        coef = (t2 - t3) / (t1 - t2)
        inv = 1.0 / (1.0 - coef)
        return (1.0 - 2.0 * coef) * inv, (1.0 + coef) * inv, inv

    def count(val, diag):
        if diag:
            sums[0] += fold(val * eye)
        sums[1] += fold(val * val) * (1.0 if diag else 2.0)

    def combine(src, row, col, co):
        acc = chain(buf_b, src, row, col, PASSES)
        return co[0] * get(src, row, col) + co[1] * get(buf_b, row, col) - co[2] * acc

    def cube(src, dst, job, before):
        co = coefs()
        sums[0:2] = jnp.zeros_like(sums[0:2])

        def turn(v, carry):
            relay_early(job, before + v)
            for row, col, diag in tiles_of(v):
                val = combine(src, row, col, co)
                put(dst, row, col, val, diag)
                count(val, diag)
            return carry

        lax.fori_loop(0, 3, turn, 0)

    def cube_last(src, rnd):
        co = coefs()
        sums[0] = jnp.zeros_like(sums[0])

        def when(v):
            pair = (v + 1) // 2 % 3
            return v + pair * (5 - 3 * pair)

        def turn(v, carry):
            @pl.when(v > 0)
            def _():
                send_out(rnd, when(v - 1))

            @pl.when((rnd == 1) & (c * differ == 1) & (v == 2))
            def _():
                relay_row(1, 0, 2)

            for step in range(3):
                row, col = unit(when(v), step)
                val = combine(src, row, col, co)
                slot = slot_of(row, col)
                weight = jnp.where(row == col, 1.0, 2.0)
                sums[0] += fold(val * stage[rnd, slot]) * weight
                stage[rnd, slot] = val
            return carry

        lax.fori_loop(0, 7, turn, 0)
        send_out(rnd, when(6))

    def one_job(job, carry):
        pl.when((job > 0) | (c == 1))(lambda: run_job(job))
        return carry

    def run_job(job):
        own_job = (job + 1) // 2
        rnd = job - 1
        put_in = (job + 2) % 3
        mat = own_job * (rnd * 8 + own) + (1 - own_job) * (8 + own - 1)
        wait_for(stage.at[put_in, pl.ds(0, 15)], so_sem.at[put_in])
        starts = job == 1 - c

        def far_block():
            wait_for(stage.at[put_in, pl.ds(15, 6), pl.ds(0, tile * 7 // 8)], r_sem.at[put_in])
            for i in range(G, NB):
                slot = slot_of(i, i)
                stage[put_in, slot, quarter:, :quarter] = stage[put_in, slot, :quarter, quarter:].T

        @pl.when(starts)
        def _():
            wait_for(t_land, t_sem)

        @pl.when(~starts)
        def _():
            far_block()
            part = fold(stage[put_in, slot_of(G, G)] * eye)
            for i in range(G + 1, NB):
                part += fold(stage[put_in, slot_of(i, i)] * eye)
            t_land[...] = part[:, :quarter] + part[:, quarter:]

        diag_sum = fold(stage[put_in, slot_of(0, 0)] * eye)
        for i in range(1, G):
            diag_sum += fold(stage[put_in, slot_of(i, i)] * eye)
        mean = (total(diag_sum) + total(t_land[...])) / order
        filled = occ[mat].astype(F32)
        scale = jnp.minimum(
            filled / (bounds[1, mat] - mean), (order - filled) / (mean - bounds[0, mat])
        )
        on_diag = (scale * mean + filled) / order
        slope = scale / order
        sums[0] = jnp.where((rows[:8] == 0) & (cols[:8] == 0), filled, 0.0)
        sums[1] = jnp.zeros_like(sums[1])

        def first_off(v, c_):
            for step in range(3):
                val = stage[put_in, slot_of(v, G + step)] * -slope
                put(buf_a, v, G + step, val, False)
                sums[1] += fold(val * val) * 2.0
            return c_

        def first(q, c_):
            v = (q + 2) % 4 + 3
            for step in range(3):
                row, col = unit(v, step)
                one = jnp.where(row == col, 1.0, 0.0)
                val = stage[put_in, slot_of(row, col)] * -slope + (on_diag * one) * eye
                put(buf_a, row, col, val, False)
                sums[1] += fold(val * val) * (2.0 - one)
            return c_

        lax.fori_loop(0, 3, first_off, 0)
        lax.fori_loop(0, 2 + 2 * jnp.where(starts, 0, 1), first, 0)
        given = (job == 2) & (c == 0)
        mine = job > 0

        def step(s, c_):
            @pl.when(((s == 0) & ~given) | ((s == 2) & mine))
            def _():
                def between():
                    @pl.when(starts & (s == 0))
                    def _():
                        far_block()
                        lax.fori_loop(2, 4, first, 0)

                square_a(job, 6 * s, between)

            pl.when((s == 0) & given)(absorb)
            pl.when((s == 1) & mine)(lambda: square_c(job, 6))
            pl.when((s == 0) & mine)(lambda: cube(buf_a, buf_c, job, 3))
            pl.when((s == 1) & mine)(lambda: cube(buf_c, buf_a, job, 9))
            pl.when((s == 2) & mine)(lambda: finish(rnd, mat))
            return c_

        lax.fori_loop(0, STEPS, step, 0)

    def finish(rnd, mat):
        cube_last(buf_a, rnd)
        lane = lax.broadcasted_iota(jnp.int32, e_vec.shape[1:], 1)
        e_vec[rnd] = jnp.where(lane == mat, 2.0 * total(sums[0]), 0.0)
        for k in range(1, 8):
            pltpu.make_async_remote_copy(
                e_vec.at[rnd], ener.at[mat], e_send, e_sem,
                device_id=device(flip(y, k // 4), flip(x, (k // 2) % 2), flip(c, k % 2)),
                device_id_type=MESH,
            ).start()
        pltpu.make_async_copy(e_vec.at[rnd], ener.at[mat], e_sem).start()

    lax.fori_loop(0, 3, one_job, 0)

    pl.when(c == 0)(lambda: relay_rest(0))
    relay_rest(1)
    wait_for(ener.at[pl.ds(0, 14)], e_send)
    wait_for(ener, e_sem)

    def wait_tiles(quarters, sem):
        lead = 8 if quarters <= 288 else 16
        wait_for(ham.at[pl.ds(0, lead), pl.ds(0, quarters * tile // (12 * lead)), :], sem)

    @pl.when(c == 1)
    def _():
        wait_for(stage.at[2, pl.ds(0, UPPER)], aid_send)
        wait_for(t3_vec, t3_send)

    @pl.when(differ == 0)
    def _():
        pl.when(c == 0)(lambda: wait_tiles(105 + 72, in_send))
        pl.when(c == 1)(lambda: wait_tiles(105 + 48, in_send))
        wait_for(t_vec, t_send)
        wait_tiles(4 * 96, out_send)
        wait_tiles(4 * 63, land_sem)

    @pl.when(differ == 1)
    def _():
        pl.when(c == 0)(lambda: wait_tiles(108, in_send))
        pl.when(c == 1)(lambda: wait_tiles(72, in_send))
        wait_tiles(414, out_send)
        wait_tiles(4 * 108, land_sem)


RING = 4
ROW_RING = 10


def ring(count, depth, load, store, work):
    def prime(unit, carry):
        load(unit, lambda copy: copy.start())
        return carry

    def turn(unit, carry):
        load(unit, None)
        pl.when(unit >= depth)(lambda: store(unit - depth).wait())
        work(unit)
        store(unit).start()
        pl.when(unit + depth < count)(lambda: load(unit + depth, lambda copy: copy.start()))
        return carry

    def drain(unit, carry):
        store(unit).wait()
        return carry

    lax.fori_loop(0, depth, prime, 0)
    lax.fori_loop(0, count, turn, 0)
    lax.fori_loop(count - depth, count, drain, 0)


def unpack_kernel(land, ener, out, energy, held, block, row_held, row_block, in_sem, out_sem, row_in, row_out):
    mats, tile = out.shape[0], land.shape[1]
    half = tile // 2
    x, c = lax.axis_index('row'), lax.axis_index('col')
    differ = flip(x, c)
    energy[...] = jnp.sum(ener[...], axis=0)[0, : energy.shape[0]]

    def load(mat, act):
        slot = mat % RING
        copy = pltpu.make_async_copy(
            land.at[pl.ds(mat * UPPER3, UPPER3)], held.at[slot], in_sem.at[slot]
        )
        copy.wait() if act is None else act(copy)

    def store(mat):
        slot = mat % RING
        return pltpu.make_async_copy(block.at[slot], out.at[mat], out_sem.at[slot])

    def mirror(mat):
        slot = mat % RING

        def write(i, j, val):
            rows, cols = val.shape
            block[slot, pl.ds(i * half, rows), pl.ds(j * half, cols)] = val

        for i in range(G):
            for j in range(i, G):
                place = slot3_of(i, j)
                if i == j:
                    top = held[slot, place, :half, :]
                    write(2 * i, 2 * i, top)
                    write(2 * i + 1, 2 * i, top[:, half:].T)
                    write(2 * i + 1, 2 * i + 1, held[slot, place, half:, half:])
                else:
                    val = held[slot, place]
                    write(2 * i, 2 * j, val)
                    write(2 * j, 2 * i, val.T)

    def turned(mat):
        return flip((mat // 2) % 2, x)

    def load_row(unit, act):
        slot, mat, row = unit % ROW_RING, unit // G, unit % G
        if act is None:
            pltpu.make_async_copy(row_held.at[slot], row_held.at[slot], row_in.at[slot]).wait()
            return
        flipped = turned(mat)
        for k in range(G):
            place = (1 - flipped) * (row * G + k) + flipped * (k * G + row)
            act(pltpu.make_async_copy(land.at[mat * G * G + place], row_held.at[slot, k], row_in.at[slot]))

    def store_row(unit):
        slot, mat, row = unit % ROW_RING, unit // G, unit % G
        return pltpu.make_async_copy(
            row_block.at[slot], out.at[mat, pl.ds(row * tile, tile), :], row_out.at[slot]
        )

    def turn_row(unit):
        slot = unit % ROW_RING
        flipped = turned(unit // G)

        @pl.when(flipped == 0)
        def _():
            for k in range(G):
                row_block[slot, :, pl.ds(k * tile, tile)] = row_held[slot, k]

        @pl.when(flipped == 1)
        def _():
            for k in range(G):
                row_block[slot, :, pl.ds(k * tile, tile)] = row_held[slot, k].T

    pl.when(differ == 0)(lambda: ring(mats, RING, load, store, mirror))
    pl.when(differ == 1)(lambda: ring(mats * G, ROW_RING, load_row, store_row, turn_row))


def solution(mesh):
    def local_purify(ham, bounds, occ):
        mats, blk, _ = ham.shape
        tile = blk // G
        any_spec = pl.BlockSpec(memory_space=pltpu.HBM)
        smem = pl.BlockSpec(memory_space=pltpu.SMEM)
        limb = pltpu.VMEM((3, NB, NB, tile, tile), BF16)
        flops = 2 * 6 * 21 * 36 * 2 * tile**3
        land, ener = pl.pallas_call(
            main_kernel,
            out_shape=(
                jax.ShapeDtypeStruct((mats * G * G, tile, tile), F32),
                jax.ShapeDtypeStruct((mats, 8, 128), F32),
            ),
            in_specs=[smem, smem, any_spec],
            out_specs=(any_spec, any_spec),
            scratch_shapes=[
                limb, limb, limb,
                pltpu.VMEM((3, UPPER + 1, tile, tile), F32),
                pltpu.VMEM((3, 8, tile), F32),
                pltpu.VMEM((2, 8, 128), F32),
                pltpu.VMEM((2, NB, tile // 2, tile // 2), F32),
                pltpu.VMEM((2, 8, tile // 2), F32),
                pltpu.VMEM((8, tile // 2), F32),
                pltpu.VMEM((8, tile), F32),
                pltpu.VMEM((8, tile), F32),
                pltpu.SemaphoreType.DMA((3,)),
                pltpu.SemaphoreType.DMA((3,)),
                pltpu.SemaphoreType.DMA((2,)),
                pltpu.SemaphoreType.DMA,
                pltpu.SemaphoreType.DMA,
                pltpu.SemaphoreType.DMA,
                pltpu.SemaphoreType.DMA,
                pltpu.SemaphoreType.DMA,
                pltpu.SemaphoreType.DMA,
                pltpu.SemaphoreType.DMA,
                pltpu.SemaphoreType.DMA,
                pltpu.SemaphoreType.DMA((2, 2, G * G)),
                pltpu.SemaphoreType.DMA,
                pltpu.SemaphoreType.DMA,
                pltpu.SemaphoreType.DMA,
            ],
            compiler_params=pltpu.CompilerParams(
                collective_id=0,
                has_side_effects=True,
                vmem_limit_bytes=67043328,
            ),
            cost_estimate=pl.CostEstimate(flops=flops, bytes_accessed=120 * 2**20, transcendentals=0),
            name='purify',
        )(bounds.T, occ, ham)

        return pl.pallas_call(
            unpack_kernel,
            out_shape=(
                jax.ShapeDtypeStruct(ham.shape, F32),
                jax.ShapeDtypeStruct((mats,), F32),
            ),
            in_specs=[any_spec, pl.BlockSpec(memory_space=pltpu.VMEM)],
            out_specs=(any_spec, pl.BlockSpec(memory_space=pltpu.VMEM)),
            scratch_shapes=[
                pltpu.VMEM((RING, UPPER3, tile, tile), F32),
                pltpu.VMEM((RING, blk, blk), F32),
                pltpu.VMEM((ROW_RING, G, tile, tile), F32),
                pltpu.VMEM((ROW_RING, tile, blk), F32),
                pltpu.SemaphoreType.DMA((RING,)),
                pltpu.SemaphoreType.DMA((RING,)),
                pltpu.SemaphoreType.DMA((ROW_RING,)),
                pltpu.SemaphoreType.DMA((ROW_RING,)),
            ],
            compiler_params=pltpu.CompilerParams(vmem_limit_bytes=40 * 2**20),
            cost_estimate=pl.CostEstimate(flops=10**6, bytes_accessed=75 * 2**20, transcendentals=0),
            name='unpack',
        )(land, ener)

    mat_spec = P('spin', 'row', 'col')
    return jax.shard_map(
        local_purify, mesh=mesh,
        in_specs=(mat_spec, P('spin', None), P('spin')),
        out_specs=(mat_spec, P('spin')), check_vma=False,
    )
```
